16 devices in a mesh: col: 4 (over z, y), row: 4 (over x, core).
Axes of the slice: x: 2, y: 2, z: 2, core: 2. Of those that a mesh axis runs over, the one named last changes fastest.
Arguments:
- vel_u: float32 [41, 384, 2048], P(None, 'row', 'col')
- vel_v: float32 [41, 384, 2048], P(None, 'row', 'col')
- temperature: float32 [41, 384, 2048], P(None, 'row', 'col')
- salinity: float32 [41, 384, 2048], P(None, 'row', 'col')
- sea_level: float32 [384, 2048], P('row', 'col')
- trans_u: float32 [384, 2048], P('row', 'col')
- trans_v: float32 [384, 2048], P('row', 'col')
- bathymetry: float32 [384, 2048], P('row', 'col')
- kmt_levels: int32 [384, 2048], P('row', 'col')
- tide_force: float32 [36, 2], replicated
Outputs:
- output 1: float32 [384, 2048], P('row', 'col')
- output 2: float32 [384, 2048], P('row', 'col')
- output 3: float32 [384, 2048], P('row', 'col')
- output 4: float32 [41, 384, 2048], P(None, 'row', 'col')
- output 5: float32 [41, 384, 2048], P(None, 'row', 'col')
- output 6: float32 [41, 384, 2048], P(None, 'row', 'col')
- output 7: float32 [41, 384, 2048], P(None, 'row', 'col')
All inputs are finite; a program needn't handle non-finite values.
Results may differ from the reference program's by a relative error of at most 0.001.
Values sent between devices are 32-bit elements.
A program may use at most 1 GiB of HBM per device.

```python
import jax
import jax.numpy as jnp
from jax import lax

LEVELS = 41
SUBCYCLES = 36
GRID_NY = 384
GRID_NX = 2048

GRAVITY = 1.0
GRID_DX = 1.0
TIME_STEP = 4.0
ALPHA_T = 0.02
BETA_S = 0.015
T_REF = 1.0
S_REF = 1.0
VISC_KV = 0.001
DIFF_KT = 0.0005


def pad_halo(field):
    wrapped = jnp.concatenate([field[..., -1:], field, field[..., :1]], axis=-1)
    walls = jnp.zeros_like(wrapped[..., :1, :])
    return jnp.concatenate([walls, wrapped, walls], axis=-2)


def level_mask(count, n_levels):
    levels = jnp.arange(n_levels, dtype=jnp.int32)[:, None, None]
    return (levels < count[None]).astype(jnp.float32)


def interface_coef(count, thick, kappa, n_levels):
    levels = jnp.arange(n_levels - 1, dtype=jnp.int32)[:, None, None]
    active = (levels + 1 < count[None]).astype(jnp.float32)
    safe = jnp.where(count > 0, thick, 1.0)
    return active * (TIME_STEP * kappa / (safe * safe))[None]


def column_solve(source, couple):
    edge = jnp.zeros_like(source[:1])
    upper = jnp.concatenate([couple, edge], axis=0)
    lower = jnp.concatenate([edge, couple], axis=0)
    diag = 1.0 + upper + lower

    def forward(carry, slab):
        gain_prev, part_prev = carry
        lower_k, diag_k, upper_k, source_k = slab
        pivot = diag_k - lower_k * gain_prev
        gain = upper_k / pivot
        part = (source_k + lower_k * part_prev) / pivot
        return (gain, part), (gain, part)

    start = (jnp.zeros_like(source[0]), jnp.zeros_like(source[0]))
    _, (gains, parts) = lax.scan(forward, start, (lower, diag, upper, source))

    def backward(below, slab):
        gain, part = slab
        here = part + gain * below
        return here, here

    _, profile = lax.scan(backward, jnp.zeros_like(source[0]), (gains, parts), reverse=True)
    return profile


def geometry(kmt_ext, depth_ext):
    kmt_cell = kmt_ext[1:-1, 1:-1]
    thick_ext = depth_ext / jnp.maximum(kmt_ext, 1).astype(jnp.float32)
    thick_cell = thick_ext[1:-1, 1:-1]
    return {"k_cell": kmt_cell, "k_u": jnp.minimum(kmt_cell, kmt_ext[1:-1, 2:]), "k_v": jnp.minimum(kmt_cell, kmt_ext[2:, 1:-1]), "dz_cell": thick_cell, "dz_u": 0.5 * (thick_cell + thick_ext[1:-1, 2:]), "dz_v": 0.5 * (thick_cell + thick_ext[2:, 1:-1])}


def surface_fields(layout):
    k_faces = jnp.stack([layout["k_u"], layout["k_v"]])
    face_depth = k_faces.astype(jnp.float32) * jnp.stack([layout["dz_u"], layout["dz_v"]])
    face_wet = (k_faces > 0).astype(jnp.float32)
    wet_cell = (layout["k_cell"] > 0).astype(jnp.float32)
    return face_depth, face_wet, wet_cell


def momentum_tend(u_ext, v_ext, p_ext):
    cen_u = 0.5 * (u_ext[:, 1:-1, :-1] + u_ext[:, 1:-1, 1:])
    corner_v = 0.5 * (v_ext[:, :-1, 1:-1] + v_ext[:, :-1, 2:])
    corner_u = 0.5 * (u_ext[:, :-1, 1:-1] + u_ext[:, 1:, 1:-1])
    flux_uu = cen_u * cen_u
    flux_vu = corner_v * corner_u
    tend_u = -(flux_uu[:, :, 1:] - flux_uu[:, :, :-1] + flux_vu[:, 1:, :] - flux_vu[:, :-1, :] + p_ext[:, 1:-1, 2:] - p_ext[:, 1:-1, 1:-1]) / GRID_DX
    cen_v = 0.5 * (v_ext[:, :-1, 1:-1] + v_ext[:, 1:, 1:-1])
    side_u = 0.5 * (u_ext[:, 1:-1, :-1] + u_ext[:, 2:, :-1])
    side_v = 0.5 * (v_ext[:, 1:-1, :-1] + v_ext[:, 1:-1, 1:])
    flux_vv = cen_v * cen_v
    flux_uv = side_u * side_v
    tend_v = -(flux_vv[:, 1:, :] - flux_vv[:, :-1, :] + flux_uv[:, :, 1:] - flux_uv[:, :, :-1] + p_ext[:, 2:, 1:-1] - p_ext[:, 1:-1, 1:-1]) / GRID_DX
    return tend_u, tend_v


def baroclinic_predict(vel_u, vel_v, temperature, salinity, layout, halo_fn):
    n_levels = vel_u.shape[0]
    mask_c = level_mask(layout["k_cell"], n_levels)
    mask_u = level_mask(layout["k_u"], n_levels)
    mask_v = level_mask(layout["k_v"], n_levels)
    vel_um = vel_u * mask_u
    vel_vm = vel_v * mask_v
    density = mask_c * (BETA_S * (salinity - S_REF) - ALPHA_T * (temperature - T_REF))
    pressure = GRAVITY * layout["dz_cell"] * (jnp.cumsum(density, axis=0) - 0.5 * density)
    cell_coef = interface_coef(layout["k_cell"], layout["dz_cell"], DIFF_KT, n_levels)
    temp_mix = column_solve(temperature * mask_c, cell_coef)
    salt_mix = column_solve(salinity * mask_c, cell_coef)
    edges = halo_fn(jnp.stack([vel_um, vel_vm, pressure, temp_mix, salt_mix]))
    tend_u, tend_v = momentum_tend(edges[0], edges[1], edges[2])
    u_star = column_solve(mask_u * (vel_um + TIME_STEP * tend_u), interface_coef(layout["k_u"], layout["dz_u"], VISC_KV, n_levels))
    v_star = column_solve(mask_v * (vel_vm + TIME_STEP * tend_v), interface_coef(layout["k_v"], layout["dz_v"], VISC_KV, n_levels))
    forcing = jnp.stack([jnp.sum(layout["dz_u"] * (u_star - vel_um), axis=0), jnp.sum(layout["dz_v"] * (v_star - vel_vm), axis=0)]) / TIME_STEP
    return u_star, v_star, forcing, edges[3:], (mask_c, mask_u, mask_v)


def barotropic(eta_start, trans_start, face_depth, face_wet, wet_cell, forcing, tide_force, halo_fn):
    n_sub = tide_force.shape[0]
    dt_sub = TIME_STEP / n_sub
    weight_norm = 6.0 / (n_sub * (n_sub + 1) * (n_sub + 2))

    def substep(step, carry):
        eta_now, trans_now, trans_avg = carry
        trans_ext = halo_fn(trans_now)
        divergence = (trans_now[0] - trans_ext[0, 1:-1, :-2] + trans_now[1] - trans_ext[1, :-2, 1:-1]) / GRID_DX
        eta_next = wet_cell * (eta_now - dt_sub * divergence)
        eta_ext = halo_fn(eta_next)
        slope = jnp.stack([eta_ext[1:-1, 2:] - eta_next, eta_ext[2:, 1:-1] - eta_next]) / GRID_DX
        tide_now = lax.dynamic_index_in_dim(tide_force, step, 0, keepdims=False)
        trans_next = face_wet * (trans_now + dt_sub * (face_depth * (tide_now[:, None, None] - GRAVITY * slope) + forcing))
        weight = weight_norm * ((step + 1) * (n_sub - step)).astype(jnp.float32)
        return eta_next, trans_next, trans_avg + weight * trans_next

    return lax.fori_loop(0, n_sub, substep, (eta_start, trans_start, jnp.zeros_like(trans_start)))


def correct_velocity(star, dz_face, depth_face, mean_trans, mask):
    safe = jnp.where(depth_face > 0, depth_face, 1.0)
    return mask * (star + ((mean_trans - jnp.sum(dz_face * star, axis=0)) / safe)[None])


def advect_tracers(tracer_ext, flow_ext, mask_c):
    flux_x = flow_ext[0, :, 1:-1, :-1] * (0.5 * (tracer_ext[..., 1:-1, :-1] + tracer_ext[..., 1:-1, 1:]))
    flux_y = flow_ext[1, :, :-1, 1:-1] * (0.5 * (tracer_ext[..., :-1, 1:-1] + tracer_ext[..., 1:, 1:-1]))
    divergence = (flux_x[..., 1:] - flux_x[..., :-1] + flux_y[..., 1:, :] - flux_y[..., :-1, :]) / GRID_DX
    return mask_c * (tracer_ext[..., 1:-1, 1:-1] - TIME_STEP * divergence)


def baroclinic_finish(u_star, v_star, trans_avg, face_depth, layout, tracer_ext, masks, halo_fn):
    mask_c, mask_u, mask_v = masks
    vel_uc = correct_velocity(u_star, layout["dz_u"], face_depth[0], trans_avg[0], mask_u)
    vel_vc = correct_velocity(v_star, layout["dz_v"], face_depth[1], trans_avg[1], mask_v)
    flows = halo_fn(jnp.stack([vel_uc, vel_vc]))
    tracers = advect_tracers(tracer_ext, flows, mask_c)
    return vel_uc, vel_vc, tracers[0], tracers[1]


def ocean_step(vel_u, vel_v, temperature, salinity, sea_level, trans_u, trans_v, bathymetry, kmt_levels, tide_force, halo_fn):
    layout = geometry(halo_fn(kmt_levels), halo_fn(bathymetry))
    u_star, v_star, forcing, tracer_ext, masks = baroclinic_predict(vel_u, vel_v, temperature, salinity, layout, halo_fn)
    face_depth, face_wet, wet_cell = surface_fields(layout)
    eta_new, trans_new, trans_avg = barotropic(wet_cell * sea_level, face_wet * jnp.stack([trans_u, trans_v]), face_depth, face_wet, wet_cell, forcing, tide_force, halo_fn)
    vel_uc, vel_vc, temp_new, salt_new = baroclinic_finish(u_star, v_star, trans_avg, face_depth, layout, tracer_ext, masks, halo_fn)
    return eta_new, trans_new[0], trans_new[1], vel_uc, vel_vc, temp_new, salt_new


def draw_levels(key):
    key_count, key_land = jax.random.split(key)
    counts = jax.random.randint(key_count, (GRID_NY, GRID_NX), (LEVELS + 2) // 3, LEVELS + 1)
    land = jax.random.randint(key_land, (GRID_NY, GRID_NX), 0, 12) == 0
    levels = jnp.where(land, 0, counts).astype(jnp.int32)
    return levels.at[0, 0].set(0).at[GRID_NY - 1, GRID_NX - 1].set(LEVELS)


def setup_inputs(seed: int = 0) -> dict:
    keys = jax.random.split(jax.random.key(seed), 10)
    shape_cube = (LEVELS, GRID_NY, GRID_NX)
    shape_plane = (GRID_NY, GRID_NX)
    depth_frac = jnp.arange(LEVELS, dtype=jnp.float32)[:, None, None] / LEVELS
    return {
        "vel_u": 0.1 * jax.random.normal(keys[0], shape_cube, jnp.float32),
        "vel_v": 0.1 * jax.random.normal(keys[1], shape_cube, jnp.float32),
        "temperature": 2.0 * (1.0 - depth_frac) + 0.5 * jax.random.normal(keys[2], shape_cube, jnp.float32),
        "salinity": 1.0 + depth_frac + 0.3 * jax.random.normal(keys[3], shape_cube, jnp.float32),
        "sea_level": 0.05 * jax.random.normal(keys[4], shape_plane, jnp.float32),
        "trans_u": 0.05 * jax.random.normal(keys[5], shape_plane, jnp.float32),
        "trans_v": 0.05 * jax.random.normal(keys[6], shape_plane, jnp.float32),
        "bathymetry": 0.6 + 0.8 * jax.random.uniform(keys[7], shape_plane, jnp.float32),
        "kmt_levels": draw_levels(keys[8]),
        "tide_force": 0.01 + 0.01 * jax.random.normal(keys[9], (SUBCYCLES, 2), jnp.float32),
    }


def reference(vel_u, vel_v, temperature, salinity, sea_level, trans_u, trans_v, bathymetry, kmt_levels, tide_force):
    return ocean_step(vel_u, vel_v, temperature, salinity, sea_level, trans_u, trans_v, bathymetry, kmt_levels, tide_force, pad_halo)
```

```python
import functools

import jax
import jax.numpy as jnp
from jax import lax
from jax.experimental import pallas as pl
from jax.experimental.pallas import tpu as pltpu
from jax.sharding import PartitionSpec as P

NL = 41
NR = 96
NC = 512
LN = 128
LP = 48
HR = 40
ER = NR + 2 * HR
EC = NC + 128
NB = NR // 8
SUB = 36
DT = 4.0
DTB = DT / SUB
KV = 0.001
KT = 0.0005
F32 = jnp.float32
HT = HR // 8
ET = ER // 8
SLAB, ROW, WIDE, TILE = (NL, 8, NC), (8, NC), (8, EC), (8, LN)
VM = pltpu.VMEM


def only(mask, x):
    return jnp.where(mask, x, jnp.zeros_like(x))


def iota(shape, dim):
    return lax.broadcasted_iota(jnp.int32, shape, dim)


def tile_rows(i):
    return slice(8 * i, 8 * (i + 1))


def from_west(x):
    return pltpu.roll(x, 1, axis=1)


def from_east(x):
    return pltpu.roll(x, x.shape[1] - 1, axis=1)


def lane_to(x, src, dst):
    shift = (dst - src) % LN
    return x if shift == 0 else pltpu.roll(x, shift, axis=1)


def up_row(x, nxt, row):
    return pltpu.roll(jnp.where(row == 0, nxt, x), 7, axis=0)


def down_row(x, prev, row):
    return pltpu.roll(jnp.where(row == 7, prev, x), 1, axis=0)


def couple(count, thick, kappa):
    safe = jnp.where(count > 0, thick, 1.0)
    return DT * kappa / (safe * safe)


def pressure_step(t, s, wet, cum, thick):
    half = only(wet, 0.5 * (0.015 * (s - 1.0) - 0.02 * (t - 1.0)))
    mid = cum + half
    return thick * mid, mid + half


def edge_kernel(u0, u3, v0, v3, t0, s0, kc, hc, uf, vf, ul, vl, tf, sf, kr, hr, pke, pkw, rn, rs):
    b = pl.program_id(0)
    lane = iota(TILE, 1)
    cnt = kc[:]
    thick = hc[:] / jnp.maximum(cnt, 1).astype(F32)
    ae = jnp.zeros(TILE, F32)
    aw = jnp.zeros(TILE, F32)
    cum = jnp.zeros(TILE, F32)
    for k in range(NL):
        p, cum = pressure_step(t0[k], s0[k], k < cnt, cum, thick)
        ae = jnp.where(lane == k, lane_to(u3[k], LN - 1, k), ae)
        ae = jnp.where(lane == NL + k, lane_to(v3[k], LN - 1, NL + k), ae)
        aw = jnp.where(lane == k, lane_to(u0[k], 0, k), aw)
        aw = jnp.where(lane == NL + k, lane_to(v0[k], 0, NL + k), aw)
        aw = jnp.where(lane == 2 * NL + k, lane_to(p, 0, 2 * NL + k), aw)
    pke[:] = ae
    pkw[:] = aw

    @pl.when(b == 0)
    def _():
        count = kr[:]
        dz = hr[:] / jnp.maximum(count, 1).astype(F32)
        acc = jnp.zeros(ROW, F32)
        for k in range(NL):
            p, acc = pressure_step(tf[k], sf[k], k < count, acc, dz)
            rn[0, k : k + 1, :] = ul[k, 7:8, :]
            rn[1, k : k + 1, :] = vl[k, 7:8, :]
            rs[0, k : k + 1, :] = uf[k, 0:1, :]
            rs[1, k : k + 1, :] = vf[k, 0:1, :]
            rs[2, k : k + 1, :] = p[0:1, :]
        for i in range(3):
            rs[i, NL:LP, :] = jnp.zeros((LP - NL, NC), F32)
            if i < 2:
                rn[i, NL:LP, :] = jnp.zeros((LP - NL, NC), F32)


def edges(u, v, t, s, kmt, depth):
    def strip(j):
        return pl.BlockSpec((NL, 8, 128), lambda b: (0, b, j))

    def slab(i):
        return pl.BlockSpec(SLAB, lambda b: (0, i, 0))

    col = pl.BlockSpec(TILE, lambda b: (b, 0))
    row0 = pl.BlockSpec(ROW, lambda b: (0, 0))
    return pl.pallas_call(
        edge_kernel,
        grid=(NB,),
        in_specs=[strip(0), strip(3), strip(0), strip(3), strip(0), strip(0), col, col, slab(0), slab(0), slab(NB - 1), slab(NB - 1), slab(0), slab(0), row0, row0],
        out_specs=[col, col, pl.BlockSpec((2, LP, NC), lambda b: (0, 0, 0)), pl.BlockSpec((3, LP, NC), lambda b: (0, 0, 0))],
        out_shape=[
            jax.ShapeDtypeStruct((NR, LN), F32),
            jax.ShapeDtypeStruct((NR, LN), F32),
            jax.ShapeDtypeStruct((2, LP, NC), F32),
            jax.ShapeDtypeStruct((3, LP, NC), F32),
        ],
        compiler_params=pltpu.CompilerParams(dimension_semantics=("arbitrary",)),
        cost_estimate=pl.CostEstimate(flops=10**7, bytes_accessed=16 * 10**6, transcendentals=0),
        name="edges",
    )(u, u, v, v, t, s, kmt, depth, u, v, u, v, t, s, kmt, depth)


def tracer_kernel(t, s, kc, hc, tm, sm, pr, pke, pkw, rn, rs, gains):
    b = pl.program_id(0)
    lane = iota(TILE, 1)
    cnt = kc[:]
    thick = hc[:] / jnp.maximum(cnt, 1).astype(F32)
    c = couple(cnt, thick, KT)
    zero = jnp.zeros(ROW, F32)
    cum = lower = pt = ps = zero
    keep = zero
    for k in range(NL):
        wet = k < cnt
        tk, sk = t[k], s[k]
        p, cum = pressure_step(tk, sk, wet, cum, thick)
        pr[k] = p
        upper = jnp.where(k + 1 < cnt, c, 0.0) if k + 1 < NL else zero
        top = 1.0 + lower * keep if k else jnp.ones_like(zero)
        inv = 1.0 / (top + upper)
        keep = top * inv
        gains[k] = upper * inv
        pt = (jnp.where(wet, tk, 0.0) + lower * pt) * inv
        ps = (jnp.where(wet, sk, 0.0) + lower * ps) * inv
        tm[k] = pt
        sm[k] = ps
        lower = upper
    ae = jnp.zeros(TILE, F32)
    aw = jnp.zeros(TILE, F32)
    bt = bs = zero
    for k in reversed(range(NL)):
        gain = gains[k]
        bt = tm[k] + gain * bt
        bs = sm[k] + gain * bs
        tm[k] = bt
        sm[k] = bs
        for x, base in ((bt, NL), (bs, 2 * NL)):
            ae = jnp.where(lane == base + k, lane_to(x[:, NC - LN :], LN - 1, base + k), ae)
            aw = jnp.where(lane == base + k, lane_to(x[:, :LN], 0, base + k), aw)
    pke[:] = ae
    pkw[:] = aw

    @pl.when(b == 0)
    def _():
        for k in range(NL):
            rs[0, k : k + 1, :] = tm[k, 0:1, :]
            rs[1, k : k + 1, :] = sm[k, 0:1, :]
        for i in range(2):
            rs[i, NL:LP, :] = jnp.zeros((LP - NL, NC), F32)

    @pl.when(b == NB - 1)
    def _():
        for k in range(NL):
            rn[0, k : k + 1, :] = tm[k, 7:8, :]
            rn[1, k : k + 1, :] = sm[k, 7:8, :]
        for i in range(2):
            rn[i, NL:LP, :] = jnp.zeros((LP - NL, NC), F32)


def tracers(t, s, kmt, depth):
    cube = pl.BlockSpec(SLAB, lambda b: (0, b, 0))
    plane = pl.BlockSpec(ROW, lambda b: (b, 0))
    col = pl.BlockSpec(TILE, lambda b: (b, 0))
    rows = pl.BlockSpec((2, LP, NC), lambda b: (0, 0, 0))
    big = jax.ShapeDtypeStruct((NL, NR, NC), F32)
    return pl.pallas_call(
        tracer_kernel,
        grid=(NB,),
        in_specs=[cube, cube, plane, plane],
        out_specs=[cube, cube, cube, col, col, rows, rows],
        out_shape=[big, big, big] + [jax.ShapeDtypeStruct((NR, LN), F32)] * 2 + [jax.ShapeDtypeStruct((2, LP, NC), F32)] * 2,
        scratch_shapes=[VM(SLAB, F32)],
        compiler_params=pltpu.CompilerParams(dimension_semantics=("arbitrary",)),
        cost_estimate=pl.CostEstimate(flops=10**8, bytes_accessed=40 * 10**6, transcendentals=0),
        name="tracers",
    )(t, s, kmt, depth)


def geometry_kernel(pl5, ku, kv, du, dv):
    row = iota(WIDE, 0)
    for i in range(ET):
        lo = tile_rows(i)
        hi = slice(8 * (i + 1), 8 * i + 16) if i + 1 < ET else lo
        k, h = pl5[0, lo, :], pl5[1, lo, :]
        dz = h / jnp.maximum(k, 1.0)
        kn, hn = pl5[0, hi, :], pl5[1, hi, :]
        dzn = hn / jnp.maximum(kn, 1.0)
        ku[lo, :] = jnp.minimum(k, from_east(k))
        kv[lo, :] = jnp.minimum(k, up_row(k, kn, row))
        du[lo, :] = 0.5 * (dz + from_east(dz))
        dv[lo, :] = 0.5 * (dz + up_row(dz, dzn, row))


def geometry(planes):
    return pl.pallas_call(geometry_kernel, out_shape=[jax.ShapeDtypeStruct((ER, EC), F32)] * 4, name="geometry")(planes)


def solve_pair(src_a, src_b, ca, cb, na, nb, out_a, out_b, gain_a, gain_b):
    zero = jnp.zeros(ROW, F32)
    la = lb = pa = pb = wa = wb = zero
    for k in range(NL):
        ua = jnp.where(k + 1 < na, ca, 0.0) if k + 1 < NL else zero
        ub = jnp.where(k + 1 < nb, cb, 0.0) if k + 1 < NL else zero
        ta = 1.0 + la * wa if k else jnp.ones_like(zero)
        tb = 1.0 + lb * wb if k else jnp.ones_like(zero)
        ia = 1.0 / (ta + ua)
        ib = 1.0 / (tb + ub)
        wa, wb = ta * ia, tb * ib
        gain_a[k] = ua * ia
        gain_b[k] = ub * ib
        pa = (src_a[k] + la * pa) * ia
        pb = (src_b[k] + lb * pb) * ib
        src_a[k] = pa
        src_b[k] = pb
        la, lb = ua, ub
    xa = xb = sa = sb = zero
    for k in reversed(range(NL)):
        xa = src_a[k] + gain_a[k] * xa
        xb = src_b[k] + gain_b[k] * xb
        out_a[k] = xa
        out_b[k] = xb
        sa += xa
        sb += xb
    return sa, sb


def momentum_kernel(
    u, un, v, vn, p, pn, ku, kun, kv, kvn, du, dv, kus, kvs, rw, rwn, re, rnorth, rsouth, rown, corner,
    us, vs, fx, fy, su, sv, pke, vrow,
    cc, hh, srcu, srcv, gu, gv,
):
    b = pl.program_id(0)
    last = b == NB - 1
    row = iota(ROW, 0)
    rowx = iota(WIDE, 0)
    lane = iota(TILE, 1)

    @pl.when(b == 0)
    def _():
        lev = iota((LP, NC), 0).astype(F32)
        lev1 = iota((LP, LN), 0)
        ks, kw = kus[7:8, :NC], kvs[7:8, :NC]
        s_u = only(lev < ks, rsouth[0])
        s_v = only(lev < kw, rsouth[1])
        pick = only(iota((LP, LN), 1) == lev1 + NL, corner[7:8, :])
        edge = jnp.sum(pick, axis=1, keepdims=True)
        edge = only(lev[:, :1] < kvs[7:8, NC : NC + 1], edge)
        s_ve = jnp.where(iota((LP, NC), 1) == NC - 1, edge, from_east(s_v))
        u_0 = only(lev < ku[0:1, :NC], rown[0])
        v_0 = only(lev < kv[0:1, :NC], rown[1])
        c_s = 0.25 * ((s_v + s_ve) * (s_u + u_0))
        h_s = s_v + v_0
        h_s = 0.25 * (h_s * h_s) + rown[2]
        for k in range(NL):
            cc[k, 7:8, :] = c_s[k : k + 1, :]
            hh[k, 7:8, :] = h_s[k : k + 1, :]

    kx, ky = ku[:], kv[:]
    kxn, kyn = kun[:], kvn[:, :NC]
    rwv, rwnv, rev = rw[:], rwn[:], re[:]
    zx = jnp.zeros(ROW, F32)
    ax, ay = zx, zx
    for k in range(NL):
        hu = jnp.where(lane == 0, lane_to(rev, k, 0), lane_to(rwv, k, LN - 1))
        hv = jnp.where(lane == 0, lane_to(rev, NL + k, 0), lane_to(rwv, NL + k, LN - 1))
        hp = lane_to(rev, 2 * NL + k, 0)
        hn = lane_to(rwnv, k, LN - 1)
        um = only(k < kx, jnp.concatenate([u[k], hu], axis=1))
        vm = only(k < ky, jnp.concatenate([v[k], hv], axis=1))
        pe = jnp.concatenate([p[k], hp], axis=1)
        nu = jnp.where(last, rnorth[0, k : k + 1, :], un[k])
        nv = jnp.where(last, rnorth[1, k : k + 1, :], vn[k])
        np_ = jnp.where(last, rnorth[2, k : k + 1, :], pn[k])
        nu = only(k < kxn, jnp.concatenate([nu, hn], axis=1))
        nv = only(k < kyn, nv)
        u_n = up_row(um, nu, rowx)
        c = 0.25 * ((vm + from_east(vm)) * (um + u_n))
        g = from_west(um) + um
        g = 0.25 * (g * g) + pe
        ge = from_east(g)[:, :NC]
        v5 = vm[:, :NC]
        h = v5 + up_row(v5, nv, row)
        h = 0.25 * (h * h) + up_row(pe[:, :NC], np_, row)
        cw = from_west(c)[:, :NC]
        c5 = c[:, :NC]
        tu = (ge - g[:, :NC]) + (c5 - down_row(c5, cc[k], row))
        tv = (h - down_row(h, hh[k], row)) + (c5 - cw)
        tu = only(k < kx[:, :NC], tu)
        tv = only(k < ky[:, :NC], tv)
        ax += tu
        ay += tv
        srcu[k] = um[:, :NC] - DT * tu
        srcv[k] = v5 - DT * tv
        cc[k] = c5
        hh[k] = h
    dzu, dzv = du[:, :NC], dv[:, :NC]
    kx, ky = kx[:, :NC], ky[:, :NC]
    fx[:] = -dzu * ax
    fy[:] = -dzv * ay
    sa, sb = solve_pair(srcu, srcv, couple(kx, dzu, KV), couple(ky, dzv, KV), kx, ky, us, vs, gu, gv)
    sa, sb = dzu * sa, dzv * sb
    su[:] = sa
    sv[:] = sb
    ae = jnp.zeros(TILE, F32)
    for k in range(NL):
        ae = jnp.where(lane == k, lane_to(us[k, :, NC - LN :], LN - 1, k), ae)
    pke[:] = jnp.where(lane == 3 * NL, lane_to(sa[:, NC - LN :], LN - 1, 3 * NL), ae)

    @pl.when(last)
    def _():
        for k in range(NL):
            vrow[k : k + 1, :] = vs[k, 7:8, :]
        vrow[NL : NL + 1, :] = sb[7:8, :]
        vrow[NL + 1 : LP, :] = jnp.zeros((LP - NL - 1, NC), F32)


def momentum(u, v, p, geo, rw, re, rnorth, rsouth, rown, corner):
    ku, kv, du, dv = geo
    cube = pl.BlockSpec(SLAB, lambda b: (0, b, 0))
    cubn = pl.BlockSpec(SLAB, lambda b: (0, jnp.minimum(b + 1, NB - 1), 0))
    wide = pl.BlockSpec(WIDE, lambda b: (HT + b, 0))
    widn = pl.BlockSpec(WIDE, lambda b: (HT + 1 + b, 0))
    wids = pl.BlockSpec(WIDE, lambda b: (HT - 1, 0))
    plane = pl.BlockSpec(ROW, lambda b: (b, 0))
    col = pl.BlockSpec(TILE, lambda b: (b, 0))
    coln = pl.BlockSpec(TILE, lambda b: (b + 1, 0))
    big = jax.ShapeDtypeStruct((NL, NR, NC), F32)
    flat = jax.ShapeDtypeStruct((NR, NC), F32)

    def rows(n):
        return pl.BlockSpec((n, LP, NC), lambda b: (0, 0, 0))

    return pl.pallas_call(
        momentum_kernel,
        grid=(NB,),
        in_specs=[cube, cubn, cube, cubn, cube, cubn, wide, widn, wide, widn, wide, wide, wids, wids, col, coln, col, rows(3), rows(2), rows(3), pl.BlockSpec(TILE, lambda b: (0, 0))],
        out_specs=[cube, cube, plane, plane, plane, plane, col, pl.BlockSpec((LP, NC), lambda b: (0, 0))],
        out_shape=[big, big, flat, flat, flat, flat, jax.ShapeDtypeStruct((NR, LN), F32), jax.ShapeDtypeStruct((LP, NC), F32)],
        scratch_shapes=[VM(SLAB, F32)] * 6,
        compiler_params=pltpu.CompilerParams(dimension_semantics=("arbitrary",)),
        cost_estimate=pl.CostEstimate(flops=2 * 10**8, bytes_accessed=64 * 10**6, transcendentals=0),
        name="momentum",
    )(u, u, v, v, p, p, ku, ku, kv, kv, du, dv, ku, kv, rw, rw, re, rnorth, rsouth, rown, corner)


def subcycle_kernel(planes, ku, kv, du, dv, force, tide, eta_o, u_o, v_o, ub_o, vb_o, eta, tu, tv, cu, cv, fu, fv, ub, vb):
    nt = ET
    row = iota(WIDE, 0)
    zero = jnp.zeros(WIDE, F32)
    for i in range(nt):
        sl = tile_rows(i)
        kx, ky = ku[sl, :], kv[sl, :]
        eta[sl, :] = only(planes[0, sl, :] > 0, planes[2, sl, :])
        tu[sl, :] = only(kx > 0, planes[3, sl, :])
        tv[sl, :] = only(ky > 0, planes[4, sl, :])
        cu[sl, :] = DTB * (kx * du[sl, :])
        cv[sl, :] = DTB * (ky * dv[sl, :])
        fu[sl, :] = only(kx > 0, DTB * force[0, sl, :])
        fv[sl, :] = only(ky > 0, DTB * force[1, sl, :])
        ub[sl, :] = zero
        vb[sl, :] = zero
    norm = 6.0 / (SUB * (SUB + 1) * (SUB + 2))

    def stage(first, last, lo, hi):
        def step(n, _):
            tx, ty = tide[n, 0], tide[n, 1]
            w = norm * ((n + 1) * (SUB - n)).astype(F32)
            prev_eta = None
            vsouth = tv[8 * lo - 8 : 8 * lo, :] if lo else zero
            for i in range(lo, hi):
                sl = tile_rows(i)
                un, vn = tu[sl, :], tv[sl, :]
                e = eta[sl, :] - DTB * ((un - from_west(un)) + (vn - down_row(vn, vsouth, row)))
                eta[sl, :] = e
                un = un + (cu[sl, :] * (tx - (from_east(e) - e)) + fu[sl, :])
                tu[sl, :] = un
                if lo_bar <= i < hi_bar:
                    ub[sl, :] = ub[sl, :] + w * un
                if i > lo:
                    finish(i - 1, prev_eta, e, vsouth, ty, w)
                prev_eta, vsouth = e, vn
            finish(hi - 1, prev_eta, prev_eta, vsouth, ty, w)
            return 0

        lax.fori_loop(first, last, step, 0)

    lo_bar, hi_bar = HT - 1, HT + NB

    def finish(i, e, north, vold, ty, w):
        sl = tile_rows(i)
        x = vold + (cv[sl, :] * (ty - (up_row(e, north, row) - e)) + fv[sl, :])
        tv[sl, :] = x
        if lo_bar <= i < hi_bar:
            vb[sl, :] = vb[sl, :] + w * x

    for s in range(0, SUB, 8):
        stage(s, min(s + 8, SUB), s // 8, nt - s // 8)
    eta_o[:] = eta[HR : HR + NR, :NC]
    u_o[:] = tu[HR : HR + NR, :NC]
    v_o[:] = tv[HR : HR + NR, :NC]
    ub_o[:] = ub[HR - 8 : HR + NR, :]
    vb_o[:] = vb[HR - 8 : HR + NR, :]


def subcycles(planes, geo, force, tide):
    flat = jax.ShapeDtypeStruct((NR, NC), F32)
    bar = jax.ShapeDtypeStruct((NR + 8, EC), F32)
    vm = pl.BlockSpec(memory_space=VM)
    return pl.pallas_call(
        subcycle_kernel,
        in_specs=[vm] * 6 + [pl.BlockSpec(memory_space=pltpu.SMEM)],
        out_specs=[vm] * 5,
        out_shape=[flat, flat, flat, bar, bar],
        scratch_shapes=[VM((ER, EC), F32)] * 9,
        cost_estimate=pl.CostEstimate(flops=10**8, bytes_accessed=10**6, transcendentals=0),
        name="subcycles",
    )(planes, *geo, force, tide)


def finish_kernel(
    us, vs, t, tn, s, sn, kc, ku, kv, du, dv, ub, vb, su, sv, kvs, dvs, vbs, rw, re, rnorth, rsouth, rown,
    uo, vo, to, so, ct, cs,
):
    b = pl.program_id(0)
    last = b == NB - 1
    row = iota(ROW, 0)
    lane = iota(TILE, 1)

    def correction(mean, total, k, dz):
        deep = k * dz
        return (mean - total) / jnp.where(deep > 0, deep, 1.0)

    @pl.when(b == 0)
    def _():
        lev = iota((LP, NC), 0).astype(F32)
        kx = kvs[7:8, :NC]
        cor = correction(vbs[7:8, :NC], rsouth[0, NL : NL + 1, :], kx, dvs[7:8, :NC])
        vel = 0.5 * DT * only(lev < kx, rsouth[0] + cor)
        ft = vel * (rsouth[1] + rown[0])
        fs = vel * (rsouth[2] + rown[1])
        for k in range(NL):
            ct[k, 7:8, :] = ft[k : k + 1, :]
            cs[k, 7:8, :] = fs[k : k + 1, :]

    kx, ky, cnt = ku[:], kv[:, :NC], kc[:]
    rwv, rev = rw[:], re[:]
    tot = jnp.concatenate([su[:], lane_to(rwv, 3 * NL, LN - 1)], axis=1)
    cx = correction(ub[:], tot, kx, du[:])
    cy = correction(vb[:, :NC], sv[:], ky, dv[:, :NC])
    for k in range(NL):
        ue = jnp.concatenate([us[k], lane_to(rwv, k, LN - 1)], axis=1)
        ue = only(k < kx, ue + cx)
        uo[k] = ue[:, :NC]
        ve = only(k < ky, vs[k] + cy)
        vo[k] = ve
        hx, hy = (0.5 * DT) * ue, (0.5 * DT) * ve
        wet = k < cnt
        for i, (x, nxt, out, carry) in enumerate(((t, tn, to, ct), (s, sn, so, cs))):
            base = NL * (i + 1) + k
            halo = jnp.where(lane == 0, lane_to(rev, base, 0), lane_to(rwv, base, LN - 1))
            own = x[k]
            xe = jnp.concatenate([own, halo], axis=1)
            f = hx * (xe + from_east(xe))
            north = jnp.where(last, rnorth[i, k : k + 1, :], nxt[k])
            fy = hy * (own + up_row(own, north, row))
            div = (f - from_west(f))[:, :NC] + (fy - down_row(fy, carry[k], row))
            carry[k] = fy
            out[k] = only(wet, own - div)


def finish(us, vs, tm, sm, kmt, geo, ub, vb, su, sv, rw, re, rnorth, rsouth, rown):
    ku, kv, du, dv = geo
    cube = pl.BlockSpec(SLAB, lambda b: (0, b, 0))
    cubn = pl.BlockSpec(SLAB, lambda b: (0, jnp.minimum(b + 1, NB - 1), 0))
    wide = pl.BlockSpec(WIDE, lambda b: (HT + b, 0))
    wids = pl.BlockSpec(WIDE, lambda b: (HT - 1, 0))
    bar = pl.BlockSpec(WIDE, lambda b: (b + 1, 0))
    bars = pl.BlockSpec(WIDE, lambda b: (0, 0))
    plane = pl.BlockSpec(ROW, lambda b: (b, 0))
    col = pl.BlockSpec(TILE, lambda b: (b, 0))
    big = jax.ShapeDtypeStruct((NL, NR, NC), F32)

    def rows(n):
        return pl.BlockSpec((n, LP, NC), lambda b: (0, 0, 0))

    return pl.pallas_call(
        finish_kernel,
        grid=(NB,),
        in_specs=[cube, cube, cube, cubn, cube, cubn, plane, wide, wide, wide, wide, bar, bar, plane, plane, wids, wids, bars, col, col, rows(2), rows(3), rows(2)],
        out_specs=[cube] * 4,
        out_shape=[big] * 4,
        scratch_shapes=[VM(SLAB, F32)] * 2,
        compiler_params=pltpu.CompilerParams(dimension_semantics=("arbitrary",)),
        cost_estimate=pl.CostEstimate(flops=10**8, bytes_accessed=80 * 10**6, transcendentals=0),
        name="finish",
    )(us, vs, tm, tm, sm, sm, kmt, ku, kv, du, dv, ub, vb, su, sv, kv, dv, vb, rw, re, rnorth, rsouth, rown)


def solution(mesh):
    n_cols, n_rows = mesh.shape["col"], mesh.shape["row"]

    def send(x, drow, dcol):
        pairs = []
        for c in range(n_cols):
            for r in range(n_rows):
                if 0 <= r + drow < n_rows:
                    pairs.append((c * n_rows + r, ((c + dcol) % n_cols) * n_rows + r + drow))
        return lax.ppermute(x, ("col", "row"), pairs)

    def widen(x):
        lane = lax.broadcasted_iota(jnp.int32, (1, 1, 128), 2)
        east, west = send(x[..., :LN], 0, -1), send(x[..., NC - LN :], 0, 1)
        wide = jnp.concatenate([x, jnp.where(lane < 64, east, west)], axis=-1)
        north, south = send(wide[:, :HR], -1, 0), send(wide[:, NR - HR :], 1, 0)
        return jnp.concatenate([south, wide, north], axis=1)

    def local_step(u, v, t, s, eta, tu, tv, depth, kmt, tide):
        pke, pkw, prn, prs = edges(u, v, t, s, kmt, depth)
        planes = widen(jnp.stack([kmt.astype(F32), depth, eta, tu, tv]))
        rw, re = send(pke, 0, 1), send(pkw, 0, -1)
        rsouth, rnorth = send(prn, 1, 0), send(prs, -1, 0)
        nw = send(pke[:8], -1, 1)
        se = send(pkw[NR - 8 :], 1, -1)
        geo = geometry(planes)
        tm, sm, pr, tke, tkw, trn, trs = tracers(t, s, kmt, depth)
        rw = jnp.concatenate([rw, nw], axis=0)
        us, vs, fx, fy, su, sv, uke, vrow = momentum(u, v, pr, geo, rw, re, rnorth, rsouth, prs, se)
        force = widen(jnp.stack([fx, fy]))
        fw, fe = send(tke + uke, 0, 1), send(tkw, 0, -1)
        fsouth, fnorth = send(jnp.concatenate([vrow[None], trn]), 1, 0), send(trs, -1, 0)
        eta_n, u_n, v_n, ub, vb = subcycles(planes, geo, force, tide)
        uo, vo, to, so = finish(us, vs, tm, sm, kmt, geo, ub, vb, su, sv, fw, fe, fnorth, fsouth, trs)
        return eta_n, u_n, v_n, uo, vo, to, so

    cube, plane = P(None, "row", "col"), P("row", "col")
    return jax.shard_map(
        local_step,
        mesh=mesh,
        in_specs=(cube,) * 4 + (plane,) * 5 + (P(None, None),),
        out_specs=(plane,) * 3 + (cube,) * 4,
        check_vma=False,
    )
```

```python
import functools

import jax
import jax.numpy as jnp
from jax import lax
from jax.experimental import pallas as pl
from jax.experimental.pallas import tpu as pltpu
from jax.sharding import PartitionSpec as P

NL = 41
NR = 96
NC = 512
LN = 128
LP = 48
HR = 40
ER = NR + 2 * HR
EC = NC + 128
NB = NR // 8
SUB = 36
DT = 4.0
DTB = DT / SUB
KV = 0.001
KT = 0.0005
F32 = jnp.float32
HT = HR // 8
ET = ER // 8
SLAB, ROW, WIDE, TILE = (NL, 8, NC), (8, NC), (8, EC), (8, LN)
VM = pltpu.VMEM


def only(mask, x):
    return jnp.where(mask, x, jnp.zeros_like(x))


def iota(shape, dim):
    return lax.broadcasted_iota(jnp.int32, shape, dim)


def tile_rows(i):
    return slice(8 * i, 8 * (i + 1))


def from_west(x):
    return pltpu.roll(x, 1, axis=1)


def from_east(x):
    return pltpu.roll(x, x.shape[1] - 1, axis=1)


def lane_to(x, src, dst):
    shift = (dst - src) % LN
    return x if shift == 0 else pltpu.roll(x, shift, axis=1)


def up_row(x, nxt, row):
    return pltpu.roll(jnp.where(row == 0, nxt, x), 7, axis=0)


def down_row(x, prev, row):
    return pltpu.roll(jnp.where(row == 7, prev, x), 1, axis=0)


def couple(count, thick, kappa):
    safe = jnp.where(count > 0, thick, 1.0)
    return DT * kappa / (safe * safe)


def pressure_step(t, s, wet, cum, thick):
    half = only(wet, 0.5 * (0.015 * (s - 1.0) - 0.02 * (t - 1.0)))
    mid = cum + half
    return thick * mid, mid + half


def edge_kernel(u0, u3, v0, v3, t0, s0, kc, hc, uf, vf, ul, vl, tf, sf, kr, hr, pke, pkw, rn, rs):
    b = pl.program_id(0)
    lane = iota(TILE, 1)
    cnt = kc[:]
    thick = hc[:] / jnp.maximum(cnt, 1).astype(F32)
    ae = jnp.zeros(TILE, F32)
    aw = jnp.zeros(TILE, F32)
    cum = jnp.zeros(TILE, F32)
    for k in range(NL):
        p, cum = pressure_step(t0[k], s0[k], k < cnt, cum, thick)
        ae = jnp.where(lane == k, lane_to(u3[k], LN - 1, k), ae)
        ae = jnp.where(lane == NL + k, lane_to(v3[k], LN - 1, NL + k), ae)
        aw = jnp.where(lane == k, lane_to(u0[k], 0, k), aw)
        aw = jnp.where(lane == NL + k, lane_to(v0[k], 0, NL + k), aw)
        aw = jnp.where(lane == 2 * NL + k, lane_to(p, 0, 2 * NL + k), aw)
    pke[:] = ae
    pkw[:] = aw

    @pl.when(b == 0)
    def _():
        count = kr[:]
        dz = hr[:] / jnp.maximum(count, 1).astype(F32)
        acc = jnp.zeros(ROW, F32)
        for k in range(NL):
            p, acc = pressure_step(tf[k], sf[k], k < count, acc, dz)
            rn[0, k : k + 1, :] = ul[k, 7:8, :]
            rn[1, k : k + 1, :] = vl[k, 7:8, :]
            rs[0, k : k + 1, :] = uf[k, 0:1, :]
            rs[1, k : k + 1, :] = vf[k, 0:1, :]
            rs[2, k : k + 1, :] = p[0:1, :]
        for i in range(3):
            rs[i, NL:LP, :] = jnp.zeros((LP - NL, NC), F32)
            if i < 2:
                rn[i, NL:LP, :] = jnp.zeros((LP - NL, NC), F32)


def edges(u, v, t, s, kmt, depth):
    def strip(j):
        return pl.BlockSpec((NL, 8, 128), lambda b: (0, b, j))

    def slab(i):
        return pl.BlockSpec(SLAB, lambda b: (0, i, 0))

    col = pl.BlockSpec(TILE, lambda b: (b, 0))
    row0 = pl.BlockSpec(ROW, lambda b: (0, 0))
    return pl.pallas_call(
        edge_kernel,
        grid=(NB,),
        in_specs=[strip(0), strip(3), strip(0), strip(3), strip(0), strip(0), col, col, slab(0), slab(0), slab(NB - 1), slab(NB - 1), slab(0), slab(0), row0, row0],
        out_specs=[col, col, pl.BlockSpec((2, LP, NC), lambda b: (0, 0, 0)), pl.BlockSpec((3, LP, NC), lambda b: (0, 0, 0))],
        out_shape=[
            jax.ShapeDtypeStruct((NR, LN), F32),
            jax.ShapeDtypeStruct((NR, LN), F32),
            jax.ShapeDtypeStruct((2, LP, NC), F32),
            jax.ShapeDtypeStruct((3, LP, NC), F32),
        ],
        compiler_params=pltpu.CompilerParams(dimension_semantics=("arbitrary",)),
        cost_estimate=pl.CostEstimate(flops=10**7, bytes_accessed=16 * 10**6, transcendentals=0),
        name="edges",
    )(u, u, v, v, t, s, kmt, depth, u, v, u, v, t, s, kmt, depth)


def tracer_kernel(t, s, kc, hc, tm_b, sm_b, pr_b, pke, pkw, rn, rs_b, gains):
    tm, sm, pr, rs = tm_b.at[0], sm_b.at[0], pr_b.at[0], rs_b.at[0]
    b = pl.program_id(0)
    lane = iota(TILE, 1)
    cnt = kc[:]
    thick = hc[:] / jnp.maximum(cnt, 1).astype(F32)
    c = couple(cnt, thick, KT)
    zero = jnp.zeros(ROW, F32)
    cum = lower = pt = ps = zero
    keep = zero
    for k in range(NL):
        wet = k < cnt
        tk, sk = t[k], s[k]
        p, cum = pressure_step(tk, sk, wet, cum, thick)
        pr[k] = p
        rs[2, k : k + 1, :] = p[0:1, :]
        upper = jnp.where(k + 1 < cnt, c, 0.0) if k + 1 < NL else zero
        top = 1.0 + lower * keep if k else jnp.ones_like(zero)
        inv = 1.0 / (top + upper)
        keep = top * inv
        gains[k] = upper * inv
        pt = (jnp.where(wet, tk, 0.0) + lower * pt) * inv
        ps = (jnp.where(wet, sk, 0.0) + lower * ps) * inv
        tm[k] = pt
        sm[k] = ps
        lower = upper
    ae = jnp.zeros(TILE, F32)
    aw = jnp.zeros(TILE, F32)
    bt = bs = zero
    for k in reversed(range(NL)):
        gain = gains[k]
        bt = tm[k] + gain * bt
        bs = sm[k] + gain * bs
        tm[k] = bt
        sm[k] = bs
        rs[0, k : k + 1, :] = bt[0:1, :]
        rs[1, k : k + 1, :] = bs[0:1, :]
        for x, base in ((bt, NL), (bs, 2 * NL)):
            ae = jnp.where(lane == base + k, lane_to(x[:, NC - LN :], LN - 1, base + k), ae)
            aw = jnp.where(lane == base + k, lane_to(x[:, :LN], 0, base + k), aw)
    pke[:] = ae
    pkw[:] = aw

    @pl.when(b == NB - 1)
    def _():
        for k in range(NL):
            rn[0, k : k + 1, :] = tm[k, 7:8, :]
            rn[1, k : k + 1, :] = sm[k, 7:8, :]
        for i in range(2):
            rn[i, NL:LP, :] = jnp.zeros((LP - NL, NC), F32)


PACK = jax.ShapeDtypeStruct((NB,) + SLAB, F32)


def block_major(f):
    return pl.BlockSpec((1,) + SLAB, lambda b: (f(b), 0, 0, 0))


def first_rows(f):
    return pl.BlockSpec((1, 3, LP, NC), lambda b: (f(b), 0, 0, 0))


def tracers(t, s, kmt, depth):
    cube = pl.BlockSpec(SLAB, lambda b: (0, b, 0))
    pack = block_major(lambda b: b)
    plane = pl.BlockSpec(ROW, lambda b: (b, 0))
    col = pl.BlockSpec(TILE, lambda b: (b, 0))
    rows = pl.BlockSpec((2, LP, NC), lambda b: (0, 0, 0))
    return pl.pallas_call(
        tracer_kernel,
        grid=(NB,),
        in_specs=[cube, cube, plane, plane],
        out_specs=[pack, pack, pack, col, col, rows, first_rows(lambda b: b)],
        out_shape=[PACK, PACK, PACK] + [jax.ShapeDtypeStruct((NR, LN), F32)] * 2 + [jax.ShapeDtypeStruct((2, LP, NC), F32), jax.ShapeDtypeStruct((NB, 3, LP, NC), F32)],
        scratch_shapes=[VM(SLAB, F32)],
        compiler_params=pltpu.CompilerParams(dimension_semantics=("arbitrary",)),
        cost_estimate=pl.CostEstimate(flops=10**8, bytes_accessed=40 * 10**6, transcendentals=0),
        name="tracers",
    )(t, s, kmt, depth)


def geometry_kernel(pl5, ku, kv, du, dv):
    row = iota(WIDE, 0)
    for i in range(ET):
        lo = tile_rows(i)
        hi = slice(8 * (i + 1), 8 * i + 16) if i + 1 < ET else lo
        k, h = pl5[0, lo, :], pl5[1, lo, :]
        dz = h / jnp.maximum(k, 1.0)
        kn, hn = pl5[0, hi, :], pl5[1, hi, :]
        dzn = hn / jnp.maximum(kn, 1.0)
        ku[lo, :] = jnp.minimum(k, from_east(k))
        kv[lo, :] = jnp.minimum(k, up_row(k, kn, row))
        du[lo, :] = 0.5 * (dz + from_east(dz))
        dv[lo, :] = 0.5 * (dz + up_row(dz, dzn, row))


def geometry(planes):
    return pl.pallas_call(geometry_kernel, out_shape=[jax.ShapeDtypeStruct((ER, EC), F32)] * 4, name="geometry")(planes)


def solve_pair(src_a, src_b, ca, cb, na, nb, out_a, out_b, gain_a, gain_b):
    zero = jnp.zeros(ROW, F32)
    la = lb = pa = pb = wa = wb = zero
    for k in range(NL):
        ua = jnp.where(k + 1 < na, ca, 0.0) if k + 1 < NL else zero
        ub = jnp.where(k + 1 < nb, cb, 0.0) if k + 1 < NL else zero
        ta = 1.0 + la * wa if k else jnp.ones_like(zero)
        tb = 1.0 + lb * wb if k else jnp.ones_like(zero)
        ia = 1.0 / (ta + ua)
        ib = 1.0 / (tb + ub)
        wa, wb = ta * ia, tb * ib
        gain_a[k] = ua * ia
        gain_b[k] = ub * ib
        pa = (src_a[k] + la * pa) * ia
        pb = (src_b[k] + lb * pb) * ib
        src_a[k] = pa
        src_b[k] = pb
        la, lb = ua, ub
    xa = xb = sa = sb = zero
    for k in reversed(range(NL)):
        xa = src_a[k] + gain_a[k] * xa
        xb = src_b[k] + gain_b[k] * xb
        out_a[k] = xa
        out_b[k] = xb
        sa += xa
        sb += xb
    return sa, sb


def momentum_kernel(
    u, v, p_b, pfirst, kun, kvn, kux, kvx, du, dv, kus, kvs, rwn, ren, re, rnorth, rsouth, rown, corner,
    us_b, vs_b, fx, fy, su, sv, pke, vrow,
    cc, hh, srcu, srcv, gu, gv, ums, vms,
):
    step = pl.program_id(0)
    last = step == NB
    us, vs, p = us_b.at[0], vs_b.at[0], p_b.at[0]
    row = iota(ROW, 0)
    rowx = iota(WIDE, 0)
    lane = iota(TILE, 1)
    kxn, kyn = kun[:], kvn[:]
    rwv, rev = rwn[:], ren[:]

    def masked(k, uk, vk):
        hu = jnp.where(lane == 0, lane_to(rev, k, 0), lane_to(rwv, k, LN - 1))
        hv = jnp.where(lane == 0, lane_to(rev, NL + k, 0), lane_to(rwv, NL + k, LN - 1))
        um = only(k < kxn, jnp.concatenate([uk, hu], axis=1))
        return um, only(k < kyn, jnp.concatenate([vk, hv], axis=1))

    @pl.when(step == 0)
    def _():
        for k in range(NL):
            ums[k], vms[k] = masked(k, u[k], v[k])
        lev = iota((LP, NC), 0).astype(F32)
        lev1 = iota((LP, LN), 0)
        ks, kw = kus[7:8, :NC], kvs[7:8, :NC]
        s_u = only(lev < ks, rsouth[0])
        s_v = only(lev < kw, rsouth[1])
        pick = only(iota((LP, LN), 1) == lev1 + NL, corner[7:8, :])
        edge = jnp.sum(pick, axis=1, keepdims=True)
        edge = only(lev[:, :1] < kvs[7:8, NC : NC + 1], edge)
        s_ve = jnp.where(iota((LP, NC), 1) == NC - 1, edge, from_east(s_v))
        u_0 = only(lev < kxn[0:1, :NC], rown[0])
        v_0 = only(lev < kyn[0:1, :NC], rown[1])
        c_s = 0.25 * ((s_v + s_ve) * (s_u + u_0))
        h_s = s_v + v_0
        h_s = 0.25 * (h_s * h_s) + rown[2]
        for k in range(NL):
            cc[k, 7:8, :] = c_s[k : k + 1, :]
            hh[k, 7:8, :] = h_s[k : k + 1, :]

    @pl.when(step > 0)
    def _():
        kx, ky = kux[:], kvx[:]
        pev = re[:]
        zx = jnp.zeros(ROW, F32)
        ax, ay = zx, zx
        for k in range(NL):
            um, vm = ums[k], vms[k]
            pe = jnp.concatenate([p[k], lane_to(pev, 2 * NL + k, 0)], axis=1)
            uk = jnp.where(last, rnorth[0, k : k + 1, :], u[k])
            vk = jnp.where(last, rnorth[1, k : k + 1, :], v[k])
            np_ = jnp.where(last, rnorth[2, k : k + 1, :], pfirst[0, 2, k : k + 1, :])
            nu, nv = masked(k, uk, vk)
            ums[k], vms[k] = nu, nv
            u_n = up_row(um, nu, rowx)
            c = 0.25 * ((vm + from_east(vm)) * (um + u_n))
            g = from_west(um) + um
            g = 0.25 * (g * g) + pe
            ge = from_east(g)[:, :NC]
            v5 = vm[:, :NC]
            h = v5 + up_row(v5, nv[:, :NC], row)
            h = 0.25 * (h * h) + up_row(pe[:, :NC], np_, row)
            cw = from_west(c)[:, :NC]
            c5 = c[:, :NC]
            tu = (ge - g[:, :NC]) + (c5 - down_row(c5, cc[k], row))
            tv = (h - down_row(h, hh[k], row)) + (c5 - cw)
            tu = only(k < kx, tu)
            tv = only(k < ky, tv)
            ax += tu
            ay += tv
            srcu[k] = um[:, :NC] - DT * tu
            srcv[k] = v5 - DT * tv
            cc[k] = c5
            hh[k] = h
        dzu, dzv = du[:], dv[:]
        fx[:] = -dzu * ax
        fy[:] = -dzv * ay
        sa, sb = solve_pair(srcu, srcv, couple(kx, dzu, KV), couple(ky, dzv, KV), kx, ky, us, vs, gu, gv)
        sa, sb = dzu * sa, dzv * sb
        su[:] = sa
        sv[:] = sb
        ae = jnp.zeros(TILE, F32)
        for k in range(NL):
            ae = jnp.where(lane == k, lane_to(us[k, :, NC - LN :], LN - 1, k), ae)
        pke[:] = jnp.where(lane == 3 * NL, lane_to(sa[:, NC - LN :], LN - 1, 3 * NL), ae)

        @pl.when(last)
        def _():
            for k in range(NL):
                vrow[k : k + 1, :] = vs[k, 7:8, :]
            vrow[NL : NL + 1, :] = sb[7:8, :]
            vrow[NL + 1 : LP, :] = jnp.zeros((LP - NL - 1, NC), F32)


def momentum(u, v, p, first, geo, rw, re, rnorth, rsouth, rown, corner):
    ku, kv, du, dv = geo

    def this(b):
        return jnp.maximum(b, 1) - 1

    def ahead(b):
        return jnp.minimum(b, NB - 1)

    cube = pl.BlockSpec(SLAB, lambda b: (0, ahead(b), 0))
    pack = block_major(this)
    near = pl.BlockSpec(ROW, lambda b: (HT + this(b), 0))
    widn = pl.BlockSpec(WIDE, lambda b: (HT + b, 0))
    wids = pl.BlockSpec(WIDE, lambda b: (HT - 1, 0))
    plane = pl.BlockSpec(ROW, lambda b: (this(b), 0))
    col = pl.BlockSpec(TILE, lambda b: (this(b), 0))
    colw = pl.BlockSpec(TILE, lambda b: (b, 0))
    cole = pl.BlockSpec(TILE, lambda b: (ahead(b), 0))
    flat = jax.ShapeDtypeStruct((NR, NC), F32)

    def rows(n):
        return pl.BlockSpec((n, LP, NC), lambda b: (0, 0, 0))

    return pl.pallas_call(
        momentum_kernel,
        grid=(NB + 1,),
        in_specs=[cube, cube, pack, first_rows(ahead), widn, widn, near, near, near, near, wids, wids, colw, cole, col, rows(3), rows(2), rows(3), pl.BlockSpec(TILE, lambda b: (0, 0))],
        out_specs=[pack, pack, plane, plane, plane, plane, col, pl.BlockSpec((LP, NC), lambda b: (0, 0))],
        out_shape=[PACK, PACK, flat, flat, flat, flat, jax.ShapeDtypeStruct((NR, LN), F32), jax.ShapeDtypeStruct((LP, NC), F32)],
        scratch_shapes=[VM(SLAB, F32)] * 6 + [VM((NL,) + WIDE, F32)] * 2,
        compiler_params=pltpu.CompilerParams(dimension_semantics=("arbitrary",)),
        cost_estimate=pl.CostEstimate(flops=2 * 10**8, bytes_accessed=64 * 10**6, transcendentals=0),
        name="momentum",
    )(u, v, p, first, ku, kv, ku, kv, du, dv, ku, kv, rw, re, re, rnorth, rsouth, rown, corner)


def subcycle_kernel(planes, ku, kv, du, dv, force, tide, eta_o, u_o, v_o, ub_o, vb_o, eta, tu, tv, cu, cv, fu, fv, ub, vb):
    nt = ET
    row = iota(WIDE, 0)
    zero = jnp.zeros(WIDE, F32)
    for i in range(nt):
        sl = tile_rows(i)
        kx, ky = ku[sl, :], kv[sl, :]
        eta[sl, :] = only(planes[0, sl, :] > 0, planes[2, sl, :])
        tu[sl, :] = only(kx > 0, planes[3, sl, :])
        tv[sl, :] = only(ky > 0, planes[4, sl, :])
        cu[sl, :] = DTB * (kx * du[sl, :])
        cv[sl, :] = DTB * (ky * dv[sl, :])
        fu[sl, :] = only(kx > 0, DTB * force[0, sl, :])
        fv[sl, :] = only(ky > 0, DTB * force[1, sl, :])
        ub[sl, :] = zero
        vb[sl, :] = zero
    norm = 6.0 / (SUB * (SUB + 1) * (SUB + 2))

    def stage(first, last, lo, hi):
        def step(n, _):
            tx, ty = tide[n, 0], tide[n, 1]
            w = norm * ((n + 1) * (SUB - n)).astype(F32)
            prev_eta = None
            vsouth = tv[8 * lo - 8 : 8 * lo, :] if lo else zero
            for i in range(lo, hi):
                sl = tile_rows(i)
                un, vn = tu[sl, :], tv[sl, :]
                e = eta[sl, :] - DTB * ((un - from_west(un)) + (vn - down_row(vn, vsouth, row)))
                eta[sl, :] = e
                un = un + (cu[sl, :] * (tx - (from_east(e) - e)) + fu[sl, :])
                tu[sl, :] = un
                if lo_bar <= i < hi_bar:
                    ub[sl, :] = ub[sl, :] + w * un
                if i > lo:
                    finish(i - 1, prev_eta, e, vsouth, ty, w)
                prev_eta, vsouth = e, vn
            finish(hi - 1, prev_eta, prev_eta, vsouth, ty, w)
            return 0

        lax.fori_loop(first, last, step, 0)

    lo_bar, hi_bar = HT - 1, HT + NB

    def finish(i, e, north, vold, ty, w):
        sl = tile_rows(i)
        x = vold + (cv[sl, :] * (ty - (up_row(e, north, row) - e)) + fv[sl, :])
        tv[sl, :] = x
        if lo_bar <= i < hi_bar:
            vb[sl, :] = vb[sl, :] + w * x

    for s in range(0, SUB, 8):
        stage(s, min(s + 8, SUB), s // 8, nt - s // 8)
    eta_o[:] = eta[HR : HR + NR, :NC]
    u_o[:] = tu[HR : HR + NR, :NC]
    v_o[:] = tv[HR : HR + NR, :NC]
    ub_o[:] = ub[HR - 8 : HR + NR, :]
    vb_o[:] = vb[HR - 8 : HR + NR, :]


def subcycles(planes, geo, force, tide):
    flat = jax.ShapeDtypeStruct((NR, NC), F32)
    bar = jax.ShapeDtypeStruct((NR + 8, EC), F32)
    vm = pl.BlockSpec(memory_space=VM)
    return pl.pallas_call(
        subcycle_kernel,
        in_specs=[vm] * 6 + [pl.BlockSpec(memory_space=pltpu.SMEM)],
        out_specs=[vm] * 5,
        out_shape=[flat, flat, flat, bar, bar],
        scratch_shapes=[VM((ER, EC), F32)] * 9,
        cost_estimate=pl.CostEstimate(flops=10**8, bytes_accessed=10**6, transcendentals=0),
        name="subcycles",
    )(planes, *geo, force, tide)


def finish_kernel(
    us_b, vs_b, t_b, s_b, first, kc, ku, kv, du, dv, ub, vb, su, sv, kvs, dvs, vbs, rw, re, rnorth, rsouth, rown,
    uo, vo, to, so, ct, cs,
):
    us, vs, t, s = us_b.at[0], vs_b.at[0], t_b.at[0], s_b.at[0]
    b = pl.program_id(0)
    last = b == NB - 1
    row = iota(ROW, 0)
    lane = iota(TILE, 1)

    def correction(mean, total, k, dz):
        deep = k * dz
        return (mean - total) / jnp.where(deep > 0, deep, 1.0)

    @pl.when(b == 0)
    def _():
        lev = iota((LP, NC), 0).astype(F32)
        kx = kvs[7:8, :NC]
        cor = correction(vbs[7:8, :NC], rsouth[0, NL : NL + 1, :], kx, dvs[7:8, :NC])
        vel = 0.5 * DT * only(lev < kx, rsouth[0] + cor)
        ft = vel * (rsouth[1] + rown[0, 0])
        fs = vel * (rsouth[2] + rown[0, 1])
        for k in range(NL):
            ct[k, 7:8, :] = ft[k : k + 1, :]
            cs[k, 7:8, :] = fs[k : k + 1, :]

    kx, ky, cnt = ku[:], kv[:, :NC], kc[:]
    rwv, rev = rw[:], re[:]
    tot = jnp.concatenate([su[:], lane_to(rwv, 3 * NL, LN - 1)], axis=1)
    cx = correction(ub[:], tot, kx, du[:])
    cy = correction(vb[:, :NC], sv[:], ky, dv[:, :NC])
    for k in range(NL):
        ue = jnp.concatenate([us[k], lane_to(rwv, k, LN - 1)], axis=1)
        ue = only(k < kx, ue + cx)
        uo[k] = ue[:, :NC]
        ve = only(k < ky, vs[k] + cy)
        vo[k] = ve
        hx, hy = (0.5 * DT) * ue, (0.5 * DT) * ve
        wet = k < cnt
        for i, (x, out, carry) in enumerate(((t, to, ct), (s, so, cs))):
            base = NL * (i + 1) + k
            halo = jnp.where(lane == 0, lane_to(rev, base, 0), lane_to(rwv, base, LN - 1))
            own = x[k]
            xe = jnp.concatenate([own, halo], axis=1)
            f = hx * (xe + from_east(xe))
            north = jnp.where(last, rnorth[i, k : k + 1, :], first[0, i, k : k + 1, :])
            fy = hy * (own + up_row(own, north, row))
            div = (f - from_west(f))[:, :NC] + (fy - down_row(fy, carry[k], row))
            carry[k] = fy
            out[k] = only(wet, own - div)


def finish(us, vs, tm, sm, first, kmt, geo, ub, vb, su, sv, rw, re, rnorth, rsouth):
    ku, kv, du, dv = geo
    cube = pl.BlockSpec(SLAB, lambda b: (0, b, 0))
    pack = block_major(lambda b: b)
    wide = pl.BlockSpec(WIDE, lambda b: (HT + b, 0))
    wids = pl.BlockSpec(WIDE, lambda b: (HT - 1, 0))
    bar = pl.BlockSpec(WIDE, lambda b: (b + 1, 0))
    bars = pl.BlockSpec(WIDE, lambda b: (0, 0))
    plane = pl.BlockSpec(ROW, lambda b: (b, 0))
    col = pl.BlockSpec(TILE, lambda b: (b, 0))
    big = jax.ShapeDtypeStruct((NL, NR, NC), F32)

    def rows(n):
        return pl.BlockSpec((n, LP, NC), lambda b: (0, 0, 0))

    return pl.pallas_call(
        finish_kernel,
        grid=(NB,),
        in_specs=[pack, pack, pack, pack, first_rows(lambda b: jnp.minimum(b + 1, NB - 1)), plane, wide, wide, wide, wide, bar, bar, plane, plane, wids, wids, bars, col, col, rows(3), rows(3), first_rows(lambda b: 0)],
        out_specs=[cube] * 4,
        out_shape=[big] * 4,
        scratch_shapes=[VM(SLAB, F32)] * 2,
        compiler_params=pltpu.CompilerParams(dimension_semantics=("arbitrary",)),
        cost_estimate=pl.CostEstimate(flops=10**8, bytes_accessed=80 * 10**6, transcendentals=0),
        name="finish",
    )(us, vs, tm, sm, first, kmt, ku, kv, du, dv, ub, vb, su, sv, kv, dv, vb, rw, re, rnorth, rsouth, first)


def solution(mesh):
    n_cols, n_rows = mesh.shape["col"], mesh.shape["row"]

    def send(x, drow, dcol):
        pairs = []
        for c in range(n_cols):
            for r in range(n_rows):
                if 0 <= r + drow < n_rows:
                    pairs.append((c * n_rows + r, ((c + dcol) % n_cols) * n_rows + r + drow))
        return lax.ppermute(x, ("col", "row"), pairs)

    def widen(x):
        lane = lax.broadcasted_iota(jnp.int32, (1, 1, 128), 2)
        east, west = send(x[..., :LN], 0, -1), send(x[..., NC - LN :], 0, 1)
        wide = jnp.concatenate([x, jnp.where(lane < 64, east, west)], axis=-1)
        north, south = send(wide[:, :HR], -1, 0), send(wide[:, NR - HR :], 1, 0)
        return jnp.concatenate([south, wide, north], axis=1)

    def local_step(u, v, t, s, eta, tu, tv, depth, kmt, tide):
        pke, pkw, prn, prs = edges(u, v, t, s, kmt, depth)
        planes = widen(jnp.stack([kmt.astype(F32), depth, eta, tu, tv]))
        rw, re = send(pke, 0, 1), send(pkw, 0, -1)
        rsouth, rnorth = send(prn, 1, 0), send(prs, -1, 0)
        nw = send(pke[:8], -1, 1)
        se = send(pkw[NR - 8 :], 1, -1)
        geo = geometry(planes)
        tm, sm, pr, tke, tkw, trn, first = tracers(t, s, kmt, depth)
        rw = jnp.concatenate([rw, nw], axis=0)
        us, vs, fx, fy, su, sv, uke, vrow = momentum(u, v, pr, first, geo, rw, re, rnorth, rsouth, prs, se)
        force = widen(jnp.stack([fx, fy]))
        fw, fe = send(tke + uke, 0, 1), send(tkw, 0, -1)
        fsouth, fnorth = send(jnp.concatenate([vrow[None], trn]), 1, 0), send(first[0], -1, 0)
        eta_n, u_n, v_n, ub, vb = subcycles(planes, geo, force, tide)
        uo, vo, to, so = finish(us, vs, tm, sm, first, kmt, geo, ub, vb, su, sv, fw, fe, fnorth, fsouth)
        return eta_n, u_n, v_n, uo, vo, to, so

    cube, plane = P(None, "row", "col"), P("row", "col")
    return jax.shard_map(
        local_step,
        mesh=mesh,
        in_specs=(cube,) * 4 + (plane,) * 5 + (P(None, None),),
        out_specs=(plane,) * 3 + (cube,) * 4,
        check_vma=False,
    )
```

```python
import functools

import jax
import jax.numpy as jnp
from jax import lax
from jax.experimental import pallas as pl
from jax.experimental.pallas import tpu as pltpu
from jax.sharding import PartitionSpec as P

NL = 41
NR = 96
NC = 512
LN = 128
LP = 48
HR = 40
ER = NR + 2 * HR
EC = NC + 128
NB = NR // 8
SUB = 36
GROUP = 2
TILES = 3
DT = 4.0
DTB = DT / SUB
KV = 0.001
KT = 0.0005
F32 = jnp.float32
HT = HR // 8
ET = ER // 8
SLAB, ROW, WIDE, TILE = (NL, 8, NC), (8, NC), (8, EC), (8, LN)
VM = pltpu.VMEM


def only(mask, x):
    return jnp.where(mask, x, jnp.zeros_like(x))


def iota(shape, dim):
    return lax.broadcasted_iota(jnp.int32, shape, dim)


def tile_rows(i):
    return slice(8 * i, 8 * (i + 1))


def from_west(x):
    return pltpu.roll(x, 1, axis=1)


def from_east(x):
    return pltpu.roll(x, x.shape[1] - 1, axis=1)


def lane_to(x, src, dst):
    shift = (dst - src) % LN
    return x if shift == 0 else pltpu.roll(x, shift, axis=1)


def up_row(x, nxt, row):
    return pltpu.roll(jnp.where(row == 0, nxt, x), 7, axis=0)


def down_row(x, prev, row):
    return pltpu.roll(jnp.where(row == 7, prev, x), 1, axis=0)


def skewed(stages, group, count=NL):
    blocks = [range(k, min(k + group, count)) for k in range(0, count, group)]
    held = {}
    for i in range(len(blocks) + len(stages) - 1):
        for n, stage in enumerate(stages):
            if 0 <= i - n < len(blocks):
                for k in blocks[i - n]:
                    held[k] = stage(k, held[k]) if n else stage(k)


def couple(count, thick, kappa):
    safe = jnp.where(count > 0, thick, 1.0)
    return DT * kappa / (safe * safe)


def pressure_step(t, s, wet, cum, thick):
    half = only(wet, 0.5 * (0.015 * (s - 1.0) - 0.02 * (t - 1.0)))
    mid = cum + half
    return thick * mid, mid + half


def edge_kernel(u0, u3, v0, v3, t0, s0, kc, hc, uf, vf, ul, vl, tf, sf, kr, hr, pke, pkw, rn, rs):
    b = pl.program_id(0)
    lane = iota(TILE, 1)
    cnt = kc[:]
    thick = hc[:] / jnp.maximum(cnt, 1).astype(F32)
    ae = jnp.zeros(TILE, F32)
    aw = jnp.zeros(TILE, F32)
    cum = jnp.zeros(TILE, F32)
    for k in range(NL):
        p, cum = pressure_step(t0[k], s0[k], k < cnt, cum, thick)
        ae = jnp.where(lane == k, lane_to(u3[k], LN - 1, k), ae)
        ae = jnp.where(lane == NL + k, lane_to(v3[k], LN - 1, NL + k), ae)
        aw = jnp.where(lane == k, lane_to(u0[k], 0, k), aw)
        aw = jnp.where(lane == NL + k, lane_to(v0[k], 0, NL + k), aw)
        aw = jnp.where(lane == 2 * NL + k, lane_to(p, 0, 2 * NL + k), aw)
    pke[:] = ae
    pkw[:] = aw

    @pl.when(b == 0)
    def _():
        count = kr[:]
        dz = hr[:] / jnp.maximum(count, 1).astype(F32)
        acc = jnp.zeros(ROW, F32)
        for k in range(NL):
            p, acc = pressure_step(tf[k], sf[k], k < count, acc, dz)
            rn[0, k : k + 1, :] = ul[k, 7:8, :]
            rn[1, k : k + 1, :] = vl[k, 7:8, :]
            rs[0, k : k + 1, :] = uf[k, 0:1, :]
            rs[1, k : k + 1, :] = vf[k, 0:1, :]
            rs[2, k : k + 1, :] = p[0:1, :]
        for i in range(3):
            rs[i, NL:LP, :] = jnp.zeros((LP - NL, NC), F32)
            if i < 2:
                rn[i, NL:LP, :] = jnp.zeros((LP - NL, NC), F32)


def edges(u, v, t, s, kmt, depth):
    def strip(j):
        return pl.BlockSpec((NL, 8, 128), lambda b: (0, b, j))

    def slab(i):
        return pl.BlockSpec(SLAB, lambda b: (0, i, 0))

    col = pl.BlockSpec(TILE, lambda b: (b, 0))
    row0 = pl.BlockSpec(ROW, lambda b: (0, 0))
    return pl.pallas_call(
        edge_kernel,
        grid=(NB,),
        in_specs=[strip(0), strip(3), strip(0), strip(3), strip(0), strip(0), col, col, slab(0), slab(0), slab(NB - 1), slab(NB - 1), slab(0), slab(0), row0, row0],
        out_specs=[col, col, pl.BlockSpec((2, LP, NC), lambda b: (0, 0, 0)), pl.BlockSpec((3, LP, NC), lambda b: (0, 0, 0))],
        out_shape=[
            jax.ShapeDtypeStruct((NR, LN), F32),
            jax.ShapeDtypeStruct((NR, LN), F32),
            jax.ShapeDtypeStruct((2, LP, NC), F32),
            jax.ShapeDtypeStruct((3, LP, NC), F32),
        ],
        compiler_params=pltpu.CompilerParams(dimension_semantics=("arbitrary",)),
        cost_estimate=pl.CostEstimate(flops=10**7, bytes_accessed=16 * 10**6, transcendentals=0),
        name="edges",
    )(u, u, v, v, t, s, kmt, depth, u, v, u, v, t, s, kmt, depth)


def tracer_kernel(t, s, kc, hc, tm_b, sm_b, pr_b, pke, pkw, rn, rs_b, gains):
    b = pl.program_id(0)
    for half in range(2):
        sl = tile_rows(half)
        tm, sm, rs = tm_b.at[half], sm_b.at[half], rs_b.at[half]
        mix_tracers(t.at[:, sl, :], s.at[:, sl, :], kc[sl, :], hc[sl, :], tm, sm, pr_b.at[half], pke.at[sl, :], pkw.at[sl, :], rs, gains)

    @pl.when(b == NB // 2 - 1)
    def _():
        for k in range(NL):
            rn[0, k : k + 1, :] = tm[k, 7:8, :]
            rn[1, k : k + 1, :] = sm[k, 7:8, :]
        for i in range(2):
            rn[i, NL:LP, :] = jnp.zeros((LP - NL, NC), F32)


def mix_tracers(t, s, cnt, depth, tm, sm, pr, pke, pkw, rs, gains):
    lane = iota(TILE, 1)
    thick = depth / jnp.maximum(cnt, 1).astype(F32)
    c = couple(cnt, thick, KT)
    zero = jnp.zeros(ROW, F32)
    cum = lower = pt = ps = zero
    keep = zero
    for k in range(NL):
        wet = k < cnt
        tk, sk = t[k], s[k]
        p, cum = pressure_step(tk, sk, wet, cum, thick)
        pr[k] = p
        rs[2, k : k + 1, :] = p[0:1, :]
        upper = jnp.where(k + 1 < cnt, c, 0.0) if k + 1 < NL else zero
        top = 1.0 + lower * keep if k else jnp.ones_like(zero)
        inv = 1.0 / (top + upper)
        keep = top * inv
        gains[k] = upper * inv
        pt = (jnp.where(wet, tk, 0.0) + lower * pt) * inv
        ps = (jnp.where(wet, sk, 0.0) + lower * ps) * inv
        tm[k] = pt
        sm[k] = ps
        lower = upper
    ae = jnp.zeros(TILE, F32)
    aw = jnp.zeros(TILE, F32)
    bt = bs = zero
    for k in reversed(range(NL)):
        gain = gains[k]
        bt = tm[k] + gain * bt
        bs = sm[k] + gain * bs
        tm[k] = bt
        sm[k] = bs
        rs[0, k : k + 1, :] = bt[0:1, :]
        rs[1, k : k + 1, :] = bs[0:1, :]
        for x, base in ((bt, NL), (bs, 2 * NL)):
            ae = jnp.where(lane == base + k, lane_to(x[:, NC - LN :], LN - 1, base + k), ae)
            aw = jnp.where(lane == base + k, lane_to(x[:, :LN], 0, base + k), aw)
    pke[:] = ae
    pkw[:] = aw


PACK = jax.ShapeDtypeStruct((NB,) + SLAB, F32)


def block_major(f, n=1):
    return pl.BlockSpec((n,) + SLAB, lambda b: (f(b), 0, 0, 0))


def first_rows(f, n=1):
    return pl.BlockSpec((n, 3, LP, NC), lambda b: (f(b), 0, 0, 0))


def tracers(t, s, kmt, depth):
    cube = pl.BlockSpec((NL, 16, NC), lambda b: (0, b, 0))
    pack = block_major(lambda b: b, 2)
    plane = pl.BlockSpec((16, NC), lambda b: (b, 0))
    col = pl.BlockSpec((16, LN), lambda b: (b, 0))
    rows = pl.BlockSpec((2, LP, NC), lambda b: (0, 0, 0))
    return pl.pallas_call(
        tracer_kernel,
        grid=(NB // 2,),
        in_specs=[cube, cube, plane, plane],
        out_specs=[pack, pack, pack, col, col, rows, first_rows(lambda b: b, 2)],
        out_shape=[PACK, PACK, PACK] + [jax.ShapeDtypeStruct((NR, LN), F32)] * 2 + [jax.ShapeDtypeStruct((2, LP, NC), F32), jax.ShapeDtypeStruct((NB, 3, LP, NC), F32)],
        scratch_shapes=[VM(SLAB, F32)],
        compiler_params=pltpu.CompilerParams(dimension_semantics=("arbitrary",)),
        cost_estimate=pl.CostEstimate(flops=10**8, bytes_accessed=40 * 10**6, transcendentals=0),
        name="tracers",
    )(t, s, kmt, depth)


def geometry_kernel(pl5, ku, kv, du, dv):
    row = iota(WIDE, 0)
    for i in range(ET):
        lo = tile_rows(i)
        hi = slice(8 * (i + 1), 8 * i + 16) if i + 1 < ET else lo
        k, h = pl5[0, lo, :], pl5[1, lo, :]
        dz = h / jnp.maximum(k, 1.0)
        kn, hn = pl5[0, hi, :], pl5[1, hi, :]
        dzn = hn / jnp.maximum(kn, 1.0)
        ku[lo, :] = jnp.minimum(k, from_east(k))
        kv[lo, :] = jnp.minimum(k, up_row(k, kn, row))
        du[lo, :] = 0.5 * (dz + from_east(dz))
        dv[lo, :] = 0.5 * (dz + up_row(dz, dzn, row))


def geometry(planes):
    return pl.pallas_call(geometry_kernel, out_shape=[jax.ShapeDtypeStruct((ER, EC), F32)] * 4, name="geometry")(planes)


def solve_pair(src_a, src_b, ca, cb, na, nb, out_a, out_b, gain_a, gain_b):
    zero = jnp.zeros(ROW, F32)
    la = lb = pa = pb = wa = wb = zero
    for k in range(NL):
        ua = jnp.where(k + 1 < na, ca, 0.0) if k + 1 < NL else zero
        ub = jnp.where(k + 1 < nb, cb, 0.0) if k + 1 < NL else zero
        ta = 1.0 + la * wa if k else jnp.ones_like(zero)
        tb = 1.0 + lb * wb if k else jnp.ones_like(zero)
        ia = 1.0 / (ta + ua)
        ib = 1.0 / (tb + ub)
        wa, wb = ta * ia, tb * ib
        gain_a[k] = ua * ia
        gain_b[k] = ub * ib
        pa = (src_a[k] + la * pa) * ia
        pb = (src_b[k] + lb * pb) * ib
        src_a[k] = pa
        src_b[k] = pb
        la, lb = ua, ub
    xa = xb = sa = sb = zero
    for k in reversed(range(NL)):
        xa = src_a[k] + gain_a[k] * xa
        xb = src_b[k] + gain_b[k] * xb
        out_a[k] = xa
        out_b[k] = xb
        sa += xa
        sb += xb
    return sa, sb


def momentum_kernel(
    u, v, p_b, pfirst, kun, kvn, kux, kvx, du, dv, kus, kvs, rwn, ren, re, rnorth, rsouth, rown, corner,
    us_b, vs_b, fx, fy, su, sv, pke, vrow,
    cc, hh, srcu, srcv, gu, gv, ums, vms,
):
    step = pl.program_id(0)
    last = step == NB
    us, vs, p = us_b.at[0], vs_b.at[0], p_b.at[0]
    row = iota(ROW, 0)
    rowx = iota(WIDE, 0)
    lane = iota(TILE, 1)
    kxn, kyn = kun[:], kvn[:]
    rwv, rev = rwn[:], ren[:]

    def halos(k):
        hu = jnp.where(lane == 0, lane_to(rev, k, 0), lane_to(rwv, k, LN - 1))
        hv = jnp.where(lane == 0, lane_to(rev, NL + k, 0), lane_to(rwv, NL + k, LN - 1))
        return hu, hv

    def masked(k, uk, vk, halo):
        um = only(k < kxn, jnp.concatenate([uk, halo[0]], axis=1))
        return um, only(k < kyn, jnp.concatenate([vk, halo[1]], axis=1))

    @pl.when(step == 0)
    def _():
        for k in range(NL):
            ums[k], vms[k] = masked(k, u[k], v[k], halos(k))
        lev = iota((LP, NC), 0).astype(F32)
        lev1 = iota((LP, LN), 0)
        ks, kw = kus[7:8, :NC], kvs[7:8, :NC]
        s_u = only(lev < ks, rsouth[0])
        s_v = only(lev < kw, rsouth[1])
        pick = only(iota((LP, LN), 1) == lev1 + NL, corner[7:8, :])
        edge = jnp.sum(pick, axis=1, keepdims=True)
        edge = only(lev[:, :1] < kvs[7:8, NC : NC + 1], edge)
        s_ve = jnp.where(iota((LP, NC), 1) == NC - 1, edge, from_east(s_v))
        u_0 = only(lev < kxn[0:1, :NC], rown[0])
        v_0 = only(lev < kyn[0:1, :NC], rown[1])
        c_s = 0.25 * ((s_v + s_ve) * (s_u + u_0))
        h_s = s_v + v_0
        h_s = 0.25 * (h_s * h_s) + rown[2]
        for k in range(NL):
            cc[k, 7:8, :] = c_s[k : k + 1, :]
            hh[k, 7:8, :] = h_s[k : k + 1, :]

    @pl.when(step > 0)
    def _():
        kx, ky = kux[:], kvx[:]
        pev = re[:]
        total = [jnp.zeros(ROW, F32)] * 2

        def edge(k):
            return halos(k) + (lane_to(pev, 2 * NL + k, 0),)

        def shift(k, halo):
            um, vm = ums[k], vms[k]
            uk = jnp.where(last, rnorth[0, k : k + 1, :], u[k])
            vk = jnp.where(last, rnorth[1, k : k + 1, :], v[k])
            pe = jnp.concatenate([p[k], halo[2]], axis=1)
            return masked(k, uk, vk, halo), pe, from_west(um), from_east(vm)

        def flux(k, arg):
            new, pe, u_w, v_e = arg
            um, vm = ums[k], vms[k]
            c = 0.25 * ((vm + v_e) * (um + up_row(um, new[0], rowx)))
            g = u_w + um
            g = 0.25 * (g * g) + pe
            c5 = c[:, :NC]
            return new, from_east(g)[:, :NC] - g[:, :NC], c5, c5 - from_west(c)[:, :NC]

        def tend(k, arg):
            new, dx, c5, dc = arg
            u5, v5, pk = ums[k, :, :NC], vms[k, :, :NC], p[k]
            north = jnp.where(last, rnorth[2, k : k + 1, :], pfirst[0, 2, k : k + 1, :])
            h = v5 + up_row(v5, new[1][:, :NC], row)
            h = 0.25 * (h * h) + up_row(pk, north, row)
            tu = only(k < kx, dx + (c5 - down_row(c5, cc[k], row)))
            tv = only(k < ky, (h - down_row(h, hh[k], row)) + dc)
            total[0] += tu
            total[1] += tv
            srcu[k] = u5 - DT * tu
            srcv[k] = v5 - DT * tv
            cc[k] = c5
            hh[k] = h
            ums[k], vms[k] = new

        skewed((edge, shift, flux, tend), GROUP)
        dzu, dzv = du[:], dv[:]
        fx[:] = -dzu * total[0]
        fy[:] = -dzv * total[1]
        sa, sb = solve_pair(srcu, srcv, couple(kx, dzu, KV), couple(ky, dzv, KV), kx, ky, us, vs, gu, gv)
        sa, sb = dzu * sa, dzv * sb
        su[:] = sa
        sv[:] = sb
        ae = jnp.zeros(TILE, F32)
        for k in range(NL):
            ae = jnp.where(lane == k, lane_to(us[k, :, NC - LN :], LN - 1, k), ae)
        pke[:] = jnp.where(lane == 3 * NL, lane_to(sa[:, NC - LN :], LN - 1, 3 * NL), ae)

        @pl.when(last)
        def _():
            for k in range(NL):
                vrow[k : k + 1, :] = vs[k, 7:8, :]
            vrow[NL : NL + 1, :] = sb[7:8, :]
            vrow[NL + 1 : LP, :] = jnp.zeros((LP - NL - 1, NC), F32)


def momentum(u, v, p, first, geo, rw, re, rnorth, rsouth, rown, corner):
    ku, kv, du, dv = geo

    def this(b):
        return jnp.maximum(b, 1) - 1

    def ahead(b):
        return jnp.minimum(b, NB - 1)

    cube = pl.BlockSpec(SLAB, lambda b: (0, ahead(b), 0))
    pack = block_major(this)
    near = pl.BlockSpec(ROW, lambda b: (HT + this(b), 0))
    widn = pl.BlockSpec(WIDE, lambda b: (HT + b, 0))
    wids = pl.BlockSpec(WIDE, lambda b: (HT - 1, 0))
    plane = pl.BlockSpec(ROW, lambda b: (this(b), 0))
    col = pl.BlockSpec(TILE, lambda b: (this(b), 0))
    colw = pl.BlockSpec(TILE, lambda b: (b, 0))
    cole = pl.BlockSpec(TILE, lambda b: (ahead(b), 0))
    flat = jax.ShapeDtypeStruct((NR, NC), F32)

    def rows(n):
        return pl.BlockSpec((n, LP, NC), lambda b: (0, 0, 0))

    return pl.pallas_call(
        momentum_kernel,
        grid=(NB + 1,),
        in_specs=[cube, cube, pack, first_rows(ahead), widn, widn, near, near, near, near, wids, wids, colw, cole, col, rows(3), rows(2), rows(3), pl.BlockSpec(TILE, lambda b: (0, 0))],
        out_specs=[pack, pack, plane, plane, plane, plane, col, pl.BlockSpec((LP, NC), lambda b: (0, 0))],
        out_shape=[PACK, PACK, flat, flat, flat, flat, jax.ShapeDtypeStruct((NR, LN), F32), jax.ShapeDtypeStruct((LP, NC), F32)],
        scratch_shapes=[VM(SLAB, F32)] * 6 + [VM((NL,) + WIDE, F32)] * 2,
        compiler_params=pltpu.CompilerParams(dimension_semantics=("arbitrary",)),
        cost_estimate=pl.CostEstimate(flops=2 * 10**8, bytes_accessed=64 * 10**6, transcendentals=0),
        name="momentum",
    )(u, v, p, first, ku, kv, ku, kv, du, dv, ku, kv, rw, re, re, rnorth, rsouth, rown, corner)


def subcycle_kernel(planes, ku, kv, du, dv, force, tide, eta_o, u_o, v_o, ub_o, vb_o, eta, tu, tv, cu, cv, fu, fv, ub, vb):
    nt = ET
    row = iota(WIDE, 0)
    zero = jnp.zeros(WIDE, F32)
    for i in range(nt):
        sl = tile_rows(i)
        kx, ky = ku[sl, :], kv[sl, :]
        eta[sl, :] = only(planes[0, sl, :] > 0, planes[2, sl, :])
        tu[sl, :] = only(kx > 0, planes[3, sl, :])
        tv[sl, :] = only(ky > 0, planes[4, sl, :])
        cu[sl, :] = DTB * (kx * du[sl, :])
        cv[sl, :] = DTB * (ky * dv[sl, :])
        fu[sl, :] = only(kx > 0, DTB * force[0, sl, :])
        fv[sl, :] = only(ky > 0, DTB * force[1, sl, :])
        ub[sl, :] = zero
        vb[sl, :] = zero
    norm = 6.0 / (SUB * (SUB + 1) * (SUB + 2))

    def stage(first, last, lo, hi):
        def step(n, _):
            tx, ty = tide[n, 0], tide[n, 1]
            w = norm * ((n + 1) * (SUB - n)).astype(F32)

            def west(i):
                return from_west(tu[tile_rows(i), :])

            def surface(i, u_w):
                sl = tile_rows(i)
                vn = tv[sl, :]
                south = tv[tile_rows(i - 1), :] if i else zero
                e = eta[sl, :] - DTB * ((tu[sl, :] - u_w) + (vn - down_row(vn, south, row)))
                eta[sl, :] = e
                return from_east(e)

            def update(i, e_e):
                sl = tile_rows(i)
                e = eta[sl, :]
                un = tu[sl, :] + (cu[sl, :] * (tx - (e_e - e)) + fu[sl, :])
                tu[sl, :] = un
                if lo_bar <= i < hi_bar:
                    ub[sl, :] = ub[sl, :] + w * un
                if i > lo:
                    north(i - 1, e, ty, w)

            skewed((lambda i: west(lo + i), lambda i, x: surface(lo + i, x), lambda i, x: update(lo + i, x)), TILES, hi - lo)
            north(hi - 1, eta[tile_rows(hi - 1), :], ty, w)
            return 0

        lax.fori_loop(first, last, step, 0)

    lo_bar, hi_bar = HT - 1, HT + NB

    def north(i, ahead, ty, w):
        sl = tile_rows(i)
        e = eta[sl, :]
        x = tv[sl, :] + (cv[sl, :] * (ty - (up_row(e, ahead, row) - e)) + fv[sl, :])
        tv[sl, :] = x
        if lo_bar <= i < hi_bar:
            vb[sl, :] = vb[sl, :] + w * x

    for s in range(0, SUB, 8):
        stage(s, min(s + 8, SUB), s // 8, nt - s // 8)
    eta_o[:] = eta[HR : HR + NR, :NC]
    u_o[:] = tu[HR : HR + NR, :NC]
    v_o[:] = tv[HR : HR + NR, :NC]
    ub_o[:] = ub[HR - 8 : HR + NR, :]
    vb_o[:] = vb[HR - 8 : HR + NR, :]


def subcycles(planes, geo, force, tide):
    flat = jax.ShapeDtypeStruct((NR, NC), F32)
    bar = jax.ShapeDtypeStruct((NR + 8, EC), F32)
    vm = pl.BlockSpec(memory_space=VM)
    return pl.pallas_call(
        subcycle_kernel,
        in_specs=[vm] * 6 + [pl.BlockSpec(memory_space=pltpu.SMEM)],
        out_specs=[vm] * 5,
        out_shape=[flat, flat, flat, bar, bar],
        scratch_shapes=[VM((ER, EC), F32)] * 9,
        cost_estimate=pl.CostEstimate(flops=10**8, bytes_accessed=10**6, transcendentals=0),
        name="subcycles",
    )(planes, *geo, force, tide)


def finish_kernel(
    us_b, vs_b, t_b, s_b, first, kc, ku, kv, du, dv, ub, vb, su, sv, kvs, dvs, vbs, rw, re, rnorth, rsouth, rown,
    uo, vo, to, so, ct, cs,
):
    us, vs, t, s = us_b.at[0], vs_b.at[0], t_b.at[0], s_b.at[0]
    b = pl.program_id(0)
    last = b == NB - 1
    row = iota(ROW, 0)
    lane = iota(TILE, 1)

    def correction(mean, total, k, dz):
        deep = k * dz
        return (mean - total) / jnp.where(deep > 0, deep, 1.0)

    @pl.when(b == 0)
    def _():
        lev = iota((LP, NC), 0).astype(F32)
        kx = kvs[7:8, :NC]
        cor = correction(vbs[7:8, :NC], rsouth[0, NL : NL + 1, :], kx, dvs[7:8, :NC])
        vel = 0.5 * DT * only(lev < kx, rsouth[0] + cor)
        ft = vel * (rsouth[1] + rown[0, 0])
        fs = vel * (rsouth[2] + rown[0, 1])
        for k in range(NL):
            ct[k, 7:8, :] = ft[k : k + 1, :]
            cs[k, 7:8, :] = fs[k : k + 1, :]

    kx, ky, cnt = ku[:], kv[:, :NC], kc[:]
    rwv, rev = rw[:], re[:]
    tot = jnp.concatenate([su[:], lane_to(rwv, 3 * NL, LN - 1)], axis=1)
    cx = correction(ub[:], tot, kx, du[:])
    cy = correction(vb[:, :NC], sv[:], ky, dv[:, :NC])
    fields = ((t, to, ct), (s, so, cs))

    def load(k):
        out = [lane_to(rwv, k, LN - 1)]
        for i in range(2):
            base = NL * (i + 1) + k
            out.append(jnp.where(lane == 0, lane_to(rev, base, 0), lane_to(rwv, base, LN - 1)))
        return out

    def east(k, halo):
        wide = [jnp.concatenate([f[0][k], h], axis=1) for f, h in zip(fields, halo[1:])]
        return halo[0], [x + from_east(x) for x in wide]

    def flux(k, arg):
        halo, sums = arg
        ue = only(k < kx, jnp.concatenate([us[k], halo], axis=1) + cx)
        uo[k] = ue[:, :NC]
        f = [(0.5 * DT) * ue * x for x in sums]
        return [(x - from_west(x))[:, :NC] for x in f]

    def store(k, div):
        ve = only(k < ky, vs[k] + cy)
        vo[k] = ve
        hy = (0.5 * DT) * ve
        for i, (x, out, carry) in enumerate(fields):
            own = x[k]
            north = jnp.where(last, rnorth[i, k : k + 1, :], first[0, i, k : k + 1, :])
            fy = hy * (own + up_row(own, north, row))
            new = own - (div[i] + (fy - down_row(fy, carry[k], row)))
            carry[k] = fy
            out[k] = only(k < cnt, new)

    skewed((load, east, flux, store), GROUP)


def finish(us, vs, tm, sm, first, kmt, geo, ub, vb, su, sv, rw, re, rnorth, rsouth):
    ku, kv, du, dv = geo
    cube = pl.BlockSpec(SLAB, lambda b: (0, b, 0))
    pack = block_major(lambda b: b)
    wide = pl.BlockSpec(WIDE, lambda b: (HT + b, 0))
    wids = pl.BlockSpec(WIDE, lambda b: (HT - 1, 0))
    bar = pl.BlockSpec(WIDE, lambda b: (b + 1, 0))
    bars = pl.BlockSpec(WIDE, lambda b: (0, 0))
    plane = pl.BlockSpec(ROW, lambda b: (b, 0))
    col = pl.BlockSpec(TILE, lambda b: (b, 0))
    big = jax.ShapeDtypeStruct((NL, NR, NC), F32)

    def rows(n):
        return pl.BlockSpec((n, LP, NC), lambda b: (0, 0, 0))

    return pl.pallas_call(
        finish_kernel,
        grid=(NB,),
        in_specs=[pack, pack, pack, pack, first_rows(lambda b: jnp.minimum(b + 1, NB - 1)), plane, wide, wide, wide, wide, bar, bar, plane, plane, wids, wids, bars, col, col, rows(3), rows(3), first_rows(lambda b: 0)],
        out_specs=[cube] * 4,
        out_shape=[big] * 4,
        scratch_shapes=[VM(SLAB, F32)] * 2,
        compiler_params=pltpu.CompilerParams(dimension_semantics=("arbitrary",)),
        cost_estimate=pl.CostEstimate(flops=10**8, bytes_accessed=80 * 10**6, transcendentals=0),
        name="finish",
    )(us, vs, tm, sm, first, kmt, ku, kv, du, dv, ub, vb, su, sv, kv, dv, vb, rw, re, rnorth, rsouth, first)


def solution(mesh):
    n_cols, n_rows = mesh.shape["col"], mesh.shape["row"]

    def send(x, drow, dcol):
        pairs = []
        for c in range(n_cols):
            for r in range(n_rows):
                if 0 <= r + drow < n_rows:
                    pairs.append((c * n_rows + r, ((c + dcol) % n_cols) * n_rows + r + drow))
        return lax.ppermute(x, ("col", "row"), pairs)

    def widen(x):
        lane = lax.broadcasted_iota(jnp.int32, (1, 1, 128), 2)
        east, west = send(x[..., :LN], 0, -1), send(x[..., NC - LN :], 0, 1)
        wide = jnp.concatenate([x, jnp.where(lane < 64, east, west)], axis=-1)
        north, south = send(wide[:, :HR], -1, 0), send(wide[:, NR - HR :], 1, 0)
        return jnp.concatenate([south, wide, north], axis=1)

    def local_step(u, v, t, s, eta, tu, tv, depth, kmt, tide):
        pke, pkw, prn, prs = edges(u, v, t, s, kmt, depth)
        planes = widen(jnp.stack([kmt.astype(F32), depth, eta, tu, tv]))
        rw, re = send(pke, 0, 1), send(pkw, 0, -1)
        rsouth, rnorth = send(prn, 1, 0), send(prs, -1, 0)
        nw = send(pke[:8], -1, 1)
        se = send(pkw[NR - 8 :], 1, -1)
        geo = geometry(planes)
        tm, sm, pr, tke, tkw, trn, first = tracers(t, s, kmt, depth)
        rw = jnp.concatenate([rw, nw], axis=0)
        us, vs, fx, fy, su, sv, uke, vrow = momentum(u, v, pr, first, geo, rw, re, rnorth, rsouth, prs, se)
        force = widen(jnp.stack([fx, fy]))
        fw, fe = send(tke + uke, 0, 1), send(tkw, 0, -1)
        fsouth, fnorth = send(jnp.concatenate([vrow[None], trn]), 1, 0), send(first[0], -1, 0)
        eta_n, u_n, v_n, ub, vb = subcycles(planes, geo, force, tide)
        uo, vo, to, so = finish(us, vs, tm, sm, first, kmt, geo, ub, vb, su, sv, fw, fe, fnorth, fsouth)
        return eta_n, u_n, v_n, uo, vo, to, so

    cube, plane = P(None, "row", "col"), P("row", "col")
    return jax.shard_map(
        local_step,
        mesh=mesh,
        in_specs=(cube,) * 4 + (plane,) * 5 + (P(None, None),),
        out_specs=(plane,) * 3 + (cube,) * 4,
        check_vma=False,
    )
```

```python
import functools

import jax
import jax.numpy as jnp
from jax import lax
from jax.experimental import pallas as pl
from jax.experimental.pallas import tpu as pltpu
from jax.sharding import PartitionSpec as P

NL = 41
NR = 96
NC = 512
LN = 128
LP = 48
HR = 40
ER = NR + 2 * HR
EC = NC + 128
NB = NR // 8
SUB = 36
GROUP = 2
HALF = 64
SIDES = (-1, 0, 1)
FIRST, LAST = slice(0, 1), slice(7, 8)
TILES = 3
DT = 4.0
DTB = DT / SUB
KV = 0.001
KT = 0.0005
F32 = jnp.float32
HT = HR // 8
ET = ER // 8
SLAB, ROW, WIDE, TILE = (NL, 8, NC), (8, NC), (8, EC), (8, LN)
VM = pltpu.VMEM


def only(mask, x):
    return jnp.where(mask, x, jnp.zeros_like(x))


def iota(shape, dim):
    return lax.broadcasted_iota(jnp.int32, shape, dim)


def whole(*shape):
    return pl.BlockSpec(shape, lambda *_: (0,) * len(shape))


def shape(*dims):
    return jax.ShapeDtypeStruct(dims, F32)


def one(k):
    return slice(k, k + 1)


def tile_rows(i):
    return slice(8 * i, 8 * (i + 1))


def from_west(x):
    return pltpu.roll(x, 1, axis=1)


def from_east(x):
    return pltpu.roll(x, x.shape[1] - 1, axis=1)


def lane_to(x, src, dst):
    shift = (dst - src) % LN
    return x if shift == 0 else pltpu.roll(x, shift, axis=1)


def up_row(x, nxt, row):
    return pltpu.roll(jnp.where(row == 0, nxt, x), 7, axis=0)


def down_row(x, prev, row):
    return pltpu.roll(jnp.where(row == 7, prev, x), 1, axis=0)


def skewed(stages, group, count=NL):
    blocks = [range(k, min(k + group, count)) for k in range(0, count, group)]
    held = {}
    for i in range(len(blocks) + len(stages) - 1):
        for n, stage in enumerate(stages):
            if 0 <= i - n < len(blocks):
                for k in blocks[i - n]:
                    held[k] = stage(k, held[k]) if n else stage(k)


def couple(count, thick, kappa):
    safe = jnp.where(count > 0, thick, 1.0)
    return DT * kappa / (safe * safe)


def pressure_step(t, s, wet, cum, thick):
    half = only(wet, 0.5 * (0.015 * (s - 1.0) - 0.02 * (t - 1.0)))
    mid = cum + half
    return thick * mid, mid + half


def edge_kernel(u0, u3, v0, v3, t0, s0, kc, hc, uf, vf, ul, vl, tf, sf, kr, hr, pke, pkw, rn, rs):
    b = pl.program_id(0)
    lane = iota(TILE, 1)
    cnt = kc[:]
    thick = hc[:] / jnp.maximum(cnt, 1).astype(F32)
    ae = jnp.zeros(TILE, F32)
    aw = jnp.zeros(TILE, F32)
    cum = jnp.zeros(TILE, F32)
    for k in range(NL):
        p, cum = pressure_step(t0[k], s0[k], k < cnt, cum, thick)
        ae = jnp.where(lane == k, lane_to(u3[k], LN - 1, k), ae)
        ae = jnp.where(lane == NL + k, lane_to(v3[k], LN - 1, NL + k), ae)
        aw = jnp.where(lane == k, lane_to(u0[k], 0, k), aw)
        aw = jnp.where(lane == NL + k, lane_to(v0[k], 0, NL + k), aw)
        aw = jnp.where(lane == 2 * NL + k, lane_to(p, 0, 2 * NL + k), aw)
    pke[:] = ae
    pkw[:] = aw

    @pl.when(b == 0)
    def _():
        count = kr[:]
        dz = hr[:] / jnp.maximum(count, 1).astype(F32)
        acc = jnp.zeros(ROW, F32)
        for k in range(NL):
            p, acc = pressure_step(tf[k], sf[k], k < count, acc, dz)
            rn[0, one(k), :] = ul[k, LAST, :]
            rn[1, one(k), :] = vl[k, LAST, :]
            rs[0, one(k), :] = uf[k, FIRST, :]
            rs[1, one(k), :] = vf[k, FIRST, :]
            rs[2, one(k), :] = p[FIRST, :]
        for i in range(3):
            rs[i, NL:LP, :] = jnp.zeros((LP - NL, NC), F32)
            if i < 2:
                rn[i, NL:LP, :] = jnp.zeros((LP - NL, NC), F32)


def edges(u, v, t, s, kmt, depth):
    def strip(j):
        return pl.BlockSpec((NL, 8, 128), lambda b: (0, b, j))

    def slab(i):
        return pl.BlockSpec(SLAB, lambda b: (0, i, 0))

    col = pl.BlockSpec(TILE, lambda b: (b, 0))
    row0 = pl.BlockSpec(ROW, lambda b: (0, 0))
    return pl.pallas_call(
        edge_kernel,
        grid=(NB,),
        in_specs=[strip(0), strip(3), strip(0), strip(3), strip(0), strip(0), col, col, slab(0), slab(0), slab(NB - 1), slab(NB - 1), slab(0), slab(0), row0, row0],
        out_specs=[col, col, pl.BlockSpec((2, LP, NC), lambda b: (0, 0, 0)), pl.BlockSpec((3, LP, NC), lambda b: (0, 0, 0))],
        out_shape=[
            jax.ShapeDtypeStruct((NR, LN), F32),
            jax.ShapeDtypeStruct((NR, LN), F32),
            jax.ShapeDtypeStruct((2, LP, NC), F32),
            jax.ShapeDtypeStruct((3, LP, NC), F32),
        ],
        name="edges",
    )(u, u, v, v, t, s, kmt, depth, u, v, u, v, t, s, kmt, depth)


def tracer_kernel(t, s, kc, hc, tm_b, sm_b, pr_b, pke, pkw, rn, rs_b, gains):
    b = pl.program_id(0)
    for half in range(2):
        sl = tile_rows(half)
        tm, sm, rs = tm_b.at[half], sm_b.at[half], rs_b.at[half]
        mix_tracers(t.at[:, sl, :], s.at[:, sl, :], kc[sl, :], hc[sl, :], tm, sm, pr_b.at[half], pke.at[sl, :], pkw.at[sl, :], rs, gains)

    @pl.when(b == NB // 2 - 1)
    def _():
        for k in range(NL):
            rn[0, one(k), :] = tm[k, LAST, :]
            rn[1, one(k), :] = sm[k, LAST, :]
        for i in range(2):
            rn[i, NL:LP, :] = jnp.zeros((LP - NL, NC), F32)


def mix_tracers(t, s, cnt, depth, tm, sm, pr, pke, pkw, rs, gains):
    lane = iota(TILE, 1)
    thick = depth / jnp.maximum(cnt, 1).astype(F32)
    c = couple(cnt, thick, KT)
    zero = jnp.zeros(ROW, F32)
    cum = lower = pt = ps = zero
    keep = zero
    for k in range(NL):
        wet = k < cnt
        tk, sk = t[k], s[k]
        p, cum = pressure_step(tk, sk, wet, cum, thick)
        pr[k] = p
        rs[2, one(k), :] = p[FIRST, :]
        upper = jnp.where(k + 1 < cnt, c, 0.0) if k + 1 < NL else zero
        top = 1.0 + lower * keep if k else jnp.ones_like(zero)
        inv = 1.0 / (top + upper)
        keep = top * inv
        gains[k] = upper * inv
        pt = (jnp.where(wet, tk, 0.0) + lower * pt) * inv
        ps = (jnp.where(wet, sk, 0.0) + lower * ps) * inv
        tm[k] = pt
        sm[k] = ps
        lower = upper
    ae = jnp.zeros(TILE, F32)
    aw = jnp.zeros(TILE, F32)
    bt = bs = zero
    for k in reversed(range(NL)):
        gain = gains[k]
        bt = tm[k] + gain * bt
        bs = sm[k] + gain * bs
        tm[k] = bt
        sm[k] = bs
        rs[0, one(k), :] = bt[FIRST, :]
        rs[1, one(k), :] = bs[FIRST, :]
        for x, base in ((bt, NL), (bs, 2 * NL)):
            ae = jnp.where(lane == base + k, lane_to(x[:, NC - LN :], LN - 1, base + k), ae)
            aw = jnp.where(lane == base + k, lane_to(x[:, :LN], 0, base + k), aw)
    pke[:] = ae
    pkw[:] = aw


PACK = jax.ShapeDtypeStruct((NB,) + SLAB, F32)


def block_major(f, n=1):
    return pl.BlockSpec((n,) + SLAB, lambda b: (f(b), 0, 0, 0))


def first_rows(f, n=1):
    return pl.BlockSpec((n, 3, LP, NC), lambda b: (f(b), 0, 0, 0))


def tracers(t, s, kmt, depth):
    cube = pl.BlockSpec((NL, 16, NC), lambda b: (0, b, 0))
    pack = block_major(lambda b: b, 2)
    plane = pl.BlockSpec((16, NC), lambda b: (b, 0))
    col = pl.BlockSpec((16, LN), lambda b: (b, 0))
    rows = pl.BlockSpec((2, LP, NC), lambda b: (0, 0, 0))
    return pl.pallas_call(
        tracer_kernel,
        grid=(NB // 2,),
        in_specs=[cube, cube, plane, plane],
        out_specs=[pack, pack, pack, col, col, rows, first_rows(lambda b: b, 2)],
        out_shape=[PACK, PACK, PACK] + [jax.ShapeDtypeStruct((NR, LN), F32)] * 2 + [jax.ShapeDtypeStruct((2, LP, NC), F32), jax.ShapeDtypeStruct((NB, 3, LP, NC), F32)],
        scratch_shapes=[VM(SLAB, F32)],
        name="tracers",
    )(t, s, kmt, depth)


class Exchange:
    def __init__(self, sizes, send_sem, recv_sem):
        self.rows, self.cols = sizes
        self.row, self.col = lax.axis_index("row"), lax.axis_index("col")
        self.sems = send_sem, recv_sem
        self.used = 0

    def inside(self, drow):
        return (self.row + drow >= 0) & (self.row + drow < self.rows)

    def at(self, drow, dcol):
        return {"row": self.row + drow, "col": lax.rem(self.col + dcol + self.cols, self.cols)}

    def when(self, drow, action):
        if drow:
            pl.when(self.inside(drow))(action)
        else:
            action()

    def barrier(self):
        ready = pltpu.get_barrier_semaphore()
        for drow in SIDES:
            for dcol in SIDES:
                if drow or dcol:
                    self.when(drow, functools.partial(pl.semaphore_signal, ready, device_id=self.at(drow, dcol), device_id_type=pl.DeviceIdType.MESH))
        per_row = len(SIDES)
        known = [self.inside(drow).astype(jnp.int32) for drow in SIDES if drow]
        pl.semaphore_wait(ready, per_row - 1 + per_row * sum(known))

    def clear(self, plan):
        for _, dst, drow, _ in plan:
            if drow:

                @pl.when(jnp.logical_not(self.inside(-drow)))
                def _():
                    dst[:] = jnp.zeros(dst.shape, F32)

    def start(self, plan):
        out = []
        for src, dst, drow, dcol in plan:
            copy = pltpu.make_async_remote_copy(
                src_ref=src,
                dst_ref=dst,
                send_sem=self.sems[0].at[self.used],
                recv_sem=self.sems[1].at[self.used],
                device_id=self.at(drow, dcol),
                device_id_type=pl.DeviceIdType.MESH,
            )
            self.used += 1
            self.when(drow, copy.start)
            out.append((copy, drow))
        return out

    def wait(self, copies):
        for copy, drow in copies:
            self.when(drow, copy.wait_send)
            self.when(-drow, copy.wait_recv)


def pack_strips(pairs, to_west, to_east):
    lane = iota(TILE, 1)
    first, last = slice(0, LN), slice(NC - LN, NC)

    def turn(n):
        q, sl = n // NB, tile_rows(n % NB)
        b = pairs[q][-1]
        return pltpu.roll(b[sl, first], HALF, axis=1), pltpu.roll(b[sl, last], HALF, axis=1)

    def store(n, turned):
        q, sl = n // NB, tile_rows(n % NB)
        a = pairs[q][0]
        to_west[q, sl, :] = jnp.where(lane < HALF, a[sl, first], turned[0])
        to_east[q, sl, :] = jnp.where(lane < HALF, turned[1], a[sl, last])

    skewed((turn, store), NB, NB * len(pairs))


def strip_plan(to_west, to_east, strips):
    top, bottom = pl.ds(NR - HR, HR), pl.ds(0, HR)
    return [
        (to_east, strips[0], 0, 1),
        (to_west, strips[1], 0, -1),
        (to_east.at[:, top], strips[2], 1, 1),
        (to_west.at[:, top], strips[3], 1, -1),
        (to_east.at[:, bottom], strips[4], -1, 1),
        (to_west.at[:, bottom], strips[5], -1, -1),
    ]


def row_plan(planes, south, north):
    plan = []
    for i, x in enumerate(planes):
        plan.append((x.at[pl.ds(NR - HR, HR), :], south.at[i], 1, 0))
        plan.append((x.at[pl.ds(0, HR), :], north.at[i], -1, 0))
    return plan


def strip_scratch(n):
    return [VM((n, NR, LN), F32)] * 4 + [VM((n, HR, LN), F32)] * 4


def side(i, own, south, north):
    if i < HT:
        return south, tile_rows(i)
    return (own, tile_rows(i - HT)) if i < HT + NB else (north, tile_rows(i - HT - NB))


def halo_pair(i, q, strips):
    (w, e), sl = side(i, strips[:2], strips[2:4], strips[4:])
    lane = iota(TILE, 1)
    w, e = w[q, sl, :], e[q, sl, :]
    return jnp.where(lane < HALF, e, w), pltpu.roll(jnp.where(lane < HALF, w, e), HALF, axis=1)


def gather_kernel(sizes, kmt, depth, eta, tu, tv, pke, pkw, prn, prs, rw, re, rsouth, rnorth, corner, ku, kv, du, dv, eta_o, tu_o, tv_o, kf, south, north, *rest):
    to_west, to_east, *strips, send_sem, recv_sem = rest
    net = Exchange(sizes, send_sem, recv_sem)
    kf[:] = kmt[:].astype(F32)
    planes = (kf, depth, eta, tu, tv)
    pack_strips((planes[:2], planes[2:4], planes[4:]), to_west, to_east)
    plan = [
        (pke, rw.at[pl.ds(0, NR), :], 0, 1),
        (pkw, re, 0, -1),
        (prn, rsouth, 1, 0),
        (prs, rnorth, -1, 0),
        (pke.at[pl.ds(0, 8), :], rw.at[pl.ds(NR, 8), :], -1, 1),
        (pkw.at[pl.ds(NR - 8, 8), :], corner, 1, -1),
    ]
    plan = strip_plan(to_west, to_east, strips) + plan + row_plan(planes, south, north)
    net.clear(plan)
    net.barrier()
    net.wait(net.start(plan))
    row = iota(WIDE, 0)

    def turn(i):
        return [halo_pair(i, q, strips) for q in range(3)]

    def build(i, halo):
        halo = [x for pair in halo for x in pair]
        vals = []
        for n in range(len(planes)):
            part, sl = side(i, planes[n], south.at[n], north.at[n])
            vals.append(jnp.concatenate([part[sl, :], halo[n]], axis=1))
        k, h = vals[:2]
        dz = h / jnp.maximum(k, 1.0)
        kv[tile_rows(i), :] = k
        dv[tile_rows(i), :] = dz
        return vals[2:], from_east(k), from_east(dz)

    def store(i, arg):
        vals, ke, dze = arg
        sl = tile_rows(i)
        hi = tile_rows(min(i + 1, ET - 1))
        k, dz = kv[sl, :], dv[sl, :]
        k_u, k_v = jnp.minimum(k, ke), jnp.minimum(k, up_row(k, kv[hi, :], row))
        dv[sl, :] = 0.5 * (dz + up_row(dz, dv[hi, :], row))
        du[sl, :] = 0.5 * (dz + dze)
        ku[sl, :] = k_u
        kv[sl, :] = k_v
        for out, x, wet in zip((eta_o, tu_o, tv_o), vals, (k, k_u, k_v)):
            out[sl, :] = only(wet > 0, x)

    skewed((turn, build, store), TILES, ET)


def gather(sizes, *args):
    vm = pl.BlockSpec(memory_space=VM)
    outs = [shape(NR + 8, LN), shape(NR, LN), shape(2, LP, NC), shape(3, LP, NC), shape(8, LN)] + [shape(ER, EC)] * 7
    sems = [pltpu.SemaphoreType.DMA((6 + 6 + 10,))] * 2
    return pl.pallas_call(
        functools.partial(gather_kernel, sizes),
        in_specs=[vm] * len(args),
        out_specs=[vm] * len(outs),
        out_shape=outs,
        scratch_shapes=[VM((NR, NC), F32)] + [VM((5, HR, NC), F32)] * 2 + strip_scratch(3) + sems,
        compiler_params=pltpu.CompilerParams(collective_id=0, has_side_effects=True),
        name="gather",
    )(*args)


def solve_pair(src_a, src_b, ca, cb, na, nb, out_a, out_b, gain_a, gain_b):
    zero = jnp.zeros(ROW, F32)
    la = lb = pa = pb = wa = wb = zero
    for k in range(NL):
        ua = jnp.where(k + 1 < na, ca, 0.0) if k + 1 < NL else zero
        ub = jnp.where(k + 1 < nb, cb, 0.0) if k + 1 < NL else zero
        ta = 1.0 + la * wa if k else jnp.ones_like(zero)
        tb = 1.0 + lb * wb if k else jnp.ones_like(zero)
        ia = 1.0 / (ta + ua)
        ib = 1.0 / (tb + ub)
        wa, wb = ta * ia, tb * ib
        gain_a[k] = ua * ia
        gain_b[k] = ub * ib
        pa = (src_a[k] + la * pa) * ia
        pb = (src_b[k] + lb * pb) * ib
        src_a[k] = pa
        src_b[k] = pb
        la, lb = ua, ub
    xa = xb = sa = sb = zero
    for k in reversed(range(NL)):
        xa = src_a[k] + gain_a[k] * xa
        xb = src_b[k] + gain_b[k] * xb
        out_a[k] = xa
        out_b[k] = xb
        sa += xa
        sb += xb
    return sa, sb


def momentum_kernel(
    u, v, p_b, pfirst, kun, kvn, kux, kvx, du, dv, kus, kvs, rwn, ren, re, rnorth, rsouth, rown, corner,
    us_b, vs_b, fx, fy, su, sv, pke, vrow,
    cc, hh, srcu, srcv, gu, gv, ums, vms,
):
    step = pl.program_id(0)
    last = step == NB
    us, vs, p = us_b.at[0], vs_b.at[0], p_b.at[0]
    row = iota(ROW, 0)
    rowx = iota(WIDE, 0)
    lane = iota(TILE, 1)
    kxn, kyn = kun[:], kvn[:]
    rwv, rev = rwn[:], ren[:]

    def halos(k):
        hu = jnp.where(lane == 0, lane_to(rev, k, 0), lane_to(rwv, k, LN - 1))
        hv = jnp.where(lane == 0, lane_to(rev, NL + k, 0), lane_to(rwv, NL + k, LN - 1))
        return hu, hv

    def masked(k, uk, vk, halo):
        um = only(k < kxn, jnp.concatenate([uk, halo[0]], axis=1))
        return um, only(k < kyn, jnp.concatenate([vk, halo[1]], axis=1))

    @pl.when(step == 0)
    def _():
        for k in range(NL):
            ums[k], vms[k] = masked(k, u[k], v[k], halos(k))
        lev = iota((LP, NC), 0).astype(F32)
        lev1 = iota((LP, LN), 0)
        ks, kw = kus[LAST, :NC], kvs[LAST, :NC]
        s_u = only(lev < ks, rsouth[0])
        s_v = only(lev < kw, rsouth[1])
        pick = only(iota((LP, LN), 1) == lev1 + NL, corner[LAST, :])
        edge = jnp.sum(pick, axis=1, keepdims=True)
        edge = only(lev[:, :1] < kvs[LAST, one(NC)], edge)
        s_ve = jnp.where(iota((LP, NC), 1) == NC - 1, edge, from_east(s_v))
        u_0 = only(lev < kxn[FIRST, :NC], rown[0])
        v_0 = only(lev < kyn[FIRST, :NC], rown[1])
        c_s = 0.25 * ((s_v + s_ve) * (s_u + u_0))
        h_s = s_v + v_0
        h_s = 0.25 * (h_s * h_s) + rown[2]
        for k in range(NL):
            cc[k, LAST, :] = c_s[one(k), :]
            hh[k, LAST, :] = h_s[one(k), :]

    @pl.when(step > 0)
    def _():
        kx, ky = kux[:], kvx[:]
        pev = re[:]
        total = [jnp.zeros(ROW, F32)] * 2

        def edge(k):
            return halos(k) + (lane_to(pev, 2 * NL + k, 0),)

        def shift(k, halo):
            um, vm = ums[k], vms[k]
            uk = jnp.where(last, rnorth[0, one(k), :], u[k])
            vk = jnp.where(last, rnorth[1, one(k), :], v[k])
            pe = jnp.concatenate([p[k], halo[2]], axis=1)
            return masked(k, uk, vk, halo), pe, from_west(um), from_east(vm)

        def flux(k, arg):
            new, pe, u_w, v_e = arg
            um, vm = ums[k], vms[k]
            c = 0.25 * ((vm + v_e) * (um + up_row(um, new[0], rowx)))
            g = u_w + um
            g = 0.25 * (g * g) + pe
            c5 = c[:, :NC]
            return new, from_east(g)[:, :NC] - g[:, :NC], c5, c5 - from_west(c)[:, :NC]

        def tend(k, arg):
            new, dx, c5, dc = arg
            u5, v5, pk = ums[k, :, :NC], vms[k, :, :NC], p[k]
            north = jnp.where(last, rnorth[2, one(k), :], pfirst[0, 2, one(k), :])
            h = v5 + up_row(v5, new[1][:, :NC], row)
            h = 0.25 * (h * h) + up_row(pk, north, row)
            tu = only(k < kx, dx + (c5 - down_row(c5, cc[k], row)))
            tv = only(k < ky, (h - down_row(h, hh[k], row)) + dc)
            total[0] += tu
            total[1] += tv
            srcu[k] = u5 - DT * tu
            srcv[k] = v5 - DT * tv
            cc[k] = c5
            hh[k] = h
            ums[k], vms[k] = new

        skewed((edge, shift, flux, tend), GROUP)
        dzu, dzv = du[:], dv[:]
        fx[:] = -dzu * total[0]
        fy[:] = -dzv * total[1]
        sa, sb = solve_pair(srcu, srcv, couple(kx, dzu, KV), couple(ky, dzv, KV), kx, ky, us, vs, gu, gv)
        sa, sb = dzu * sa, dzv * sb
        su[:] = sa
        sv[:] = sb
        ae = jnp.zeros(TILE, F32)
        for k in range(NL):
            ae = jnp.where(lane == k, lane_to(us[k, :, NC - LN :], LN - 1, k), ae)
        pke[:] = jnp.where(lane == 3 * NL, lane_to(sa[:, NC - LN :], LN - 1, 3 * NL), ae)

        @pl.when(last)
        def _():
            for k in range(NL):
                vrow[one(k), :] = vs[k, LAST, :]
            vrow[one(NL), :] = sb[LAST, :]
            vrow[NL + 1 : LP, :] = jnp.zeros((LP - NL - 1, NC), F32)


def momentum(u, v, p, first, geo, rw, re, rnorth, rsouth, rown, corner):
    ku, kv, du, dv = geo

    def this(b):
        return jnp.maximum(b, 1) - 1

    def ahead(b):
        return jnp.minimum(b, NB - 1)

    cube = pl.BlockSpec(SLAB, lambda b: (0, ahead(b), 0))
    pack = block_major(this)
    near = pl.BlockSpec(ROW, lambda b: (HT + this(b), 0))
    widn = pl.BlockSpec(WIDE, lambda b: (HT + b, 0))
    wids = pl.BlockSpec(WIDE, lambda b: (HT - 1, 0))
    plane = pl.BlockSpec(ROW, lambda b: (this(b), 0))
    col = pl.BlockSpec(TILE, lambda b: (this(b), 0))
    colw = pl.BlockSpec(TILE, lambda b: (b, 0))
    cole = pl.BlockSpec(TILE, lambda b: (ahead(b), 0))
    flat = jax.ShapeDtypeStruct((NR, NC), F32)

    def rows(n):
        return pl.BlockSpec((n, LP, NC), lambda b: (0, 0, 0))

    return pl.pallas_call(
        momentum_kernel,
        grid=(NB + 1,),
        in_specs=[cube, cube, pack, first_rows(ahead), widn, widn, near, near, near, near, wids, wids, colw, cole, col, rows(3), rows(2), rows(3), pl.BlockSpec(TILE, lambda b: (0, 0))],
        out_specs=[pack, pack, plane, plane, plane, plane, col, pl.BlockSpec((LP, NC), lambda b: (0, 0))],
        out_shape=[PACK, PACK, flat, flat, flat, flat, jax.ShapeDtypeStruct((NR, LN), F32), jax.ShapeDtypeStruct((LP, NC), F32)],
        scratch_shapes=[VM(SLAB, F32)] * 6 + [VM((NL,) + WIDE, F32)] * 2,
        name="momentum",
    )(u, v, p, first, ku, kv, ku, kv, du, dv, ku, kv, rw, re, re, rnorth, rsouth, rown, corner)


def subcycle_kernel(
    sizes, eta_i, tu_i, tv_i, ku, kv, du, dv, fx, fy, tide, uke, tke, tkw, vrow, trn, trs,
    eta_o, u_o, v_o, ub_o, vb_o, fw, fe, fsouth, fnorth,
    eta, tu, tv, cu, cv, fu, fv, ub, vb, edge, south, north, *rest,
):
    to_west, to_east, *strips, send_sem, recv_sem = rest
    net = Exchange(sizes, send_sem, recv_sem)
    edge[:] = uke[:] + tke[:]
    pack_strips(((fx, fy),), to_west, to_east)
    plan = strip_plan(to_west, to_east, strips) + row_plan((fx, fy), south, north)
    late = [
        (edge, fw, 0, 1),
        (tkw, fe, 0, -1),
        (vrow, fsouth.at[0], 1, 0),
        (trn, fsouth.at[pl.ds(1, 2)], 1, 0),
        (trs.at[0], fnorth, -1, 0),
    ]
    net.clear(plan + late)
    net.barrier()
    plan, late = net.start(plan), net.start(late)
    row = iota(WIDE, 0)
    zero = jnp.zeros(WIDE, F32)
    ub[:] = jnp.zeros(ub.shape, F32)
    vb[:] = jnp.zeros(vb.shape, F32)
    eta[:] = eta_i[:]
    tu[:] = tu_i[:]
    tv[:] = tv_i[:]
    cu[:] = DTB * (ku[:] * du[:])
    cv[:] = DTB * (kv[:] * dv[:])
    net.wait(plan)

    def turn(i):
        return halo_pair(i, 0, strips)

    def build(i, halo):
        sl = tile_rows(i)
        for n, (x, out, wet) in enumerate(((fx, fu, ku), (fy, fv, kv))):
            part, rows = side(i, x, south.at[n], north.at[n])
            out[sl, :] = only(wet[sl, :] > 0, DTB * jnp.concatenate([part[rows, :], halo[n]], axis=1))

    skewed((turn, build), TILES, ET)
    norm = 6.0 / (SUB * (SUB + 1) * (SUB + 2))

    def stage(first, last, lo, hi):
        def step(n, _):
            tx, ty = tide[n, 0], tide[n, 1]
            w = norm * ((n + 1) * (SUB - n)).astype(F32)

            def west(i):
                return from_west(tu[tile_rows(i), :])

            def surface(i, u_w):
                sl = tile_rows(i)
                vn = tv[sl, :]
                south = tv[tile_rows(i - 1), :] if i else zero
                e = eta[sl, :] - DTB * ((tu[sl, :] - u_w) + (vn - down_row(vn, south, row)))
                eta[sl, :] = e
                return from_east(e)

            def update(i, e_e):
                sl = tile_rows(i)
                e = eta[sl, :]
                un = tu[sl, :] + (cu[sl, :] * (tx - (e_e - e)) + fu[sl, :])
                tu[sl, :] = un
                if lo_bar <= i < hi_bar:
                    ub[sl, :] = ub[sl, :] + w * un
                if i > lo:
                    north(i - 1, e, ty, w)

            skewed((lambda i: west(lo + i), lambda i, x: surface(lo + i, x), lambda i, x: update(lo + i, x)), TILES, hi - lo)
            north(hi - 1, eta[tile_rows(hi - 1), :], ty, w)
            return 0

        lax.fori_loop(first, last, step, 0)

    lo_bar, hi_bar = HT - 1, HT + NB

    def north(i, ahead, ty, w):
        sl = tile_rows(i)
        e = eta[sl, :]
        x = tv[sl, :] + (cv[sl, :] * (ty - (up_row(e, ahead, row) - e)) + fv[sl, :])
        tv[sl, :] = x
        if lo_bar <= i < hi_bar:
            vb[sl, :] = vb[sl, :] + w * x

    for s in range(0, SUB, 8):
        stage(s, min(s + 8, SUB), s // 8, ET - s // 8)
    eta_o[:] = eta[HR : HR + NR, :NC]
    u_o[:] = tu[HR : HR + NR, :NC]
    v_o[:] = tv[HR : HR + NR, :NC]
    ub_o[:] = ub[HR - 8 : HR + NR, :]
    vb_o[:] = vb[HR - 8 : HR + NR, :]
    net.wait(late)


def subcycles(sizes, *args):
    vm = pl.BlockSpec(memory_space=VM)
    outs = [shape(NR, NC)] * 3 + [shape(NR + 8, EC)] * 2 + [shape(NR, LN)] * 2 + [shape(3, LP, NC)] * 2
    sems = [pltpu.SemaphoreType.DMA((6 + 4 + 5,))] * 2
    wide = [VM((ER, EC), F32)] * 9
    return pl.pallas_call(
        functools.partial(subcycle_kernel, sizes),
        in_specs=[vm] * 9 + [pl.BlockSpec(memory_space=pltpu.SMEM)] + [vm] * 5 + [pl.BlockSpec(memory_space=pl.ANY)],
        out_specs=[vm] * len(outs),
        out_shape=outs,
        scratch_shapes=wide + [VM((NR, LN), F32)] + [VM((2, HR, NC), F32)] * 2 + strip_scratch(1) + sems,
        compiler_params=pltpu.CompilerParams(collective_id=1, has_side_effects=True),
        name="subcycles",
    )(*args)


def finish_kernel(
    us_b, vs_b, t_b, s_b, first, kc, ku, kv, du, dv, ub, vb, su, sv, kvs, dvs, vbs, rw, re, rnorth, rsouth, rown,
    uo, vo, to, so, ct, cs,
):
    us, vs, t, s = us_b.at[0], vs_b.at[0], t_b.at[0], s_b.at[0]
    b = pl.program_id(0)
    last = b == NB - 1
    row = iota(ROW, 0)
    lane = iota(TILE, 1)

    def correction(mean, total, k, dz):
        deep = k * dz
        return (mean - total) / jnp.where(deep > 0, deep, 1.0)

    @pl.when(b == 0)
    def _():
        lev = iota((LP, NC), 0).astype(F32)
        kx = kvs[LAST, :NC]
        cor = correction(vbs[LAST, :NC], rsouth[0, one(NL), :], kx, dvs[LAST, :NC])
        vel = 0.5 * DT * only(lev < kx, rsouth[0] + cor)
        ft = vel * (rsouth[1] + rown[0, 0])
        fs = vel * (rsouth[2] + rown[0, 1])
        for k in range(NL):
            ct[k, LAST, :] = ft[one(k), :]
            cs[k, LAST, :] = fs[one(k), :]

    kx, ky, cnt = ku[:], kv[:, :NC], kc[:]
    rwv, rev = rw[:], re[:]
    tot = jnp.concatenate([su[:], lane_to(rwv, 3 * NL, LN - 1)], axis=1)
    cx = correction(ub[:], tot, kx, du[:])
    cy = correction(vb[:, :NC], sv[:], ky, dv[:, :NC])
    fields = ((t, to, ct), (s, so, cs))

    def load(k):
        out = [lane_to(rwv, k, LN - 1)]
        for i in range(2):
            base = NL * (i + 1) + k
            out.append(jnp.where(lane == 0, lane_to(rev, base, 0), lane_to(rwv, base, LN - 1)))
        return out

    def east(k, halo):
        wide = [jnp.concatenate([f[0][k], h], axis=1) for f, h in zip(fields, halo[1:])]
        return halo[0], [x + from_east(x) for x in wide]

    def flux(k, arg):
        halo, sums = arg
        ue = only(k < kx, jnp.concatenate([us[k], halo], axis=1) + cx)
        uo[k] = ue[:, :NC]
        f = [(0.5 * DT) * ue * x for x in sums]
        return [(x - from_west(x))[:, :NC] for x in f]

    def store(k, div):
        ve = only(k < ky, vs[k] + cy)
        vo[k] = ve
        hy = (0.5 * DT) * ve
        for i, (x, out, carry) in enumerate(fields):
            own = x[k]
            north = jnp.where(last, rnorth[i, one(k), :], first[0, i, one(k), :])
            fy = hy * (own + up_row(own, north, row))
            new = own - (div[i] + (fy - down_row(fy, carry[k], row)))
            carry[k] = fy
            out[k] = only(k < cnt, new)

    skewed((load, east, flux, store), GROUP)


def finish(us, vs, tm, sm, first, kmt, geo, ub, vb, su, sv, rw, re, rnorth, rsouth):
    ku, kv, du, dv = geo
    cube = pl.BlockSpec(SLAB, lambda b: (0, b, 0))
    pack = block_major(lambda b: b)
    wide = pl.BlockSpec(WIDE, lambda b: (HT + b, 0))
    wids = pl.BlockSpec(WIDE, lambda b: (HT - 1, 0))
    bar = pl.BlockSpec(WIDE, lambda b: (b + 1, 0))
    bars = pl.BlockSpec(WIDE, lambda b: (0, 0))
    plane = pl.BlockSpec(ROW, lambda b: (b, 0))
    col = pl.BlockSpec(TILE, lambda b: (b, 0))
    big = jax.ShapeDtypeStruct((NL, NR, NC), F32)

    def rows(n):
        return pl.BlockSpec((n, LP, NC), lambda b: (0, 0, 0))

    return pl.pallas_call(
        finish_kernel,
        grid=(NB,),
        in_specs=[pack, pack, pack, pack, first_rows(lambda b: jnp.minimum(b + 1, NB - 1)), plane, wide, wide, wide, wide, bar, bar, plane, plane, wids, wids, bars, col, col, rows(3), rows(3), first_rows(lambda b: 0)],
        out_specs=[cube] * 4,
        out_shape=[big] * 4,
        scratch_shapes=[VM(SLAB, F32)] * 2,
        name="finish",
    )(us, vs, tm, sm, first, kmt, ku, kv, du, dv, ub, vb, su, sv, kv, dv, vb, rw, re, rnorth, rsouth, first)


def solution(mesh):
    sizes = mesh.shape["row"], mesh.shape["col"]

    def local_step(u, v, t, s, eta, tu, tv, depth, kmt, tide):
        pke, pkw, prn, prs = edges(u, v, t, s, kmt, depth)
        rw, re, rsouth, rnorth, corner, *wide = gather(sizes, kmt, depth, eta, tu, tv, pke, pkw, prn, prs)
        geo, state = wide[:4], wide[4:]
        tm, sm, pr, tke, tkw, trn, first = tracers(t, s, kmt, depth)
        us, vs, fx, fy, su, sv, uke, vrow = momentum(u, v, pr, first, geo, rw, re, rnorth, rsouth, prs, corner)
        eta_n, u_n, v_n, ub, vb, fw, fe, fsouth, fnorth = subcycles(sizes, *state, *geo, fx, fy, tide, uke, tke, tkw, vrow, trn, first)
        uo, vo, to, so = finish(us, vs, tm, sm, first, kmt, geo, ub, vb, su, sv, fw, fe, fnorth, fsouth)
        return eta_n, u_n, v_n, uo, vo, to, so

    cube, plane = P(None, "row", "col"), P("row", "col")
    return jax.shard_map(
        local_step,
        mesh=mesh,
        in_specs=(cube,) * 4 + (plane,) * 5 + (P(None, None),),
        out_specs=(plane,) * 3 + (cube,) * 4,
        check_vma=False,
    )
```

```python
import functools

import jax
import jax.numpy as jnp
from jax import lax
from jax.experimental import pallas as pl
from jax.experimental.pallas import tpu as pltpu
from jax.sharding import PartitionSpec as P

NL = 41
NR = 96
NC = 512
LN = 128
LP = 48
HR = 40
ER = NR + 2 * HR
EC = NC + 128
NB = NR // 8
SUB = 36
GROUP = 2
HALF = 64
SIDES = (-1, 0, 1)
FIRST, LAST = slice(0, 1), slice(7, 8)
TILES = 3
DT = 4.0
DTB = DT / SUB
KV = 0.001
KT = 0.0005
F32 = jnp.float32
HT = HR // 8
ET = ER // 8
SLAB, ROW, WIDE, TILE = (NL, 8, NC), (8, NC), (8, EC), (8, LN)
VM = pltpu.VMEM


def only(mask, x):
    return jnp.where(mask, x, jnp.zeros_like(x))


def iota(shape, dim):
    return lax.broadcasted_iota(jnp.int32, shape, dim)


def whole(*shape):
    return pl.BlockSpec(shape, lambda *_: (0,) * len(shape))


def shape(*dims):
    return jax.ShapeDtypeStruct(dims, F32)


def one(k):
    return slice(k, k + 1)


def tile_rows(i):
    return slice(8 * i, 8 * (i + 1))


def from_west(x):
    return pltpu.roll(x, 1, axis=1)


def from_east(x):
    return pltpu.roll(x, x.shape[1] - 1, axis=1)


def lane_to(x, src, dst):
    shift = (dst - src) % LN
    return x if shift == 0 else pltpu.roll(x, shift, axis=1)


def up_row(x, nxt, row):
    return pltpu.roll(jnp.where(row == 0, nxt, x), 7, axis=0)


def down_row(x, prev, row):
    return pltpu.roll(jnp.where(row == 7, prev, x), 1, axis=0)


def skewed(stages, group, count=NL):
    blocks = [range(k, min(k + group, count)) for k in range(0, count, group)]
    held = {}
    for i in range(len(blocks) + len(stages) - 1):
        for n, stage in enumerate(stages):
            if 0 <= i - n < len(blocks):
                for k in blocks[i - n]:
                    held[k] = stage(k, held[k]) if n else stage(k)


def couple(count, thick, kappa):
    safe = jnp.where(count > 0, thick, 1.0)
    return DT * kappa / (safe * safe)


def pressure_step(t, s, wet, cum, thick):
    half = only(wet, 0.5 * (0.015 * (s - 1.0) - 0.02 * (t - 1.0)))
    mid = cum + half
    return thick * mid, mid + half


class Exchange:
    def __init__(self, sizes, send_sem, recv_sem):
        self.rows, self.cols = sizes
        self.row, self.col = lax.axis_index("row"), lax.axis_index("col")
        self.sems = send_sem, recv_sem
        self.used = 0

    def inside(self, drow):
        return (self.row + drow >= 0) & (self.row + drow < self.rows)

    def at(self, drow, dcol):
        return {"row": self.row + drow, "col": lax.rem(self.col + dcol + self.cols, self.cols)}

    def when(self, drow, action):
        if drow:
            pl.when(self.inside(drow))(action)
        else:
            action()

    def barrier(self):
        ready = pltpu.get_barrier_semaphore()
        for drow in SIDES:
            for dcol in SIDES:
                if drow or dcol:
                    self.when(drow, functools.partial(pl.semaphore_signal, ready, device_id=self.at(drow, dcol), device_id_type=pl.DeviceIdType.MESH))
        per_row = len(SIDES)
        known = [self.inside(drow).astype(jnp.int32) for drow in SIDES if drow]
        pl.semaphore_wait(ready, per_row - 1 + per_row * sum(known))

    def clear(self, plan):
        for _, dst, drow, _ in plan:
            if drow:

                @pl.when(jnp.logical_not(self.inside(-drow)))
                def _():
                    dst[:] = jnp.zeros(dst.shape, F32)

    def make(self, plan):
        out = []
        for src, dst, drow, dcol in plan:
            copy = pltpu.make_async_remote_copy(
                src_ref=src,
                dst_ref=dst,
                send_sem=self.sems[0].at[self.used],
                recv_sem=self.sems[1].at[self.used],
                device_id=self.at(drow, dcol),
                device_id_type=pl.DeviceIdType.MESH,
            )
            self.used += 1
            out.append((copy, drow))
        return out

    def start(self, copies):
        for copy, drow in copies:
            self.when(drow, copy.start)

    def wait(self, copies):
        for copy, drow in copies:
            self.when(drow, copy.wait_send)
            self.when(-drow, copy.wait_recv)


def pack_strips(pairs, to_west, to_east):
    lane = iota(TILE, 1)
    first, last = slice(0, LN), slice(NC - LN, NC)

    def turn(n):
        q, sl = n // NB, tile_rows(n % NB)
        b = pairs[q][-1]
        return pltpu.roll(b[sl, first], HALF, axis=1), pltpu.roll(b[sl, last], HALF, axis=1)

    def store(n, turned):
        q, sl = n // NB, tile_rows(n % NB)
        a = pairs[q][0]
        to_west[q, sl, :] = jnp.where(lane < HALF, a[sl, first], turned[0])
        to_east[q, sl, :] = jnp.where(lane < HALF, turned[1], a[sl, last])

    skewed((turn, store), NB, NB * len(pairs))


def strip_plan(to_west, to_east, strips):
    top, bottom = pl.ds(NR - HR, HR), pl.ds(0, HR)
    return [
        (to_east, strips[0], 0, 1),
        (to_west, strips[1], 0, -1),
        (to_east.at[:, top], strips[2], 1, 1),
        (to_west.at[:, top], strips[3], 1, -1),
        (to_east.at[:, bottom], strips[4], -1, 1),
        (to_west.at[:, bottom], strips[5], -1, -1),
    ]


def row_plan(planes, south, north):
    plan = []
    for i, x in enumerate(planes):
        plan.append((x.at[pl.ds(NR - HR, HR), :], south.at[i], 1, 0))
        plan.append((x.at[pl.ds(0, HR), :], north.at[i], -1, 0))
    return plan


def strip_scratch(n):
    return [VM((n, NR, LN), F32)] * 4 + [VM((n, HR, LN), F32)] * 4


def side(i, own, south, north):
    if i < HT:
        return south, tile_rows(i)
    return (own, tile_rows(i - HT)) if i < HT + NB else (north, tile_rows(i - HT - NB))


def halo_pair(i, q, strips):
    (w, e), sl = side(i, strips[:2], strips[2:4], strips[4:])
    lane = iota(TILE, 1)
    w, e = w[q, sl, :], e[q, sl, :]
    return jnp.where(lane < HALF, e, w), pltpu.roll(jnp.where(lane < HALF, w, e), HALF, axis=1)


def mix_tracers(t, s, cnt, depth, strips, tm, sm, pr, pke, pkw, tke, tkw, rs, gains):
    lane = iota(TILE, 1)
    thick = depth / jnp.maximum(cnt, 1).astype(F32)
    c = couple(cnt, thick, KT)
    zero = jnp.zeros(ROW, F32)
    cum = lower = pt = ps = zero
    keep = zero
    ae = aw = jnp.zeros(TILE, F32)
    u0, u3, v0, v3 = strips
    for k in range(NL):
        wet = k < cnt
        tk, sk = t[k], s[k]
        p, cum = pressure_step(tk, sk, wet, cum, thick)
        pr[k] = p
        for n, (x0, x3) in enumerate(((u0, u3), (v0, v3))):
            base = NL * n + k
            ae = jnp.where(lane == base, lane_to(x3[k], LN - 1, base), ae)
            aw = jnp.where(lane == base, lane_to(x0[k], 0, base), aw)
        aw = jnp.where(lane == 2 * NL + k, lane_to(p[:, :LN], 0, 2 * NL + k), aw)
        rs[2, one(k), :] = p[FIRST, :]
        upper = jnp.where(k + 1 < cnt, c, 0.0) if k + 1 < NL else zero
        top = 1.0 + lower * keep if k else jnp.ones_like(zero)
        inv = 1.0 / (top + upper)
        keep = top * inv
        gains[k] = upper * inv
        pt = (jnp.where(wet, tk, 0.0) + lower * pt) * inv
        ps = (jnp.where(wet, sk, 0.0) + lower * ps) * inv
        tm[k] = pt
        sm[k] = ps
        lower = upper
    pke[:] = ae
    pkw[:] = aw
    ae = aw = jnp.zeros(TILE, F32)
    bt = bs = zero
    for k in reversed(range(NL)):
        gain = gains[k]
        bt = tm[k] + gain * bt
        bs = sm[k] + gain * bs
        tm[k] = bt
        sm[k] = bs
        rs[0, one(k), :] = bt[FIRST, :]
        rs[1, one(k), :] = bs[FIRST, :]
        for x, base in ((bt, NL), (bs, 2 * NL)):
            ae = jnp.where(lane == base + k, lane_to(x[:, NC - LN :], LN - 1, base + k), ae)
            aw = jnp.where(lane == base + k, lane_to(x[:, :LN], 0, base + k), aw)
    tke[:] = ae
    tkw[:] = aw


def wide_geometry(planes, strips, south, north, outs):
    ku, kv, du, dv, *state = outs
    row = iota(WIDE, 0)

    def turn(i):
        return [halo_pair(i, q, strips) for q in range(3)]

    def build(i, halo):
        halo = [x for pair in halo for x in pair]
        vals = []
        for n in range(len(planes)):
            part, sl = side(i, planes[n], south.at[n], north.at[n])
            vals.append(jnp.concatenate([part[sl, :], halo[n]], axis=1))
        k, h = vals[:2]
        dz = h / jnp.maximum(k, 1.0)
        kv[tile_rows(i), :] = k
        dv[tile_rows(i), :] = dz
        return vals[2:], from_east(k), from_east(dz)

    def store(i, arg):
        vals, ke, dze = arg
        sl = tile_rows(i)
        hi = tile_rows(min(i + 1, ET - 1))
        k, dz = kv[sl, :], dv[sl, :]
        k_u, k_v = jnp.minimum(k, ke), jnp.minimum(k, up_row(k, kv[hi, :], row))
        dv[sl, :] = 0.5 * (dz + up_row(dz, dv[hi, :], row))
        du[sl, :] = 0.5 * (dz + dze)
        ku[sl, :] = k_u
        kv[sl, :] = k_v
        for out, x, wet in zip(state, vals, (k, k_u, k_v)):
            out[sl, :] = only(wet > 0, x)

    skewed((turn, build, store), TILES, ET)


def tracer_kernel(sizes, t, s, u0, u3, v0, v3, kc, hc, uf, ul, vf, vl, kmt, depth, eta, tu, tv, *rest):
    tm_b, sm_b, pr_b, tke, tkw, rn, rs_b, *rest = rest
    received, rown, wide, rest = rest[:5], rest[5], rest[6:13], rest[13:]
    gains, kf, pke, pkw, prn, prs, south, north, rw, re, rsouth, rnorth, corner, to_west, to_east, *strips, send_sem, recv_sem = rest
    b = pl.program_id(0)
    last = NB // 2 - 1
    net = Exchange(sizes, send_sem, recv_sem)
    planes = (kf, depth, eta, tu, tv)
    head = strip_plan(to_west, to_east, strips) + [(prn, rsouth, 1, 0)] + row_plan(planes, south, north)
    middle = [(prs, rnorth, -1, 0), (pke.at[pl.ds(0, 8), :], rw.at[pl.ds(NR, 8), :], -1, 1)]
    tail = [(pkw.at[pl.ds(NR - 8, 8), :], corner, 1, -1)]

    def piece(i):
        part = pl.ds(16 * i, 16)
        return net.make([(pke.at[part, :], rw.at[part, :], 0, 1), (pkw.at[part, :], re.at[part, :], 0, -1)])

    first_plan = head + middle + tail
    head, middle, tail = net.make(head), net.make(middle), net.make(tail)
    pieces = [piece(i) for i in range(last + 1)]

    @pl.when(b == 0)
    def _():
        kf[:] = kmt[:].astype(F32)
        pack_strips((planes[:2], planes[2:4], planes[4:]), to_west, to_east)
        prn[:] = jnp.zeros(prn.shape, F32)
        prs[:] = jnp.zeros(prs.shape, F32)
        for k in range(NL):
            for n, (lo, hi) in enumerate(((uf, ul), (vf, vl))):
                prn[n, one(k), :] = hi[k, LAST, :]
                prs[n, one(k), :] = lo[k, FIRST, :]
        net.clear(first_plan)
        net.barrier()
        net.start(head)

    for i in range(last):

        @pl.when(b == i + 1)
        def _():
            net.start(pieces[i])

    for half in range(2):
        sl = tile_rows(half)
        tm, sm, rs = tm_b.at[half], sm_b.at[half], rs_b.at[half]
        out = pl.ds(pl.multiple_of(16 * b + 8 * half, 8), 8)
        parts = [x.at[:, sl, :] for x in (t, s, u0, u3, v0, v3)]
        mix_tracers(*parts[:2], kc[sl, :], hc[sl, :], parts[2:], tm, sm, pr_b.at[half], pke.at[out, :], pkw.at[out, :], tke.at[sl, :], tkw.at[sl, :], rs, gains)

    @pl.when(b == 0)
    def _():
        prs[2] = rs_b[0, 2]
        net.start(middle)

    @pl.when(b == last)
    def _():
        net.start(pieces[last] + tail)
        for k in range(NL):
            rn[0, one(k), :] = tm[k, LAST, :]
            rn[1, one(k), :] = sm[k, LAST, :]
        rown[:] = prs[:]
        net.wait(head)
        wide_geometry(planes, strips, south, north, wide)
        net.wait(middle + tail)
        for copies in pieces:
            net.wait(copies)
        for out, x in zip(received, (rw, re, rsouth, rnorth, corner)):
            out[:] = x[:]


PACK = shape(NB, *SLAB)


def block_major(f, n=1):
    return pl.BlockSpec((n,) + SLAB, lambda b: (f(b), 0, 0, 0))


def first_rows(f, n=1):
    return pl.BlockSpec((n, 3, LP, NC), lambda b: (f(b), 0, 0, 0))


def tracers(sizes, t, s, u, v, kmt, depth, eta, tu, tv):
    def cols(width, j):
        return pl.BlockSpec((NL, 16, width), lambda b: (0, b, j))

    def slab(i):
        return pl.BlockSpec(SLAB, lambda b: (0, i, 0))

    pack = block_major(lambda b: b, 2)
    plane = pl.BlockSpec((16, NC), lambda b: (b, 0))
    col = pl.BlockSpec((16, LN), lambda b: (b, 0))
    ends = [slab(0), slab(NB - 1)]
    edge = [(NR + 8, LN), (NR, LN), (2, LP, NC), (3, LP, NC), (8, LN)]
    extra = edge + [(3, LP, NC)] + [(ER, EC)] * 7
    sems = [pltpu.SemaphoreType.DMA((6 + 1 + 10 + 3 + NB,))] * 2
    rows = [VM((2, LP, NC), F32), VM((3, LP, NC), F32)] + [VM((5, HR, NC), F32)] * 2
    return pl.pallas_call(
        functools.partial(tracer_kernel, sizes),
        grid=(NB // 2,),
        in_specs=[cols(NC, 0)] * 2 + [cols(LN, 0), cols(LN, 3)] * 2 + [plane] * 2 + ends * 2 + [whole(NR, NC)] * 5,
        out_specs=[pack] * 3 + [col] * 2 + [whole(2, LP, NC), first_rows(lambda b: b, 2)] + [whole(*x) for x in extra],
        out_shape=[PACK] * 3 + [shape(NR, LN)] * 2 + [shape(2, LP, NC), shape(NB, 3, LP, NC)] + [shape(*x) for x in extra],
        scratch_shapes=[VM(SLAB, F32), VM((NR, NC), F32)] + [VM((NR, LN), F32)] * 2 + rows + [VM(x, F32) for x in edge] + strip_scratch(3) + sems,
        compiler_params=pltpu.CompilerParams(collective_id=0, has_side_effects=True),
        name="tracers",
    )(t, s, u, u, v, v, kmt, depth, u, u, v, v, kmt, depth, eta, tu, tv)


def solve_pair(src_a, src_b, ca, cb, na, nb, out_a, out_b, gain_a, gain_b):
    zero = jnp.zeros(ROW, F32)
    la = lb = pa = pb = wa = wb = zero
    for k in range(NL):
        ua = jnp.where(k + 1 < na, ca, 0.0) if k + 1 < NL else zero
        ub = jnp.where(k + 1 < nb, cb, 0.0) if k + 1 < NL else zero
        ta = 1.0 + la * wa if k else jnp.ones_like(zero)
        tb = 1.0 + lb * wb if k else jnp.ones_like(zero)
        ia = 1.0 / (ta + ua)
        ib = 1.0 / (tb + ub)
        wa, wb = ta * ia, tb * ib
        gain_a[k] = ua * ia
        gain_b[k] = ub * ib
        pa = (src_a[k] + la * pa) * ia
        pb = (src_b[k] + lb * pb) * ib
        src_a[k] = pa
        src_b[k] = pb
        la, lb = ua, ub
    xa = xb = sa = sb = zero
    for k in reversed(range(NL)):
        xa = src_a[k] + gain_a[k] * xa
        xb = src_b[k] + gain_b[k] * xb
        out_a[k] = xa
        out_b[k] = xb
        sa += xa
        sb += xb
    return sa, sb


def momentum_kernel(
    u, v, p_b, pfirst, kun, kvn, kux, kvx, du, dv, kus, kvs, rwn, ren, re, rnorth, rsouth, rown, corner,
    us_b, vs_b, fx, fy, su, sv, pke, vrow,
    cc, hh, srcu, srcv, gu, gv, ums, vms,
):
    step = pl.program_id(0)
    last = step == NB
    us, vs, p = us_b.at[0], vs_b.at[0], p_b.at[0]
    row = iota(ROW, 0)
    rowx = iota(WIDE, 0)
    lane = iota(TILE, 1)
    kxn, kyn = kun[:], kvn[:]
    rwv, rev = rwn[:], ren[:]

    def halos(k):
        hu = jnp.where(lane == 0, lane_to(rev, k, 0), lane_to(rwv, k, LN - 1))
        hv = jnp.where(lane == 0, lane_to(rev, NL + k, 0), lane_to(rwv, NL + k, LN - 1))
        return hu, hv

    def masked(k, uk, vk, halo):
        um = only(k < kxn, jnp.concatenate([uk, halo[0]], axis=1))
        return um, only(k < kyn, jnp.concatenate([vk, halo[1]], axis=1))

    @pl.when(step == 0)
    def _():
        for k in range(NL):
            ums[k], vms[k] = masked(k, u[k], v[k], halos(k))
        lev = iota((LP, NC), 0).astype(F32)
        lev1 = iota((LP, LN), 0)
        ks, kw = kus[LAST, :NC], kvs[LAST, :NC]
        s_u = only(lev < ks, rsouth[0])
        s_v = only(lev < kw, rsouth[1])
        pick = only(iota((LP, LN), 1) == lev1 + NL, corner[LAST, :])
        edge = jnp.sum(pick, axis=1, keepdims=True)
        edge = only(lev[:, :1] < kvs[LAST, one(NC)], edge)
        s_ve = jnp.where(iota((LP, NC), 1) == NC - 1, edge, from_east(s_v))
        u_0 = only(lev < kxn[FIRST, :NC], rown[0])
        v_0 = only(lev < kyn[FIRST, :NC], rown[1])
        c_s = 0.25 * ((s_v + s_ve) * (s_u + u_0))
        h_s = s_v + v_0
        h_s = 0.25 * (h_s * h_s) + rown[2]
        for k in range(NL):
            cc[k, LAST, :] = c_s[one(k), :]
            hh[k, LAST, :] = h_s[one(k), :]

    @pl.when(step > 0)
    def _():
        kx, ky = kux[:], kvx[:]
        pev = re[:]
        total = [jnp.zeros(ROW, F32)] * 2

        def edge(k):
            return halos(k) + (lane_to(pev, 2 * NL + k, 0),)

        def shift(k, halo):
            um, vm = ums[k], vms[k]
            uk = jnp.where(last, rnorth[0, one(k), :], u[k])
            vk = jnp.where(last, rnorth[1, one(k), :], v[k])
            pe = jnp.concatenate([p[k], halo[2]], axis=1)
            return masked(k, uk, vk, halo), pe, from_west(um), from_east(vm)

        def flux(k, arg):
            new, pe, u_w, v_e = arg
            um, vm = ums[k], vms[k]
            c = 0.25 * ((vm + v_e) * (um + up_row(um, new[0], rowx)))
            g = u_w + um
            g = 0.25 * (g * g) + pe
            c5 = c[:, :NC]
            return new, from_east(g)[:, :NC] - g[:, :NC], c5, c5 - from_west(c)[:, :NC]

        def tend(k, arg):
            new, dx, c5, dc = arg
            u5, v5, pk = ums[k, :, :NC], vms[k, :, :NC], p[k]
            north = jnp.where(last, rnorth[2, one(k), :], pfirst[0, 2, one(k), :])
            h = v5 + up_row(v5, new[1][:, :NC], row)
            h = 0.25 * (h * h) + up_row(pk, north, row)
            tu = only(k < kx, dx + (c5 - down_row(c5, cc[k], row)))
            tv = only(k < ky, (h - down_row(h, hh[k], row)) + dc)
            total[0] += tu
            total[1] += tv
            srcu[k] = u5 - DT * tu
            srcv[k] = v5 - DT * tv
            cc[k] = c5
            hh[k] = h
            ums[k], vms[k] = new

        skewed((edge, shift, flux, tend), GROUP)
        dzu, dzv = du[:], dv[:]
        fx[:] = -dzu * total[0]
        fy[:] = -dzv * total[1]
        sa, sb = solve_pair(srcu, srcv, couple(kx, dzu, KV), couple(ky, dzv, KV), kx, ky, us, vs, gu, gv)
        sa, sb = dzu * sa, dzv * sb
        su[:] = sa
        sv[:] = sb
        ae = jnp.zeros(TILE, F32)
        for k in range(NL):
            ae = jnp.where(lane == k, lane_to(us[k, :, NC - LN :], LN - 1, k), ae)
        pke[:] = jnp.where(lane == 3 * NL, lane_to(sa[:, NC - LN :], LN - 1, 3 * NL), ae)

        @pl.when(last)
        def _():
            for k in range(NL):
                vrow[one(k), :] = vs[k, LAST, :]
            vrow[one(NL), :] = sb[LAST, :]
            vrow[NL + 1 : LP, :] = jnp.zeros((LP - NL - 1, NC), F32)


def momentum(u, v, p, first, geo, rw, re, rnorth, rsouth, rown, corner):
    ku, kv, du, dv = geo

    def this(b):
        return jnp.maximum(b, 1) - 1

    def ahead(b):
        return jnp.minimum(b, NB - 1)

    cube = pl.BlockSpec(SLAB, lambda b: (0, ahead(b), 0))
    pack = block_major(this)
    near = pl.BlockSpec(ROW, lambda b: (HT + this(b), 0))
    widn = pl.BlockSpec(WIDE, lambda b: (HT + b, 0))
    wids = pl.BlockSpec(WIDE, lambda b: (HT - 1, 0))
    plane = pl.BlockSpec(ROW, lambda b: (this(b), 0))
    col = pl.BlockSpec(TILE, lambda b: (this(b), 0))
    colw = pl.BlockSpec(TILE, lambda b: (b, 0))
    cole = pl.BlockSpec(TILE, lambda b: (ahead(b), 0))
    flat = jax.ShapeDtypeStruct((NR, NC), F32)

    def rows(n):
        return pl.BlockSpec((n, LP, NC), lambda b: (0, 0, 0))

    return pl.pallas_call(
        momentum_kernel,
        grid=(NB + 1,),
        in_specs=[cube, cube, pack, first_rows(ahead), widn, widn, near, near, near, near, wids, wids, colw, cole, col, rows(3), rows(2), rows(3), pl.BlockSpec(TILE, lambda b: (0, 0))],
        out_specs=[pack, pack, plane, plane, plane, plane, col, pl.BlockSpec((LP, NC), lambda b: (0, 0))],
        out_shape=[PACK, PACK, flat, flat, flat, flat, jax.ShapeDtypeStruct((NR, LN), F32), jax.ShapeDtypeStruct((LP, NC), F32)],
        scratch_shapes=[VM(SLAB, F32)] * 6 + [VM((NL,) + WIDE, F32)] * 2,
        name="momentum",
    )(u, v, p, first, ku, kv, ku, kv, du, dv, ku, kv, rw, re, re, rnorth, rsouth, rown, corner)


def subcycle_kernel(
    sizes, eta_i, tu_i, tv_i, ku, kv, du, dv, fx, fy, tide, uke, tke, tkw, vrow, trn, trs,
    eta_o, u_o, v_o, ub_o, vb_o, fw, fe, fsouth, fnorth,
    eta, tu, tv, cu, cv, fu, fv, ub, vb, edge, south, north, *rest,
):
    to_west, to_east, *strips, send_sem, recv_sem = rest
    net = Exchange(sizes, send_sem, recv_sem)
    edge[:] = uke[:] + tke[:]
    pack_strips(((fx, fy),), to_west, to_east)
    plan = strip_plan(to_west, to_east, strips) + row_plan((fx, fy), south, north)
    late = [
        (edge, fw, 0, 1),
        (tkw, fe, 0, -1),
        (vrow, fsouth.at[0], 1, 0),
        (trn, fsouth.at[pl.ds(1, 2)], 1, 0),
        (trs.at[0], fnorth, -1, 0),
    ]
    net.clear(plan + late)
    net.barrier()
    plan, late = net.make(plan), net.make(late)
    net.start(plan + late)
    row = iota(WIDE, 0)
    zero = jnp.zeros(WIDE, F32)
    ub[:] = jnp.zeros(ub.shape, F32)
    vb[:] = jnp.zeros(vb.shape, F32)
    eta[:] = eta_i[:]
    tu[:] = tu_i[:]
    tv[:] = tv_i[:]
    cu[:] = DTB * (ku[:] * du[:])
    cv[:] = DTB * (kv[:] * dv[:])
    net.wait(plan)

    def turn(i):
        return halo_pair(i, 0, strips)

    def build(i, halo):
        sl = tile_rows(i)
        for n, (x, out, wet) in enumerate(((fx, fu, ku), (fy, fv, kv))):
            part, rows = side(i, x, south.at[n], north.at[n])
            out[sl, :] = only(wet[sl, :] > 0, DTB * jnp.concatenate([part[rows, :], halo[n]], axis=1))

    skewed((turn, build), TILES, ET)
    norm = 6.0 / (SUB * (SUB + 1) * (SUB + 2))

    def stage(first, last, lo, hi):
        def step(n, _):
            tx, ty = tide[n, 0], tide[n, 1]
            w = norm * ((n + 1) * (SUB - n)).astype(F32)

            def west(i):
                return from_west(tu[tile_rows(i), :])

            def surface(i, u_w):
                sl = tile_rows(i)
                vn = tv[sl, :]
                south = tv[tile_rows(i - 1), :] if i else zero
                e = eta[sl, :] - DTB * ((tu[sl, :] - u_w) + (vn - down_row(vn, south, row)))
                eta[sl, :] = e
                return from_east(e)

            def update(i, e_e):
                sl = tile_rows(i)
                e = eta[sl, :]
                un = tu[sl, :] + (cu[sl, :] * (tx - (e_e - e)) + fu[sl, :])
                tu[sl, :] = un
                if lo_bar <= i < hi_bar:
                    ub[sl, :] = ub[sl, :] + w * un
                if i > lo:
                    north(i - 1, e, ty, w)

            skewed((lambda i: west(lo + i), lambda i, x: surface(lo + i, x), lambda i, x: update(lo + i, x)), TILES, hi - lo)
            north(hi - 1, eta[tile_rows(hi - 1), :], ty, w)
            return 0

        lax.fori_loop(first, last, step, 0)

    lo_bar, hi_bar = HT - 1, HT + NB

    def north(i, ahead, ty, w):
        sl = tile_rows(i)
        e = eta[sl, :]
        x = tv[sl, :] + (cv[sl, :] * (ty - (up_row(e, ahead, row) - e)) + fv[sl, :])
        tv[sl, :] = x
        if lo_bar <= i < hi_bar:
            vb[sl, :] = vb[sl, :] + w * x

    for s in range(0, SUB, 8):
        stage(s, min(s + 8, SUB), s // 8, ET - s // 8)
    eta_o[:] = eta[HR : HR + NR, :NC]
    u_o[:] = tu[HR : HR + NR, :NC]
    v_o[:] = tv[HR : HR + NR, :NC]
    ub_o[:] = ub[HR - 8 : HR + NR, :]
    vb_o[:] = vb[HR - 8 : HR + NR, :]
    net.wait(late)


def subcycles(sizes, *args):
    vm = pl.BlockSpec(memory_space=VM)
    outs = [shape(NR, NC)] * 3 + [shape(NR + 8, EC)] * 2 + [shape(NR, LN)] * 2 + [shape(3, LP, NC)] * 2
    sems = [pltpu.SemaphoreType.DMA((6 + 4 + 5,))] * 2
    wide = [VM((ER, EC), F32)] * 9
    return pl.pallas_call(
        functools.partial(subcycle_kernel, sizes),
        in_specs=[vm] * 9 + [pl.BlockSpec(memory_space=pltpu.SMEM)] + [vm] * 5 + [pl.BlockSpec(memory_space=pl.ANY)],
        out_specs=[vm] * len(outs),
        out_shape=outs,
        scratch_shapes=wide + [VM((NR, LN), F32)] + [VM((2, HR, NC), F32)] * 2 + strip_scratch(1) + sems,
        compiler_params=pltpu.CompilerParams(collective_id=1, has_side_effects=True),
        name="subcycles",
    )(*args)


def finish_kernel(
    us_b, vs_b, t_b, s_b, first, kc, ku, kv, du, dv, ub, vb, su, sv, kvs, dvs, vbs, rw, re, rnorth, rsouth, rown,
    uo, vo, to, so, ct, cs,
):
    us, vs, t, s = us_b.at[0], vs_b.at[0], t_b.at[0], s_b.at[0]
    b = pl.program_id(0)
    last = b == NB - 1
    row = iota(ROW, 0)
    lane = iota(TILE, 1)

    def correction(mean, total, k, dz):
        deep = k * dz
        return (mean - total) / jnp.where(deep > 0, deep, 1.0)

    @pl.when(b == 0)
    def _():
        lev = iota((LP, NC), 0).astype(F32)
        kx = kvs[LAST, :NC]
        cor = correction(vbs[LAST, :NC], rsouth[0, one(NL), :], kx, dvs[LAST, :NC])
        vel = 0.5 * DT * only(lev < kx, rsouth[0] + cor)
        ft = vel * (rsouth[1] + rown[0, 0])
        fs = vel * (rsouth[2] + rown[0, 1])
        for k in range(NL):
            ct[k, LAST, :] = ft[one(k), :]
            cs[k, LAST, :] = fs[one(k), :]

    kx, ky, cnt = ku[:], kv[:, :NC], kc[:]
    rwv, rev = rw[:], re[:]
    tot = jnp.concatenate([su[:], lane_to(rwv, 3 * NL, LN - 1)], axis=1)
    cx = correction(ub[:], tot, kx, du[:])
    cy = correction(vb[:, :NC], sv[:], ky, dv[:, :NC])
    fields = ((t, to, ct), (s, so, cs))

    def load(k):
        out = [lane_to(rwv, k, LN - 1)]
        for i in range(2):
            base = NL * (i + 1) + k
            out.append(jnp.where(lane == 0, lane_to(rev, base, 0), lane_to(rwv, base, LN - 1)))
        return out

    def east(k, halo):
        wide = [jnp.concatenate([f[0][k], h], axis=1) for f, h in zip(fields, halo[1:])]
        return halo[0], [x + from_east(x) for x in wide]

    def flux(k, arg):
        halo, sums = arg
        ue = only(k < kx, jnp.concatenate([us[k], halo], axis=1) + cx)
        uo[k] = ue[:, :NC]
        f = [(0.5 * DT) * ue * x for x in sums]
        return [(x - from_west(x))[:, :NC] for x in f]

    def store(k, div):
        ve = only(k < ky, vs[k] + cy)
        vo[k] = ve
        hy = (0.5 * DT) * ve
        for i, (x, out, carry) in enumerate(fields):
            own = x[k]
            north = jnp.where(last, rnorth[i, one(k), :], first[0, i, one(k), :])
            fy = hy * (own + up_row(own, north, row))
            new = own - (div[i] + (fy - down_row(fy, carry[k], row)))
            carry[k] = fy
            out[k] = only(k < cnt, new)

    skewed((load, east, flux, store), GROUP)


def finish(us, vs, tm, sm, first, kmt, geo, ub, vb, su, sv, rw, re, rnorth, rsouth):
    ku, kv, du, dv = geo
    cube = pl.BlockSpec(SLAB, lambda b: (0, b, 0))
    pack = block_major(lambda b: b)
    wide = pl.BlockSpec(WIDE, lambda b: (HT + b, 0))
    wids = pl.BlockSpec(WIDE, lambda b: (HT - 1, 0))
    bar = pl.BlockSpec(WIDE, lambda b: (b + 1, 0))
    bars = pl.BlockSpec(WIDE, lambda b: (0, 0))
    plane = pl.BlockSpec(ROW, lambda b: (b, 0))
    col = pl.BlockSpec(TILE, lambda b: (b, 0))
    big = jax.ShapeDtypeStruct((NL, NR, NC), F32)

    def rows(n):
        return pl.BlockSpec((n, LP, NC), lambda b: (0, 0, 0))

    return pl.pallas_call(
        finish_kernel,
        grid=(NB,),
        in_specs=[pack, pack, pack, pack, first_rows(lambda b: jnp.minimum(b + 1, NB - 1)), plane, wide, wide, wide, wide, bar, bar, plane, plane, wids, wids, bars, col, col, rows(3), rows(3), first_rows(lambda b: 0)],
        out_specs=[cube] * 4,
        out_shape=[big] * 4,
        scratch_shapes=[VM(SLAB, F32)] * 2,
        name="finish",
    )(us, vs, tm, sm, first, kmt, ku, kv, du, dv, ub, vb, su, sv, kv, dv, vb, rw, re, rnorth, rsouth, first)


def solution(mesh):
    sizes = mesh.shape["row"], mesh.shape["col"]

    def local_step(u, v, t, s, eta, tu, tv, depth, kmt, tide):
        tm, sm, pr, tke, tkw, trn, first, rw, re, rsouth, rnorth, corner, rown, *wide = tracers(sizes, t, s, u, v, kmt, depth, eta, tu, tv)
        geo, state = wide[:4], wide[4:]
        us, vs, fx, fy, su, sv, uke, vrow = momentum(u, v, pr, first, geo, rw, re, rnorth, rsouth, rown, corner)
        eta_n, u_n, v_n, ub, vb, fw, fe, fsouth, fnorth = subcycles(sizes, *state, *geo, fx, fy, tide, uke, tke, tkw, vrow, trn, first)
        uo, vo, to, so = finish(us, vs, tm, sm, first, kmt, geo, ub, vb, su, sv, fw, fe, fnorth, fsouth)
        return eta_n, u_n, v_n, uo, vo, to, so

    cube, plane = P(None, "row", "col"), P("row", "col")
    return jax.shard_map(
        local_step,
        mesh=mesh,
        in_specs=(cube,) * 4 + (plane,) * 5 + (P(None, None),),
        out_specs=(plane,) * 3 + (cube,) * 4,
        check_vma=False,
    )
```

```python
import functools

import jax
import jax.numpy as jnp
from jax import lax
from jax.experimental import pallas as pl
from jax.experimental.pallas import tpu as pltpu
from jax.sharding import PartitionSpec as P

NL = 41
NR = 96
NC = 512
LN = 128
LP = 48
HR = 40
ER = NR + 2 * HR
EC = NC + 128
NB = NR // 8
SUB = 36
GROUP = 2
HALF = 64
SIDES = (-1, 0, 1)
FIRST, LAST = slice(0, 1), slice(7, 8)
TILES = 3
DT = 4.0
DTB = DT / SUB
KV = 0.001
KT = 0.0005
F32 = jnp.float32
HT = HR // 8
ET = ER // 8
SLAB, ROW, WIDE, TILE = (NL, 8, NC), (8, NC), (8, EC), (8, LN)
VM = pltpu.VMEM


def only(mask, x):
    return jnp.where(mask, x, jnp.zeros_like(x))


def iota(shape, dim):
    return lax.broadcasted_iota(jnp.int32, shape, dim)


def whole(*shape):
    return pl.BlockSpec(shape, lambda *_: (0,) * len(shape))


def shape(*dims):
    return jax.ShapeDtypeStruct(dims, F32)


def one(k):
    return slice(k, k + 1)


def tile_rows(i):
    return slice(8 * i, 8 * (i + 1))


def from_west(x):
    return pltpu.roll(x, 1, axis=1)


def from_east(x):
    return pltpu.roll(x, x.shape[1] - 1, axis=1)


def lane_to(x, src, dst):
    shift = (dst - src) % LN
    return x if shift == 0 else pltpu.roll(x, shift, axis=1)


def up_row(x, nxt, row):
    return pltpu.roll(jnp.where(row == 0, nxt, x), 7, axis=0)


def down_row(x, prev, row):
    return pltpu.roll(jnp.where(row == 7, prev, x), 1, axis=0)


def skewed(stages, group, count=NL):
    blocks = [range(k, min(k + group, count)) for k in range(0, count, group)]
    held = {}
    for i in range(len(blocks) + len(stages) - 1):
        for n, stage in enumerate(stages):
            if 0 <= i - n < len(blocks):
                for k in blocks[i - n]:
                    held[k] = stage(k, held[k]) if n else stage(k)


def couple(count, thick, kappa):
    safe = jnp.where(count > 0, thick, 1.0)
    return DT * kappa / (safe * safe)


def pressure_step(t, s, wet, cum, thick):
    half = only(wet, 0.5 * (0.015 * (s - 1.0) - 0.02 * (t - 1.0)))
    mid = cum + half
    return thick * mid, mid + half


class Exchange:
    def __init__(self, sizes, send_sem, recv_sem):
        self.rows, self.cols = sizes
        self.row, self.col = lax.axis_index("row"), lax.axis_index("col")
        self.sems = send_sem, recv_sem
        self.used = 0

    def inside(self, drow):
        return (self.row + drow >= 0) & (self.row + drow < self.rows)

    def at(self, drow, dcol):
        return {"row": self.row + drow, "col": lax.rem(self.col + dcol + self.cols, self.cols)}

    def when(self, drow, action):
        if drow:
            pl.when(self.inside(drow))(action)
        else:
            action()

    def barrier(self):
        ready = pltpu.get_barrier_semaphore()
        for drow in SIDES:
            for dcol in SIDES:
                if drow or dcol:
                    self.when(drow, functools.partial(pl.semaphore_signal, ready, device_id=self.at(drow, dcol), device_id_type=pl.DeviceIdType.MESH))
        per_row = len(SIDES)
        known = [self.inside(drow).astype(jnp.int32) for drow in SIDES if drow]
        pl.semaphore_wait(ready, per_row - 1 + per_row * sum(known))

    def clear(self, plan):
        for _, dst, drow, _ in plan:
            if drow:

                @pl.when(jnp.logical_not(self.inside(-drow)))
                def _():
                    dst[:] = jnp.zeros(dst.shape, F32)

    def make(self, plan):
        out = []
        for src, dst, drow, dcol in plan:
            copy = pltpu.make_async_remote_copy(
                src_ref=src,
                dst_ref=dst,
                send_sem=self.sems[0].at[self.used],
                recv_sem=self.sems[1].at[self.used],
                device_id=self.at(drow, dcol),
                device_id_type=pl.DeviceIdType.MESH,
            )
            self.used += 1
            out.append((copy, drow))
        return out

    def start(self, copies):
        for copy, drow in copies:
            self.when(drow, copy.start)

    def wait(self, copies):
        for copy, drow in copies:
            self.when(drow, copy.wait_send)
            self.when(-drow, copy.wait_recv)


def pack_strips(pairs, to_west, to_east):
    lane = iota(TILE, 1)
    first, last = slice(0, LN), slice(NC - LN, NC)

    def turn(n):
        q, sl = n // NB, tile_rows(n % NB)
        b = pairs[q][-1]
        return pltpu.roll(b[sl, first], HALF, axis=1), pltpu.roll(b[sl, last], HALF, axis=1)

    def store(n, turned):
        q, sl = n // NB, tile_rows(n % NB)
        a = pairs[q][0]
        to_west[q, sl, :] = jnp.where(lane < HALF, a[sl, first], turned[0])
        to_east[q, sl, :] = jnp.where(lane < HALF, turned[1], a[sl, last])

    skewed((turn, store), NB, NB * len(pairs))


def strip_plan(to_west, to_east, strips):
    top, bottom = pl.ds(NR - HR, HR), pl.ds(0, HR)
    return [
        (to_east, strips[0], 0, 1),
        (to_west, strips[1], 0, -1),
        (to_east.at[:, top], strips[2], 1, 1),
        (to_west.at[:, top], strips[3], 1, -1),
        (to_east.at[:, bottom], strips[4], -1, 1),
        (to_west.at[:, bottom], strips[5], -1, -1),
    ]


def row_plan(planes, south, north):
    plan = []
    for i, x in enumerate(planes):
        plan.append((x.at[pl.ds(NR - HR, HR), :], south.at[i], 1, 0))
        plan.append((x.at[pl.ds(0, HR), :], north.at[i], -1, 0))
    return plan


def strip_scratch(n):
    return [VM((n, NR, LN), F32)] * 4 + [VM((n, HR, LN), F32)] * 4


def side(i, own, south, north):
    if i < HT:
        return south, tile_rows(i)
    return (own, tile_rows(i - HT)) if i < HT + NB else (north, tile_rows(i - HT - NB))


def halo_pair(i, q, strips):
    (w, e), sl = side(i, strips[:2], strips[2:4], strips[4:])
    lane = iota(TILE, 1)
    w, e = w[q, sl, :], e[q, sl, :]
    return jnp.where(lane < HALF, e, w), pltpu.roll(jnp.where(lane < HALF, w, e), HALF, axis=1)


def mix_tracers(t, s, cnt, depth, strips, tm, sm, pr, pke, pkw, tke, tkw, rs, gains):
    lane = iota(TILE, 1)
    thick = depth / jnp.maximum(cnt, 1).astype(F32)
    c = couple(cnt, thick, KT)
    zero = jnp.zeros(ROW, F32)
    cum = lower = pt = ps = zero
    keep = zero
    ae = aw = jnp.zeros(TILE, F32)
    u0, u3, v0, v3 = strips
    for k in range(NL):
        wet = k < cnt
        tk, sk = t[k], s[k]
        p, cum = pressure_step(tk, sk, wet, cum, thick)
        pr[k] = p
        for n, (x0, x3) in enumerate(((u0, u3), (v0, v3))):
            base = NL * n + k
            ae = jnp.where(lane == base, lane_to(x3[k], LN - 1, base), ae)
            aw = jnp.where(lane == base, lane_to(x0[k], 0, base), aw)
        aw = jnp.where(lane == 2 * NL + k, lane_to(p[:, :LN], 0, 2 * NL + k), aw)
        rs[2, one(k), :] = p[FIRST, :]
        upper = jnp.where(k + 1 < cnt, c, 0.0) if k + 1 < NL else zero
        top = 1.0 + lower * keep if k else jnp.ones_like(zero)
        inv = 1.0 / (top + upper)
        keep = top * inv
        gains[k] = upper * inv
        pt = (jnp.where(wet, tk, 0.0) + lower * pt) * inv
        ps = (jnp.where(wet, sk, 0.0) + lower * ps) * inv
        tm[k] = pt
        sm[k] = ps
        lower = upper
    pke[:] = ae
    pkw[:] = aw
    ae = aw = jnp.zeros(TILE, F32)
    bt = bs = zero
    for k in reversed(range(NL)):
        gain = gains[k]
        bt = tm[k] + gain * bt
        bs = sm[k] + gain * bs
        tm[k] = bt
        sm[k] = bs
        rs[0, one(k), :] = bt[FIRST, :]
        rs[1, one(k), :] = bs[FIRST, :]
        for x, base in ((bt, NL), (bs, 2 * NL)):
            ae = jnp.where(lane == base + k, lane_to(x[:, NC - LN :], LN - 1, base + k), ae)
            aw = jnp.where(lane == base + k, lane_to(x[:, :LN], 0, base + k), aw)
    tke[:] = ae
    tkw[:] = aw


def wide_geometry(planes, strips, south, north, outs):
    ku, kv, du, dv, *state = outs
    row = iota(WIDE, 0)

    def turn(i):
        return [halo_pair(i, q, strips) for q in range(3)]

    def build(i, halo):
        halo = [x for pair in halo for x in pair]
        vals = []
        for n in range(len(planes)):
            part, sl = side(i, planes[n], south.at[n], north.at[n])
            vals.append(jnp.concatenate([part[sl, :], halo[n]], axis=1))
        k, h = vals[:2]
        dz = h / jnp.maximum(k, 1.0)
        kv[tile_rows(i), :] = k
        dv[tile_rows(i), :] = dz
        return vals[2:], from_east(k), from_east(dz)

    def store(i, arg):
        vals, ke, dze = arg
        sl = tile_rows(i)
        hi = tile_rows(min(i + 1, ET - 1))
        k, dz = kv[sl, :], dv[sl, :]
        k_u, k_v = jnp.minimum(k, ke), jnp.minimum(k, up_row(k, kv[hi, :], row))
        dv[sl, :] = 0.5 * (dz + up_row(dz, dv[hi, :], row))
        du[sl, :] = 0.5 * (dz + dze)
        ku[sl, :] = k_u
        kv[sl, :] = k_v
        for out, x, wet in zip(state, vals, (k, k_u, k_v)):
            out[sl, :] = only(wet > 0, x)

    skewed((turn, build, store), TILES, ET)


def tracer_kernel(sizes, t, s, u0, u3, v0, v3, kc, hc, uf, ul, vf, vl, kmt, depth, eta, tu, tv, *rest):
    tm_b, sm_b, pr_b, tke, tkw, rn, rs_b, *rest = rest
    received, rown, wide, rest = rest[:5], rest[5], rest[6:13], rest[13:]
    gains, kf, pke, pkw, prn, prs, south, north, rw, re, rsouth, rnorth, corner, to_west, to_east, *strips, send_sem, recv_sem = rest
    b = pl.program_id(0)
    last = NB // 2 - 1
    net = Exchange(sizes, send_sem, recv_sem)
    planes = (kf, depth, eta, tu, tv)
    head = strip_plan(to_west, to_east, strips) + [(prn, rsouth, 1, 0)] + row_plan(planes, south, north)
    middle = [(prs, rnorth, -1, 0), (pke.at[pl.ds(0, 8), :], rw.at[pl.ds(NR, 8), :], -1, 1)]
    tail = [(pkw.at[pl.ds(NR - 8, 8), :], corner, 1, -1)]

    def piece(i):
        part = pl.ds(16 * i, 16)
        return net.make([(pke.at[part, :], rw.at[part, :], 0, 1), (pkw.at[part, :], re.at[part, :], 0, -1)])

    first_plan = head + middle + tail
    head, middle, tail = net.make(head), net.make(middle), net.make(tail)
    pieces = [piece(i) for i in range(last + 1)]

    @pl.when(b == 0)
    def _():
        kf[:] = kmt[:].astype(F32)
        pack_strips((planes[:2], planes[2:4], planes[4:]), to_west, to_east)
        prn[:] = jnp.zeros(prn.shape, F32)
        prs[:] = jnp.zeros(prs.shape, F32)
        for k in range(NL):
            for n, (lo, hi) in enumerate(((uf, ul), (vf, vl))):
                prn[n, one(k), :] = hi[k, LAST, :]
                prs[n, one(k), :] = lo[k, FIRST, :]
        net.clear(first_plan)
        net.barrier()
        net.start(head)

    for i in range(last):

        @pl.when(b == i + 1)
        def _():
            net.start(pieces[i])

    for half in range(2):
        sl = tile_rows(half)
        tm, sm, rs = tm_b.at[half], sm_b.at[half], rs_b.at[half]
        out = pl.ds(pl.multiple_of(16 * b + 8 * half, 8), 8)
        parts = [x.at[:, sl, :] for x in (t, s, u0, u3, v0, v3)]
        mix_tracers(*parts[:2], kc[sl, :], hc[sl, :], parts[2:], tm, sm, pr_b.at[half], pke.at[out, :], pkw.at[out, :], tke.at[sl, :], tkw.at[sl, :], rs, gains)

    @pl.when(b == 0)
    def _():
        prs[2] = rs_b[0, 2]
        net.start(middle)

    @pl.when(b == last)
    def _():
        net.start(pieces[last] + tail)
        for k in range(NL):
            rn[0, one(k), :] = tm[k, LAST, :]
            rn[1, one(k), :] = sm[k, LAST, :]
        rown[:] = prs[:]
        net.wait(head)
        wide_geometry(planes, strips, south, north, wide)
        net.wait(middle + tail)
        for copies in pieces:
            net.wait(copies)
        for out, x in zip(received, (rw, re, rsouth, rnorth, corner)):
            out[:] = x[:]


PACK = shape(NB, *SLAB)


def block_major(f, n=1):
    return pl.BlockSpec((n,) + SLAB, lambda b: (f(b), 0, 0, 0))


def first_rows(f, n=1):
    return pl.BlockSpec((n, 3, LP, NC), lambda b: (f(b), 0, 0, 0))


def tracers(sizes, t, s, u, v, kmt, depth, eta, tu, tv):
    def cols(width, j):
        return pl.BlockSpec((NL, 16, width), lambda b: (0, b, j))

    def slab(i):
        return pl.BlockSpec(SLAB, lambda b: (0, i, 0))

    pack = block_major(lambda b: b, 2)
    plane = pl.BlockSpec((16, NC), lambda b: (b, 0))
    col = pl.BlockSpec((16, LN), lambda b: (b, 0))
    ends = [slab(0), slab(NB - 1)]
    edge = [(NR + 8, LN), (NR, LN), (2, LP, NC), (3, LP, NC), (8, LN)]
    extra = edge + [(3, LP, NC)] + [(ER, EC)] * 7
    sems = [pltpu.SemaphoreType.DMA((6 + 1 + 10 + 3 + NB,))] * 2
    rows = [VM((2, LP, NC), F32), VM((3, LP, NC), F32)] + [VM((5, HR, NC), F32)] * 2
    return pl.pallas_call(
        functools.partial(tracer_kernel, sizes),
        grid=(NB // 2,),
        in_specs=[cols(NC, 0)] * 2 + [cols(LN, 0), cols(LN, 3)] * 2 + [plane] * 2 + ends * 2 + [whole(NR, NC)] * 5,
        out_specs=[pack] * 3 + [col] * 2 + [whole(2, LP, NC), first_rows(lambda b: b, 2)] + [whole(*x) for x in extra],
        out_shape=[PACK] * 3 + [shape(NR, LN)] * 2 + [shape(2, LP, NC), shape(NB, 3, LP, NC)] + [shape(*x) for x in extra],
        scratch_shapes=[VM(SLAB, F32), VM((NR, NC), F32)] + [VM((NR, LN), F32)] * 2 + rows + [VM(x, F32) for x in edge] + strip_scratch(3) + sems,
        compiler_params=pltpu.CompilerParams(collective_id=0, has_side_effects=True),
        name="tracers",
    )(t, s, u, u, v, v, kmt, depth, u, u, v, v, kmt, depth, eta, tu, tv)


def solve_pair(src_a, src_b, ca, cb, na, nb, out_a, out_b, gain_a, gain_b):
    zero = jnp.zeros(ROW, F32)
    la = lb = pa = pb = wa = wb = zero
    for k in range(NL):
        ua = jnp.where(k + 1 < na, ca, 0.0) if k + 1 < NL else zero
        ub = jnp.where(k + 1 < nb, cb, 0.0) if k + 1 < NL else zero
        ta = 1.0 + la * wa if k else jnp.ones_like(zero)
        tb = 1.0 + lb * wb if k else jnp.ones_like(zero)
        ia = 1.0 / (ta + ua)
        ib = 1.0 / (tb + ub)
        wa, wb = ta * ia, tb * ib
        gain_a[k] = ua * ia
        gain_b[k] = ub * ib
        pa = (src_a[k] + la * pa) * ia
        pb = (src_b[k] + lb * pb) * ib
        src_a[k] = pa
        src_b[k] = pb
        la, lb = ua, ub
    xa = xb = sa = sb = zero
    for k in reversed(range(NL)):
        xa = src_a[k] + gain_a[k] * xa
        xb = src_b[k] + gain_b[k] * xb
        out_a[k] = xa
        out_b[k] = xb
        sa += xa
        sb += xb
    return sa, sb


def momentum_kernel(
    u, v, p_b, pfirst, kun, kvn, kux, kvx, du, dv, kus, kvs, rwn, ren, re, rnorth, rsouth, rown, corner,
    us_b, vs_b, fx, fy, su, sv, pke, vrow,
    cc, hh, srcu, srcv, gu, gv, ums, vms,
):
    step = pl.program_id(0)
    last = step == NB
    us, vs, p = us_b.at[0], vs_b.at[0], p_b.at[0]
    row = iota(ROW, 0)
    rowx = iota(WIDE, 0)
    lane = iota(TILE, 1)
    kxn, kyn = kun[:], kvn[:]
    rwv, rev = rwn[:], ren[:]

    def halos(k):
        hu = jnp.where(lane == 0, lane_to(rev, k, 0), lane_to(rwv, k, LN - 1))
        hv = jnp.where(lane == 0, lane_to(rev, NL + k, 0), lane_to(rwv, NL + k, LN - 1))
        return hu, hv

    def masked(k, uk, vk, halo):
        um = only(k < kxn, jnp.concatenate([uk, halo[0]], axis=1))
        return um, only(k < kyn, jnp.concatenate([vk, halo[1]], axis=1))

    @pl.when(step == 0)
    def _():
        for k in range(NL):
            ums[k], vms[k] = masked(k, u[k], v[k], halos(k))
        lev = iota((LP, NC), 0).astype(F32)
        lev1 = iota((LP, LN), 0)
        ks, kw = kus[LAST, :NC], kvs[LAST, :NC]
        s_u = only(lev < ks, rsouth[0])
        s_v = only(lev < kw, rsouth[1])
        pick = only(iota((LP, LN), 1) == lev1 + NL, corner[LAST, :])
        edge = jnp.sum(pick, axis=1, keepdims=True)
        edge = only(lev[:, :1] < kvs[LAST, one(NC)], edge)
        s_ve = jnp.where(iota((LP, NC), 1) == NC - 1, edge, from_east(s_v))
        u_0 = only(lev < kxn[FIRST, :NC], rown[0])
        v_0 = only(lev < kyn[FIRST, :NC], rown[1])
        c_s = 0.25 * ((s_v + s_ve) * (s_u + u_0))
        h_s = s_v + v_0
        h_s = 0.25 * (h_s * h_s) + rown[2]
        for k in range(NL):
            cc[k, LAST, :] = c_s[one(k), :]
            hh[k, LAST, :] = h_s[one(k), :]

    @pl.when(step > 0)
    def _():
        kx, ky = kux[:], kvx[:]
        pev = re[:]
        total = [jnp.zeros(ROW, F32)] * 2

        def edge(k):
            return halos(k) + (lane_to(pev, 2 * NL + k, 0),)

        def shift(k, halo):
            um, vm = ums[k], vms[k]
            uk = jnp.where(last, rnorth[0, one(k), :], u[k])
            vk = jnp.where(last, rnorth[1, one(k), :], v[k])
            pe = jnp.concatenate([p[k], halo[2]], axis=1)
            return masked(k, uk, vk, halo), pe, from_west(um), from_east(vm)

        def flux(k, arg):
            new, pe, u_w, v_e = arg
            um, vm = ums[k], vms[k]
            c = 0.25 * ((vm + v_e) * (um + up_row(um, new[0], rowx)))
            g = u_w + um
            g = 0.25 * (g * g) + pe
            c5 = c[:, :NC]
            return new, from_east(g)[:, :NC] - g[:, :NC], c5, c5 - from_west(c)[:, :NC]

        def tend(k, arg):
            new, dx, c5, dc = arg
            u5, v5, pk = ums[k, :, :NC], vms[k, :, :NC], p[k]
            north = jnp.where(last, rnorth[2, one(k), :], pfirst[0, 2, one(k), :])
            h = v5 + up_row(v5, new[1][:, :NC], row)
            h = 0.25 * (h * h) + up_row(pk, north, row)
            tu = only(k < kx, dx + (c5 - down_row(c5, cc[k], row)))
            tv = only(k < ky, (h - down_row(h, hh[k], row)) + dc)
            total[0] += tu
            total[1] += tv
            srcu[k] = u5 - DT * tu
            srcv[k] = v5 - DT * tv
            cc[k] = c5
            hh[k] = h
            ums[k], vms[k] = new

        skewed((edge, shift, flux, tend), GROUP)
        dzu, dzv = du[:], dv[:]
        fx[:] = -dzu * total[0]
        fy[:] = -dzv * total[1]
        sa, sb = solve_pair(srcu, srcv, couple(kx, dzu, KV), couple(ky, dzv, KV), kx, ky, us, vs, gu, gv)
        sa, sb = dzu * sa, dzv * sb
        su[:] = sa
        sv[:] = sb
        ae = jnp.zeros(TILE, F32)
        for k in range(NL):
            ae = jnp.where(lane == k, lane_to(us[k, :, NC - LN :], LN - 1, k), ae)
        pke[:] = jnp.where(lane == 3 * NL, lane_to(sa[:, NC - LN :], LN - 1, 3 * NL), ae)

        @pl.when(last)
        def _():
            for k in range(NL):
                vrow[one(k), :] = vs[k, LAST, :]
            vrow[one(NL), :] = sb[LAST, :]
            vrow[NL + 1 : LP, :] = jnp.zeros((LP - NL - 1, NC), F32)


def momentum(u, v, p, first, geo, rw, re, rnorth, rsouth, rown, corner):
    ku, kv, du, dv = geo

    def this(b):
        return jnp.maximum(b, 1) - 1

    def ahead(b):
        return jnp.minimum(b, NB - 1)

    cube = pl.BlockSpec(SLAB, lambda b: (0, ahead(b), 0))
    pack = block_major(this)
    near = pl.BlockSpec(ROW, lambda b: (HT + this(b), 0))
    widn = pl.BlockSpec(WIDE, lambda b: (HT + b, 0))
    wids = pl.BlockSpec(WIDE, lambda b: (HT - 1, 0))
    plane = pl.BlockSpec(ROW, lambda b: (this(b), 0))
    col = pl.BlockSpec(TILE, lambda b: (this(b), 0))
    colw = pl.BlockSpec(TILE, lambda b: (b, 0))
    cole = pl.BlockSpec(TILE, lambda b: (ahead(b), 0))
    flat = jax.ShapeDtypeStruct((NR, NC), F32)

    def rows(n):
        return pl.BlockSpec((n, LP, NC), lambda b: (0, 0, 0))

    return pl.pallas_call(
        momentum_kernel,
        grid=(NB + 1,),
        in_specs=[cube, cube, pack, first_rows(ahead), widn, widn, near, near, near, near, wids, wids, colw, cole, col, rows(3), rows(2), rows(3), pl.BlockSpec(TILE, lambda b: (0, 0))],
        out_specs=[pack, pack, plane, plane, plane, plane, col, pl.BlockSpec((LP, NC), lambda b: (0, 0))],
        out_shape=[PACK, PACK, flat, flat, flat, flat, jax.ShapeDtypeStruct((NR, LN), F32), jax.ShapeDtypeStruct((LP, NC), F32)],
        scratch_shapes=[VM(SLAB, F32)] * 6 + [VM((NL,) + WIDE, F32)] * 2,
        name="momentum",
    )(u, v, p, first, ku, kv, ku, kv, du, dv, ku, kv, rw, re, re, rnorth, rsouth, rown, corner)


def subcycle_kernel(
    sizes, eta_i, tu_i, tv_i, ku, kv, du, dv, fx, fy, tide, uke, tke, tkw, vrow, trn, trs,
    eta_o, u_o, v_o, ub_o, vb_o, fw, fe, fsouth, fnorth,
    eta, tu, tv, cu, cv, fu, fv, ub, vb, edge, south, north, *rest,
):
    to_west, to_east, *strips, send_sem, recv_sem = rest
    net = Exchange(sizes, send_sem, recv_sem)
    edge[:] = uke[:] + tke[:]
    pack_strips(((fx, fy),), to_west, to_east)
    plan = strip_plan(to_west, to_east, strips) + row_plan((fx, fy), south, north)
    late = [
        (edge, fw, 0, 1),
        (tkw, fe, 0, -1),
        (vrow, fsouth.at[0], 1, 0),
        (trn, fsouth.at[pl.ds(1, 2)], 1, 0),
        (trs.at[0], fnorth, -1, 0),
    ]
    net.clear(plan + late)
    net.barrier()
    plan, late = net.make(plan), net.make(late)
    net.start(plan + late)
    row = iota(WIDE, 0)
    zero = jnp.zeros(WIDE, F32)
    ub[:] = jnp.zeros(ub.shape, F32)
    vb[:] = jnp.zeros(vb.shape, F32)
    eta[:] = eta_i[:]
    tu[:] = tu_i[:]
    tv[:] = tv_i[:]
    cu[:] = DTB * (ku[:] * du[:])
    cv[:] = DTB * (kv[:] * dv[:])
    net.wait(plan)

    def turn(i):
        return halo_pair(i, 0, strips)

    def build(i, halo):
        sl = tile_rows(i)
        for n, (x, out, wet) in enumerate(((fx, fu, ku), (fy, fv, kv))):
            part, rows = side(i, x, south.at[n], north.at[n])
            out[sl, :] = only(wet[sl, :] > 0, DTB * jnp.concatenate([part[rows, :], halo[n]], axis=1))

    skewed((turn, build), TILES, ET)
    norm = 6.0 / (SUB * (SUB + 1) * (SUB + 2))

    def stage(first, last, lo, hi):
        def step(n, _):
            tx, ty = tide[n, 0], tide[n, 1]
            w = norm * ((n + 1) * (SUB - n)).astype(F32)

            def west(i):
                return from_west(tu[tile_rows(i), :])

            def surface(i, u_w):
                sl = tile_rows(i)
                vn = tv[sl, :]
                south = tv[tile_rows(i - 1), :] if i else zero
                e = eta[sl, :] - DTB * ((tu[sl, :] - u_w) + (vn - down_row(vn, south, row)))
                eta[sl, :] = e
                return from_east(e)

            def update(i, e_e):
                sl = tile_rows(i)
                e = eta[sl, :]
                un = tu[sl, :] + (cu[sl, :] * (tx - (e_e - e)) + fu[sl, :])
                tu[sl, :] = un
                if lo_bar <= i < hi_bar:
                    ub[sl, :] = ub[sl, :] + w * un
                if i > lo:
                    north(i - 1, e, ty, w)

            skewed((lambda i: west(lo + i), lambda i, x: surface(lo + i, x), lambda i, x: update(lo + i, x)), TILES, hi - lo)
            north(hi - 1, eta[tile_rows(hi - 1), :], ty, w)
            return 0

        lax.fori_loop(first, last, step, 0)

    lo_bar, hi_bar = HT - 1, HT + NB

    def north(i, ahead, ty, w):
        sl = tile_rows(i)
        e = eta[sl, :]
        x = tv[sl, :] + (cv[sl, :] * (ty - (up_row(e, ahead, row) - e)) + fv[sl, :])
        tv[sl, :] = x
        if lo_bar <= i < hi_bar:
            vb[sl, :] = vb[sl, :] + w * x

    for s in range(0, SUB, 8):
        stage(s, min(s + 8, SUB), s // 8, ET - s // 8)
    eta_o[:] = eta[HR : HR + NR, :NC]
    u_o[:] = tu[HR : HR + NR, :NC]
    v_o[:] = tv[HR : HR + NR, :NC]
    ub_o[:] = ub[HR - 8 : HR + NR, :]
    vb_o[:] = vb[HR - 8 : HR + NR, :]
    net.wait(late)


def subcycles(sizes, *args):
    vm = pl.BlockSpec(memory_space=VM)
    outs = [shape(NR, NC)] * 3 + [shape(NR + 8, EC)] * 2 + [shape(NR, LN)] * 2 + [shape(3, LP, NC)] * 2
    sems = [pltpu.SemaphoreType.DMA((6 + 4 + 5,))] * 2
    wide = [VM((ER, EC), F32)] * 9
    return pl.pallas_call(
        functools.partial(subcycle_kernel, sizes),
        in_specs=[vm] * 9 + [pl.BlockSpec(memory_space=pltpu.SMEM)] + [vm] * 5 + [pl.BlockSpec(memory_space=pl.ANY)],
        out_specs=[vm] * len(outs),
        out_shape=outs,
        scratch_shapes=wide + [VM((NR, LN), F32)] + [VM((2, HR, NC), F32)] * 2 + strip_scratch(1) + sems,
        compiler_params=pltpu.CompilerParams(collective_id=1, has_side_effects=True),
        name="subcycles",
    )(*args)


def finish_kernel(*refs):
    ins, kvs, dvs, vbs, eta, tu, tv, rnorth, rsouth, rown, eta_o, tu_o, tv_o, uo, vo, to, so, ct, cs = refs[:23], *refs[23:]
    cubes, planes, wide = ins[:4], ins[4:9], ins[9:]
    b = pl.program_id(0)
    eta_o[:] = eta[:]
    tu_o[:] = tu[:]
    tv_o[:] = tv[:]

    @pl.when(b == 0)
    def _():
        lev = iota((LP, NC), 0).astype(F32)
        kx = kvs[LAST, :NC]
        cor = correction(vbs[LAST, :NC], rsouth[0, one(NL), :], kx, dvs[LAST, :NC])
        vel = 0.5 * DT * only(lev < kx, rsouth[0] + cor)
        ft = vel * (rsouth[1] + rown[0, 0])
        fs = vel * (rsouth[2] + rown[0, 1])
        for k in range(NL):
            ct[k, LAST, :] = ft[one(k), :]
            cs[k, LAST, :] = fs[one(k), :]

    for half in range(2):
        sl = tile_rows(half)
        outs = [x.at[:, sl, :] for x in (uo, vo, to, so)]
        last = (b == NB // 2 - 1) if half else None
        finish_rows(last, *[x.at[half] for x in cubes], *[x[sl, :] for x in planes], *wide[half::2], rnorth, *outs, ct, cs)


def correction(mean, total, k, dz):
    deep = k * dz
    return (mean - total) / jnp.where(deep > 0, deep, 1.0)


def finish_rows(last, us, vs, t, s, cnt, su, sv, rwv, rev, ku, kv, du, dv, ub, vb, first, rnorth, uo, vo, to, so, ct, cs):
    row = iota(ROW, 0)
    lane = iota(TILE, 1)

    kx, ky = ku[:], kv[:, :NC]
    tot = jnp.concatenate([su, lane_to(rwv, 3 * NL, LN - 1)], axis=1)
    cx = correction(ub[:], tot, kx, du[:])
    cy = correction(vb[:, :NC], sv, ky, dv[:, :NC])
    fields = ((t, to, ct), (s, so, cs))

    def load(k):
        out = [lane_to(rwv, k, LN - 1)]
        for i in range(2):
            base = NL * (i + 1) + k
            out.append(jnp.where(lane == 0, lane_to(rev, base, 0), lane_to(rwv, base, LN - 1)))
        return out

    def east(k, halo):
        wide = [jnp.concatenate([f[0][k], h], axis=1) for f, h in zip(fields, halo[1:])]
        return halo[0], [x + from_east(x) for x in wide]

    def flux(k, arg):
        halo, sums = arg
        ue = only(k < kx, jnp.concatenate([us[k], halo], axis=1) + cx)
        uo[k] = ue[:, :NC]
        f = [(0.5 * DT) * ue * x for x in sums]
        return [(x - from_west(x))[:, :NC] for x in f]

    def store(k, div):
        ve = only(k < ky, vs[k] + cy)
        vo[k] = ve
        hy = (0.5 * DT) * ve
        for i, (x, out, carry) in enumerate(fields):
            own = x[k]
            north = first[0, i, one(k), :]
            if last is not None:
                north = jnp.where(last, rnorth[i, one(k), :], north)
            fy = hy * (own + up_row(own, north, row))
            new = own - (div[i] + (fy - down_row(fy, carry[k], row)))
            carry[k] = fy
            out[k] = only(k < cnt, new)

    skewed((load, east, flux, store), GROUP)


def finish(us, vs, tm, sm, first, kmt, geo, ub, vb, su, sv, rw, re, rnorth, rsouth, state):
    kv, dv = geo[1], geo[3]

    def rows(width):
        return pl.BlockSpec((16, width), lambda b: (b, 0))

    def pair(start):
        return [pl.BlockSpec(WIDE, lambda b, h=h: (start + 2 * b + h, 0)) for h in range(2)]

    def fixed(i):
        return pl.BlockSpec(WIDE, lambda b: (i, 0))

    ahead = [first_rows(lambda b: 2 * b + 1), first_rows(lambda b: jnp.minimum(2 * b + 2, NB - 1))]
    cube = pl.BlockSpec((NL, 16, NC), lambda b: (0, b, 0))
    south = [fixed(HT - 1)] * 2 + [fixed(0)]
    wide = [x for x in (*geo, ub, vb, first) for _ in range(2)]
    return pl.pallas_call(
        finish_kernel,
        grid=(NB // 2,),
        in_specs=[block_major(lambda b: b, 2)] * 4 + [rows(NC)] * 3 + [rows(LN)] * 2 + pair(HT) * 4 + pair(1) * 2 + ahead + south + [rows(NC)] * 3 + [whole(3, LP, NC)] * 2 + [first_rows(lambda b: 0)],
        out_specs=[rows(NC)] * 3 + [cube] * 4,
        out_shape=[shape(NR, NC)] * 3 + [shape(NL, NR, NC)] * 4,
        scratch_shapes=[VM(SLAB, F32)] * 2,
        name="finish",
    )(us, vs, tm, sm, kmt, su, sv, rw, re, *wide, kv, dv, vb, *state, rnorth, rsouth, first)


def solution(mesh):
    sizes = mesh.shape["row"], mesh.shape["col"]

    def local_step(u, v, t, s, eta, tu, tv, depth, kmt, tide):
        tm, sm, pr, tke, tkw, trn, first, rw, re, rsouth, rnorth, corner, rown, *wide = tracers(sizes, t, s, u, v, kmt, depth, eta, tu, tv)
        geo, state = wide[:4], wide[4:]
        us, vs, fx, fy, su, sv, uke, vrow = momentum(u, v, pr, first, geo, rw, re, rnorth, rsouth, rown, corner)
        eta_n, u_n, v_n, ub, vb, fw, fe, fsouth, fnorth = subcycles(sizes, *state, *geo, fx, fy, tide, uke, tke, tkw, vrow, trn, first)
        return finish(us, vs, tm, sm, first, kmt, geo, ub, vb, su, sv, fw, fe, fnorth, fsouth, (eta_n, u_n, v_n))

    cube, plane = P(None, "row", "col"), P("row", "col")
    return jax.shard_map(
        local_step,
        mesh=mesh,
        in_specs=(cube,) * 4 + (plane,) * 5 + (P(None, None),),
        out_specs=(plane,) * 3 + (cube,) * 4,
        check_vma=False,
    )
```

```python
import functools

import jax
import jax.numpy as jnp
from jax import lax
from jax.experimental import pallas as pl
from jax.experimental.pallas import tpu as pltpu
from jax.sharding import PartitionSpec as P

NL = 41
NR = 96
NC = 512
LN = 128
LP = 48
HR = 40
ER = NR + 2 * HR
EC = NC + 128
NB = NR // 8
SUB = 36
GROUP = 2
HALF = 64
SIDES = (-1, 0, 1)
FIRST, LAST = slice(0, 1), slice(7, 8)
TILES = 3
DT = 4.0
DTB = DT / SUB
KV = 0.001
KT = 0.0005
F32 = jnp.float32
HT = HR // 8
ET = ER // 8
SLAB, ROW, WIDE, TILE = (NL, 8, NC), (8, NC), (8, EC), (8, LN)
VM = pltpu.VMEM


def only(mask, x):
    return jnp.where(mask, x, jnp.zeros_like(x))


def iota(shape, dim):
    return lax.broadcasted_iota(jnp.int32, shape, dim)


def whole(*shape):
    return pl.BlockSpec(shape, lambda *_: (0,) * len(shape))


def shape(*dims):
    return jax.ShapeDtypeStruct(dims, F32)


def one(k):
    return slice(k, k + 1)


def tile_rows(i):
    return slice(8 * i, 8 * (i + 1))


def from_west(x):
    return pltpu.roll(x, 1, axis=1)


def from_east(x):
    return pltpu.roll(x, x.shape[1] - 1, axis=1)


def lane_to(x, src, dst):
    shift = (dst - src) % LN
    return x if shift == 0 else pltpu.roll(x, shift, axis=1)


def up_row(x, nxt, row):
    return pltpu.roll(jnp.where(row == 0, nxt, x), 7, axis=0)


def down_row(x, prev, row):
    return pltpu.roll(jnp.where(row == 7, prev, x), 1, axis=0)


def skewed(stages, group, count=NL):
    blocks = [range(k, min(k + group, count)) for k in range(0, count, group)]
    held = {}
    for i in range(len(blocks) + len(stages) - 1):
        for n, stage in enumerate(stages):
            if 0 <= i - n < len(blocks):
                for k in blocks[i - n]:
                    held[k] = stage(k, held[k]) if n else stage(k)


def couple(count, thick, kappa):
    safe = jnp.where(count > 0, thick, 1.0)
    return DT * kappa / (safe * safe)


def pressure_step(t, s, wet, cum, thick):
    half = only(wet, 0.5 * (0.015 * (s - 1.0) - 0.02 * (t - 1.0)))
    mid = cum + half
    return thick * mid, mid + half


class Exchange:
    def __init__(self, sizes, send_sem, recv_sem):
        self.rows, self.cols = sizes
        self.row, self.col = lax.axis_index("row"), lax.axis_index("col")
        self.sems = send_sem, recv_sem
        self.used = 0

    def inside(self, drow):
        return (self.row + drow >= 0) & (self.row + drow < self.rows)

    def at(self, drow, dcol):
        return {"row": self.row + drow, "col": lax.rem(self.col + dcol + self.cols, self.cols)}

    def when(self, drow, action):
        if drow:
            pl.when(self.inside(drow))(action)
        else:
            action()

    def barrier(self):
        ready = pltpu.get_barrier_semaphore()
        for drow in SIDES:
            for dcol in SIDES:
                if drow or dcol:
                    self.when(drow, functools.partial(pl.semaphore_signal, ready, device_id=self.at(drow, dcol), device_id_type=pl.DeviceIdType.MESH))
        per_row = len(SIDES)
        known = [self.inside(drow).astype(jnp.int32) for drow in SIDES if drow]
        pl.semaphore_wait(ready, per_row - 1 + per_row * sum(known))

    def clear(self, plan):
        for _, dst, drow, _ in plan:
            if drow:

                @pl.when(jnp.logical_not(self.inside(-drow)))
                def _():
                    dst[:] = jnp.zeros(dst.shape, F32)

    def make(self, plan):
        out = []
        for src, dst, drow, dcol in plan:
            copy = pltpu.make_async_remote_copy(
                src_ref=src,
                dst_ref=dst,
                send_sem=self.sems[0].at[self.used],
                recv_sem=self.sems[1].at[self.used],
                device_id=self.at(drow, dcol),
                device_id_type=pl.DeviceIdType.MESH,
            )
            self.used += 1
            out.append((copy, drow))
        return out

    def start(self, copies):
        for copy, drow in copies:
            self.when(drow, copy.start)

    def wait(self, copies):
        for copy, drow in copies:
            self.when(drow, copy.wait_send)
            self.when(-drow, copy.wait_recv)


def pack_strips(pairs, to_west, to_east):
    lane = iota(TILE, 1)
    first, last = slice(0, LN), slice(NC - LN, NC)

    def turn(n):
        q, sl = n // NB, tile_rows(n % NB)
        b = pairs[q][-1]
        return pltpu.roll(b[sl, first], HALF, axis=1), pltpu.roll(b[sl, last], HALF, axis=1)

    def store(n, turned):
        q, sl = n // NB, tile_rows(n % NB)
        a = pairs[q][0]
        to_west[q, sl, :] = jnp.where(lane < HALF, a[sl, first], turned[0])
        to_east[q, sl, :] = jnp.where(lane < HALF, turned[1], a[sl, last])

    skewed((turn, store), NB, NB * len(pairs))


def strip_plan(to_west, to_east, strips):
    top, bottom = pl.ds(NR - HR, HR), pl.ds(0, HR)
    return [
        (to_east, strips[0], 0, 1),
        (to_west, strips[1], 0, -1),
        (to_east.at[:, top], strips[2], 1, 1),
        (to_west.at[:, top], strips[3], 1, -1),
        (to_east.at[:, bottom], strips[4], -1, 1),
        (to_west.at[:, bottom], strips[5], -1, -1),
    ]


def row_plan(planes, south, north):
    plan = []
    for i, x in enumerate(planes):
        plan.append((x.at[pl.ds(NR - HR, HR), :], south.at[i], 1, 0))
        plan.append((x.at[pl.ds(0, HR), :], north.at[i], -1, 0))
    return plan


def strip_scratch(n):
    return [VM((n, NR, LN), F32)] * 4 + [VM((n, HR, LN), F32)] * 4


def side(i, own, south, north):
    if i < HT:
        return south, tile_rows(i)
    return (own, tile_rows(i - HT)) if i < HT + NB else (north, tile_rows(i - HT - NB))


def halo_pair(i, q, strips):
    (w, e), sl = side(i, strips[:2], strips[2:4], strips[4:])
    lane = iota(TILE, 1)
    w, e = w[q, sl, :], e[q, sl, :]
    return jnp.where(lane < HALF, e, w), pltpu.roll(jnp.where(lane < HALF, w, e), HALF, axis=1)


def mix_tracers(t, s, cnt, depth, strips, tm, sm, pr, pke, pkw, tke, tkw, rs, gains):
    lane = iota(TILE, 1)
    thick = depth / jnp.maximum(cnt, 1).astype(F32)
    c = couple(cnt, thick, KT)
    zero = jnp.zeros(ROW, F32)
    cum = lower = pt = ps = zero
    keep = zero
    ae = aw = jnp.zeros(TILE, F32)
    u0, u3, v0, v3 = strips
    for k in range(NL):
        wet = k < cnt
        tk, sk = t[k], s[k]
        p, cum = pressure_step(tk, sk, wet, cum, thick)
        pr[k] = p
        for n, (x0, x3) in enumerate(((u0, u3), (v0, v3))):
            base = NL * n + k
            ae = jnp.where(lane == base, lane_to(x3[k], LN - 1, base), ae)
            aw = jnp.where(lane == base, lane_to(x0[k], 0, base), aw)
        aw = jnp.where(lane == 2 * NL + k, lane_to(p[:, :LN], 0, 2 * NL + k), aw)
        rs[2, one(k), :] = p[FIRST, :]
        upper = jnp.where(k + 1 < cnt, c, 0.0) if k + 1 < NL else zero
        top = 1.0 + lower * keep if k else jnp.ones_like(zero)
        inv = 1.0 / (top + upper)
        keep = top * inv
        gains[k] = upper * inv
        pt = (jnp.where(wet, tk, 0.0) + lower * pt) * inv
        ps = (jnp.where(wet, sk, 0.0) + lower * ps) * inv
        tm[k] = pt
        sm[k] = ps
        lower = upper
    pke[:] = ae
    pkw[:] = aw
    ae = aw = jnp.zeros(TILE, F32)
    bt = bs = zero
    for k in reversed(range(NL)):
        gain = gains[k]
        bt = tm[k] + gain * bt
        bs = sm[k] + gain * bs
        tm[k] = bt
        sm[k] = bs
        rs[0, one(k), :] = bt[FIRST, :]
        rs[1, one(k), :] = bs[FIRST, :]
        for x, base in ((bt, NL), (bs, 2 * NL)):
            ae = jnp.where(lane == base + k, lane_to(x[:, NC - LN :], LN - 1, base + k), ae)
            aw = jnp.where(lane == base + k, lane_to(x[:, :LN], 0, base + k), aw)
    tke[:] = ae
    tkw[:] = aw


def wide_geometry(planes, strips, south, north, outs):
    ku, kv, du, dv, *state = outs
    row = iota(WIDE, 0)

    def turn(i):
        return [halo_pair(i, q, strips) for q in range(3)]

    def build(i, halo):
        halo = [x for pair in halo for x in pair]
        vals = []
        for n in range(len(planes)):
            part, sl = side(i, planes[n], south.at[n], north.at[n])
            vals.append(jnp.concatenate([part[sl, :], halo[n]], axis=1))
        k, h = vals[:2]
        dz = h / jnp.maximum(k, 1.0)
        kv[tile_rows(i), :] = k
        dv[tile_rows(i), :] = dz
        return vals[2:], from_east(k), from_east(dz)

    def store(i, arg):
        vals, ke, dze = arg
        sl = tile_rows(i)
        hi = tile_rows(min(i + 1, ET - 1))
        k, dz = kv[sl, :], dv[sl, :]
        k_u, k_v = jnp.minimum(k, ke), jnp.minimum(k, up_row(k, kv[hi, :], row))
        dv[sl, :] = 0.5 * (dz + up_row(dz, dv[hi, :], row))
        du[sl, :] = 0.5 * (dz + dze)
        ku[sl, :] = k_u
        kv[sl, :] = k_v
        for out, x, wet in zip(state, vals, (k, k_u, k_v)):
            out[sl, :] = only(wet > 0, x)

    skewed((turn, build, store), TILES, ET)


def tracer_kernel(sizes, t, s, u0, u3, v0, v3, kc, hc, uf, ul, vf, vl, kmt, depth, eta, tu, tv, *rest):
    tm_b, sm_b, pr_b, tke, tkw, rn, rs_b, *rest = rest
    received, rown, wide, rest = rest[:5], rest[5], rest[6:13], rest[13:]
    gains, kf, pke, pkw, prn, prs, south, north, rw, re, rsouth, rnorth, corner, to_west, to_east, *strips, send_sem, recv_sem = rest
    b = pl.program_id(0)
    last = NB // 2 - 1
    net = Exchange(sizes, send_sem, recv_sem)
    planes = (kf, depth, eta, tu, tv)
    head = strip_plan(to_west, to_east, strips) + [(prn, rsouth, 1, 0)] + row_plan(planes, south, north)
    middle = [(prs, rnorth, -1, 0), (pke.at[pl.ds(0, 8), :], rw.at[pl.ds(NR, 8), :], -1, 1)]
    tail = [(pkw.at[pl.ds(NR - 8, 8), :], corner, 1, -1)]

    def piece(i):
        part = pl.ds(16 * i, 16)
        return net.make([(pke.at[part, :], rw.at[part, :], 0, 1), (pkw.at[part, :], re.at[part, :], 0, -1)])

    first_plan = head + middle + tail
    head, middle, tail = net.make(head), net.make(middle), net.make(tail)
    pieces = [piece(i) for i in range(last + 1)]

    @pl.when(b == 0)
    def _():
        kf[:] = kmt[:].astype(F32)
        pack_strips((planes[:2], planes[2:4], planes[4:]), to_west, to_east)
        prn[:] = jnp.zeros(prn.shape, F32)
        prs[:] = jnp.zeros(prs.shape, F32)
        for k in range(NL):
            for n, (lo, hi) in enumerate(((uf, ul), (vf, vl))):
                prn[n, one(k), :] = hi[k, LAST, :]
                prs[n, one(k), :] = lo[k, FIRST, :]
        net.clear(first_plan)
        net.barrier()
        net.start(head)

    for i in range(last):

        @pl.when(b == i + 1)
        def _():
            net.start(pieces[i])

    for half in range(2):
        sl = tile_rows(half)
        tm, sm, rs = tm_b.at[half], sm_b.at[half], rs_b.at[half]
        out = pl.ds(pl.multiple_of(16 * b + 8 * half, 8), 8)
        parts = [x.at[:, sl, :] for x in (t, s, u0, u3, v0, v3)]
        mix_tracers(*parts[:2], kc[sl, :], hc[sl, :], parts[2:], tm, sm, pr_b.at[half], pke.at[out, :], pkw.at[out, :], tke.at[sl, :], tkw.at[sl, :], rs, gains)

    @pl.when(b == 0)
    def _():
        prs[2] = rs_b[0, 2]
        net.start(middle)

    @pl.when(b == last)
    def _():
        net.start(pieces[last] + tail)
        for k in range(NL):
            rn[0, one(k), :] = tm[k, LAST, :]
            rn[1, one(k), :] = sm[k, LAST, :]
        rown[:] = prs[:]
        net.wait(head)
        wide_geometry(planes, strips, south, north, wide)
        net.wait(middle + tail)
        for copies in pieces:
            net.wait(copies)
        for out, x in zip(received, (rw, re, rsouth, rnorth, corner)):
            out[:] = x[:]


PACK = VM((NB,) + SLAB, F32)
PACK_HBM = pltpu.HBM((NB,) + SLAB, F32)


def block_major(f, n=1):
    return pl.BlockSpec((n,) + SLAB, lambda b: (f(b), 0, 0, 0))


def first_rows(f, n=1):
    return pl.BlockSpec((n, 3, LP, NC), lambda b: (f(b), 0, 0, 0))


def tracers(sizes, t, s, u, v, kmt, depth, eta, tu, tv):
    def cols(width, j):
        return pl.BlockSpec((NL, 16, width), lambda b: (0, b, j))

    def slab(i):
        return pl.BlockSpec(SLAB, lambda b: (0, i, 0))

    pack = block_major(lambda b: b, 2)
    plane = pl.BlockSpec((16, NC), lambda b: (b, 0))
    col = pl.BlockSpec((16, LN), lambda b: (b, 0))
    ends = [slab(0), slab(NB - 1)]
    edge = [(NR + 8, LN), (NR, LN), (2, LP, NC), (3, LP, NC), (8, LN)]
    extra = edge + [(3, LP, NC)] + [(ER, EC)] * 7
    sems = [pltpu.SemaphoreType.DMA((6 + 1 + 10 + 3 + NB,))] * 2
    rows = [VM((2, LP, NC), F32), VM((3, LP, NC), F32)] + [VM((5, HR, NC), F32)] * 2
    return pl.pallas_call(
        functools.partial(tracer_kernel, sizes),
        grid=(NB // 2,),
        in_specs=[cols(NC, 0)] * 2 + [cols(LN, 0), cols(LN, 3)] * 2 + [plane] * 2 + ends * 2 + [whole(NR, NC)] * 5,
        out_specs=[pack] * 3 + [col] * 2 + [whole(2, LP, NC), first_rows(lambda b: b, 2)] + [whole(*x) for x in extra],
        out_shape=[PACK] * 2 + [PACK_HBM] + [shape(NR, LN)] * 2 + [shape(2, LP, NC), pltpu.HBM((NB, 3, LP, NC), F32)] + [shape(*x) for x in extra],
        scratch_shapes=[VM(SLAB, F32), VM((NR, NC), F32)] + [VM((NR, LN), F32)] * 2 + rows + [VM(x, F32) for x in edge] + strip_scratch(3) + sems,
        compiler_params=pltpu.CompilerParams(collective_id=0, has_side_effects=True, vmem_limit_bytes=26 << 20),
        name="tracers",
    )(t, s, u, u, v, v, kmt, depth, u, u, v, v, kmt, depth, eta, tu, tv)


def solve_pair(src_a, src_b, ca, cb, na, nb, out_a, out_b, gain_a, gain_b):
    zero = jnp.zeros(ROW, F32)
    la = lb = pa = pb = wa = wb = zero
    for k in range(NL):
        ua = jnp.where(k + 1 < na, ca, 0.0) if k + 1 < NL else zero
        ub = jnp.where(k + 1 < nb, cb, 0.0) if k + 1 < NL else zero
        ta = 1.0 + la * wa if k else jnp.ones_like(zero)
        tb = 1.0 + lb * wb if k else jnp.ones_like(zero)
        ia = 1.0 / (ta + ua)
        ib = 1.0 / (tb + ub)
        wa, wb = ta * ia, tb * ib
        gain_a[k] = ua * ia
        gain_b[k] = ub * ib
        pa = (src_a[k] + la * pa) * ia
        pb = (src_b[k] + lb * pb) * ib
        src_a[k] = pa
        src_b[k] = pb
        la, lb = ua, ub
    xa = xb = sa = sb = zero
    for k in reversed(range(NL)):
        xa = src_a[k] + gain_a[k] * xa
        xb = src_b[k] + gain_b[k] * xb
        out_a[k] = xa
        out_b[k] = xb
        sa += xa
        sb += xb
    return sa, sb


def momentum_kernel(
    u, v, p_b, pfirst, kun, kvn, kux, kvx, du, dv, kus, kvs, rwn, ren, re, rnorth, rsouth, rown, corner,
    us_b, vs_b, fx, fy, su, sv, pke, vrow,
    cc, hh, srcu, srcv, gu, gv, ums, vms,
):
    step = pl.program_id(0)
    last = step == NB
    us, vs, p = us_b.at[0], vs_b.at[0], p_b.at[0]
    row = iota(ROW, 0)
    rowx = iota(WIDE, 0)
    lane = iota(TILE, 1)
    kxn, kyn = kun[:], kvn[:]
    rwv, rev = rwn[:], ren[:]

    def halos(k):
        hu = jnp.where(lane == 0, lane_to(rev, k, 0), lane_to(rwv, k, LN - 1))
        hv = jnp.where(lane == 0, lane_to(rev, NL + k, 0), lane_to(rwv, NL + k, LN - 1))
        return hu, hv

    def masked(k, uk, vk, halo):
        um = only(k < kxn, jnp.concatenate([uk, halo[0]], axis=1))
        return um, only(k < kyn, jnp.concatenate([vk, halo[1]], axis=1))

    @pl.when(step == 0)
    def _():
        for k in range(NL):
            ums[k], vms[k] = masked(k, u[k], v[k], halos(k))
        lev = iota((LP, NC), 0).astype(F32)
        lev1 = iota((LP, LN), 0)
        ks, kw = kus[LAST, :NC], kvs[LAST, :NC]
        s_u = only(lev < ks, rsouth[0])
        s_v = only(lev < kw, rsouth[1])
        pick = only(iota((LP, LN), 1) == lev1 + NL, corner[LAST, :])
        edge = jnp.sum(pick, axis=1, keepdims=True)
        edge = only(lev[:, :1] < kvs[LAST, one(NC)], edge)
        s_ve = jnp.where(iota((LP, NC), 1) == NC - 1, edge, from_east(s_v))
        u_0 = only(lev < kxn[FIRST, :NC], rown[0])
        v_0 = only(lev < kyn[FIRST, :NC], rown[1])
        c_s = 0.25 * ((s_v + s_ve) * (s_u + u_0))
        h_s = s_v + v_0
        h_s = 0.25 * (h_s * h_s) + rown[2]
        for k in range(NL):
            cc[k, LAST, :] = c_s[one(k), :]
            hh[k, LAST, :] = h_s[one(k), :]

    @pl.when(step > 0)
    def _():
        kx, ky = kux[:], kvx[:]
        pev = re[:]
        total = [jnp.zeros(ROW, F32)] * 2

        def edge(k):
            return halos(k) + (lane_to(pev, 2 * NL + k, 0),)

        def shift(k, halo):
            um, vm = ums[k], vms[k]
            uk = jnp.where(last, rnorth[0, one(k), :], u[k])
            vk = jnp.where(last, rnorth[1, one(k), :], v[k])
            pe = jnp.concatenate([p[k], halo[2]], axis=1)
            return masked(k, uk, vk, halo), pe, from_west(um), from_east(vm)

        def flux(k, arg):
            new, pe, u_w, v_e = arg
            um, vm = ums[k], vms[k]
            c = 0.25 * ((vm + v_e) * (um + up_row(um, new[0], rowx)))
            g = u_w + um
            g = 0.25 * (g * g) + pe
            c5 = c[:, :NC]
            return new, from_east(g)[:, :NC] - g[:, :NC], c5, c5 - from_west(c)[:, :NC]

        def tend(k, arg):
            new, dx, c5, dc = arg
            u5, v5, pk = ums[k, :, :NC], vms[k, :, :NC], p[k]
            north = jnp.where(last, rnorth[2, one(k), :], pfirst[0, 2, one(k), :])
            h = v5 + up_row(v5, new[1][:, :NC], row)
            h = 0.25 * (h * h) + up_row(pk, north, row)
            tu = only(k < kx, dx + (c5 - down_row(c5, cc[k], row)))
            tv = only(k < ky, (h - down_row(h, hh[k], row)) + dc)
            total[0] += tu
            total[1] += tv
            srcu[k] = u5 - DT * tu
            srcv[k] = v5 - DT * tv
            cc[k] = c5
            hh[k] = h
            ums[k], vms[k] = new

        skewed((edge, shift, flux, tend), GROUP)
        dzu, dzv = du[:], dv[:]
        fx[:] = -dzu * total[0]
        fy[:] = -dzv * total[1]
        sa, sb = solve_pair(srcu, srcv, couple(kx, dzu, KV), couple(ky, dzv, KV), kx, ky, us, vs, gu, gv)
        sa, sb = dzu * sa, dzv * sb
        su[:] = sa
        sv[:] = sb
        ae = jnp.zeros(TILE, F32)
        for k in range(NL):
            ae = jnp.where(lane == k, lane_to(us[k, :, NC - LN :], LN - 1, k), ae)
        pke[:] = jnp.where(lane == 3 * NL, lane_to(sa[:, NC - LN :], LN - 1, 3 * NL), ae)

        @pl.when(last)
        def _():
            for k in range(NL):
                vrow[one(k), :] = vs[k, LAST, :]
            vrow[one(NL), :] = sb[LAST, :]
            vrow[NL + 1 : LP, :] = jnp.zeros((LP - NL - 1, NC), F32)


def momentum(u, v, p, first, geo, rw, re, rnorth, rsouth, rown, corner):
    ku, kv, du, dv = geo

    def this(b):
        return jnp.maximum(b, 1) - 1

    def ahead(b):
        return jnp.minimum(b, NB - 1)

    cube = pl.BlockSpec(SLAB, lambda b: (0, ahead(b), 0))
    pack = block_major(this)
    near = pl.BlockSpec(ROW, lambda b: (HT + this(b), 0))
    widn = pl.BlockSpec(WIDE, lambda b: (HT + b, 0))
    wids = pl.BlockSpec(WIDE, lambda b: (HT - 1, 0))
    plane = pl.BlockSpec(ROW, lambda b: (this(b), 0))
    col = pl.BlockSpec(TILE, lambda b: (this(b), 0))
    colw = pl.BlockSpec(TILE, lambda b: (b, 0))
    cole = pl.BlockSpec(TILE, lambda b: (ahead(b), 0))
    flat = jax.ShapeDtypeStruct((NR, NC), F32)

    def rows(n):
        return pl.BlockSpec((n, LP, NC), lambda b: (0, 0, 0))

    return pl.pallas_call(
        momentum_kernel,
        grid=(NB + 1,),
        in_specs=[cube, cube, pack, first_rows(ahead), widn, widn, near, near, near, near, wids, wids, colw, cole, col, rows(3), rows(2), rows(3), pl.BlockSpec(TILE, lambda b: (0, 0))],
        out_specs=[pack, pack, plane, plane, plane, plane, col, pl.BlockSpec((LP, NC), lambda b: (0, 0))],
        out_shape=[PACK, PACK_HBM, flat, flat, flat, flat, jax.ShapeDtypeStruct((NR, LN), F32), jax.ShapeDtypeStruct((LP, NC), F32)],
        scratch_shapes=[VM(SLAB, F32)] * 6 + [VM((NL,) + WIDE, F32)] * 2,
        compiler_params=pltpu.CompilerParams(vmem_limit_bytes=22 << 20),
        name="momentum",
    )(u, v, p, first, ku, kv, ku, kv, du, dv, ku, kv, rw, re, re, rnorth, rsouth, rown, corner)


def subcycle_kernel(
    sizes, eta_i, tu_i, tv_i, ku, kv, du, dv, fx, fy, tide, uke, tke, tkw, vrow, trn, trs,
    eta_o, u_o, v_o, ub_o, vb_o, fw, fe, fsouth, fnorth,
    eta, tu, tv, cu, cv, fu, fv, ub, vb, edge, south, north, *rest,
):
    to_west, to_east, *strips, send_sem, recv_sem = rest
    net = Exchange(sizes, send_sem, recv_sem)
    edge[:] = uke[:] + tke[:]
    pack_strips(((fx, fy),), to_west, to_east)
    plan = strip_plan(to_west, to_east, strips) + row_plan((fx, fy), south, north)
    late = [
        (edge, fw, 0, 1),
        (tkw, fe, 0, -1),
        (vrow, fsouth.at[0], 1, 0),
        (trn, fsouth.at[pl.ds(1, 2)], 1, 0),
        (trs.at[0], fnorth, -1, 0),
    ]
    net.clear(plan + late)
    net.barrier()
    plan, late = net.make(plan), net.make(late)
    net.start(plan + late)
    row = iota(WIDE, 0)
    zero = jnp.zeros(WIDE, F32)
    ub[:] = jnp.zeros(ub.shape, F32)
    vb[:] = jnp.zeros(vb.shape, F32)
    eta[:] = eta_i[:]
    tu[:] = tu_i[:]
    tv[:] = tv_i[:]
    cu[:] = DTB * (ku[:] * du[:])
    cv[:] = DTB * (kv[:] * dv[:])
    net.wait(plan)

    def turn(i):
        return halo_pair(i, 0, strips)

    def build(i, halo):
        sl = tile_rows(i)
        for n, (x, out, wet) in enumerate(((fx, fu, ku), (fy, fv, kv))):
            part, rows = side(i, x, south.at[n], north.at[n])
            out[sl, :] = only(wet[sl, :] > 0, DTB * jnp.concatenate([part[rows, :], halo[n]], axis=1))

    skewed((turn, build), TILES, ET)
    norm = 6.0 / (SUB * (SUB + 1) * (SUB + 2))

    def stage(first, last, lo, hi):
        def step(n, _):
            tx, ty = tide[n, 0], tide[n, 1]
            w = norm * ((n + 1) * (SUB - n)).astype(F32)

            def west(i):
                return from_west(tu[tile_rows(i), :])

            def surface(i, u_w):
                sl = tile_rows(i)
                vn = tv[sl, :]
                south = tv[tile_rows(i - 1), :] if i else zero
                e = eta[sl, :] - DTB * ((tu[sl, :] - u_w) + (vn - down_row(vn, south, row)))
                eta[sl, :] = e
                return from_east(e)

            def update(i, e_e):
                sl = tile_rows(i)
                e = eta[sl, :]
                un = tu[sl, :] + (cu[sl, :] * (tx - (e_e - e)) + fu[sl, :])
                tu[sl, :] = un
                if lo_bar <= i < hi_bar:
                    ub[sl, :] = ub[sl, :] + w * un
                if i > lo:
                    north(i - 1, e, ty, w)

            skewed((lambda i: west(lo + i), lambda i, x: surface(lo + i, x), lambda i, x: update(lo + i, x)), TILES, hi - lo)
            north(hi - 1, eta[tile_rows(hi - 1), :], ty, w)
            return 0

        lax.fori_loop(first, last, step, 0)

    lo_bar, hi_bar = HT - 1, HT + NB

    def north(i, ahead, ty, w):
        sl = tile_rows(i)
        e = eta[sl, :]
        x = tv[sl, :] + (cv[sl, :] * (ty - (up_row(e, ahead, row) - e)) + fv[sl, :])
        tv[sl, :] = x
        if lo_bar <= i < hi_bar:
            vb[sl, :] = vb[sl, :] + w * x

    for s in range(0, SUB, 8):
        stage(s, min(s + 8, SUB), s // 8, ET - s // 8)
    eta_o[:] = eta[HR : HR + NR, :NC]
    u_o[:] = tu[HR : HR + NR, :NC]
    v_o[:] = tv[HR : HR + NR, :NC]
    ub_o[:] = ub[HR - 8 : HR + NR, :]
    vb_o[:] = vb[HR - 8 : HR + NR, :]
    net.wait(late)


def subcycles(sizes, *args):
    vm = pl.BlockSpec(memory_space=VM)
    outs = [shape(NR, NC)] * 3 + [shape(NR + 8, EC)] * 2 + [shape(NR, LN)] * 2 + [shape(3, LP, NC)] * 2
    sems = [pltpu.SemaphoreType.DMA((6 + 4 + 5,))] * 2
    wide = [VM((ER, EC), F32)] * 9
    return pl.pallas_call(
        functools.partial(subcycle_kernel, sizes),
        in_specs=[vm] * 9 + [pl.BlockSpec(memory_space=pltpu.SMEM)] + [vm] * 5 + [pl.BlockSpec(memory_space=pl.ANY)],
        out_specs=[vm] * len(outs),
        out_shape=outs,
        scratch_shapes=wide + [VM((NR, LN), F32)] + [VM((2, HR, NC), F32)] * 2 + strip_scratch(1) + sems,
        compiler_params=pltpu.CompilerParams(collective_id=1, has_side_effects=True, vmem_limit_bytes=22 << 20),
        name="subcycles",
    )(*args)


def finish_kernel(*refs):
    ins, kvs, dvs, vbs, eta, tu, tv, rnorth, rsouth, rown, eta_o, tu_o, tv_o, uo, vo, to, so, ct, cs = refs[:23], *refs[23:]
    cubes, planes, wide = ins[:4], ins[4:9], ins[9:]
    b = pl.program_id(0)
    eta_o[:] = eta[:]
    tu_o[:] = tu[:]
    tv_o[:] = tv[:]

    @pl.when(b == 0)
    def _():
        lev = iota((LP, NC), 0).astype(F32)
        kx = kvs[LAST, :NC]
        cor = correction(vbs[LAST, :NC], rsouth[0, one(NL), :], kx, dvs[LAST, :NC])
        vel = 0.5 * DT * only(lev < kx, rsouth[0] + cor)
        ft = vel * (rsouth[1] + rown[0, 0])
        fs = vel * (rsouth[2] + rown[0, 1])
        for k in range(NL):
            ct[k, LAST, :] = ft[one(k), :]
            cs[k, LAST, :] = fs[one(k), :]

    for half in range(2):
        sl = tile_rows(half)
        outs = [x.at[:, sl, :] for x in (uo, vo, to, so)]
        last = (b == NB // 2 - 1) if half else None
        finish_rows(last, *[x.at[half] for x in cubes], *[x[sl, :] for x in planes], *wide[half::2], rnorth, *outs, ct, cs)


def correction(mean, total, k, dz):
    deep = k * dz
    return (mean - total) / jnp.where(deep > 0, deep, 1.0)


def finish_rows(last, us, vs, t, s, cnt, su, sv, rwv, rev, ku, kv, du, dv, ub, vb, first, rnorth, uo, vo, to, so, ct, cs):
    row = iota(ROW, 0)
    lane = iota(TILE, 1)

    kx, ky = ku[:], kv[:, :NC]
    tot = jnp.concatenate([su, lane_to(rwv, 3 * NL, LN - 1)], axis=1)
    cx = correction(ub[:], tot, kx, du[:])
    cy = correction(vb[:, :NC], sv, ky, dv[:, :NC])
    fields = ((t, to, ct), (s, so, cs))

    def load(k):
        out = [lane_to(rwv, k, LN - 1)]
        for i in range(2):
            base = NL * (i + 1) + k
            out.append(jnp.where(lane == 0, lane_to(rev, base, 0), lane_to(rwv, base, LN - 1)))
        return out

    def east(k, halo):
        wide = [jnp.concatenate([f[0][k], h], axis=1) for f, h in zip(fields, halo[1:])]
        return halo[0], [x + from_east(x) for x in wide]

    def flux(k, arg):
        halo, sums = arg
        ue = only(k < kx, jnp.concatenate([us[k], halo], axis=1) + cx)
        uo[k] = ue[:, :NC]
        f = [(0.5 * DT) * ue * x for x in sums]
        return [(x - from_west(x))[:, :NC] for x in f]

    def store(k, div):
        ve = only(k < ky, vs[k] + cy)
        vo[k] = ve
        hy = (0.5 * DT) * ve
        for i, (x, out, carry) in enumerate(fields):
            own = x[k]
            north = first[0, i, one(k), :]
            if last is not None:
                north = jnp.where(last, rnorth[i, one(k), :], north)
            fy = hy * (own + up_row(own, north, row))
            new = own - (div[i] + (fy - down_row(fy, carry[k], row)))
            carry[k] = fy
            out[k] = only(k < cnt, new)

    skewed((load, east, flux, store), GROUP)


def finish(us, vs, tm, sm, first, kmt, geo, ub, vb, su, sv, rw, re, rnorth, rsouth, state):
    kv, dv = geo[1], geo[3]

    def rows(width):
        return pl.BlockSpec((16, width), lambda b: (b, 0))

    def pair(start):
        return [pl.BlockSpec(WIDE, lambda b, h=h: (start + 2 * b + h, 0)) for h in range(2)]

    def fixed(i):
        return pl.BlockSpec(WIDE, lambda b: (i, 0))

    ahead = [first_rows(lambda b: 2 * b + 1), first_rows(lambda b: jnp.minimum(2 * b + 2, NB - 1))]
    cube = pl.BlockSpec((NL, 16, NC), lambda b: (0, b, 0))
    south = [fixed(HT - 1)] * 2 + [fixed(0)]
    wide = [x for x in (*geo, ub, vb, first) for _ in range(2)]
    return pl.pallas_call(
        finish_kernel,
        grid=(NB // 2,),
        in_specs=[block_major(lambda b: b, 2)] * 4 + [rows(NC)] * 3 + [rows(LN)] * 2 + pair(HT) * 4 + pair(1) * 2 + ahead + south + [rows(NC)] * 3 + [whole(3, LP, NC)] * 2 + [first_rows(lambda b: 0)],
        out_specs=[rows(NC)] * 3 + [cube] * 4,
        out_shape=[shape(NR, NC)] * 3 + [shape(NL, NR, NC)] * 4,
        scratch_shapes=[VM(SLAB, F32)] * 2,
        compiler_params=pltpu.CompilerParams(vmem_limit_bytes=26 << 20),
        name="finish",
    )(us, vs, tm, sm, kmt, su, sv, rw, re, *wide, kv, dv, vb, *state, rnorth, rsouth, first)


def solution(mesh):
    sizes = mesh.shape["row"], mesh.shape["col"]

    def local_step(u, v, t, s, eta, tu, tv, depth, kmt, tide):
        u, v, t, s = (pltpu.with_memory_space_constraint(x, pltpu.HBM) for x in (u, v, t, s))
        tm, sm, pr, tke, tkw, trn, first, rw, re, rsouth, rnorth, corner, rown, *wide = tracers(sizes, t, s, u, v, kmt, depth, eta, tu, tv)
        geo, state = wide[:4], wide[4:]
        tm, sm = (pltpu.with_memory_space_constraint(x, pltpu.VMEM) for x in (tm, sm))
        first = pltpu.with_memory_space_constraint(first, pltpu.HBM)
        pr = pltpu.with_memory_space_constraint(pr, pltpu.HBM)
        us, vs, fx, fy, su, sv, uke, vrow = momentum(u, v, pr, first, geo, rw, re, rnorth, rsouth, rown, corner)
        eta_n, u_n, v_n, ub, vb, fw, fe, fsouth, fnorth = subcycles(sizes, *state, *geo, fx, fy, tide, uke, tke, tkw, vrow, trn, first)
        us = pltpu.with_memory_space_constraint(us, pltpu.VMEM)
        vs = pltpu.with_memory_space_constraint(vs, pltpu.HBM)
        return finish(us, vs, tm, sm, first, kmt, geo, ub, vb, su, sv, fw, fe, fnorth, fsouth, (eta_n, u_n, v_n))

    cube, plane = P(None, "row", "col"), P("row", "col")
    return jax.shard_map(
        local_step,
        mesh=mesh,
        in_specs=(cube,) * 4 + (plane,) * 5 + (P(None, None),),
        out_specs=(plane,) * 3 + (cube,) * 4,
        check_vma=False,
    )
```

```python
import functools

import jax
import jax.numpy as jnp
from jax import lax
from jax.experimental import pallas as pl
from jax.experimental.pallas import tpu as pltpu
from jax.sharding import PartitionSpec as P

NL = 41
NR = 96
NC = 512
LN = 128
LP = 48
HR = 40
ER = NR + 2 * HR
EC = NC + 128
NB = NR // 8
SUB = 36
GROUP = 2
HALF = 64
SIDES = (-1, 0, 1)
FIRST, LAST = slice(0, 1), slice(7, 8)
TILES = 3
DT = 4.0
DTB = DT / SUB
KV = 0.001
KT = 0.0005
F32 = jnp.float32
HT = HR // 8
ET = ER // 8
SLAB, ROW, WIDE, TILE = (NL, 8, NC), (8, NC), (8, EC), (8, LN)
VM = pltpu.VMEM


def only(mask, x):
    return jnp.where(mask, x, jnp.zeros_like(x))


def iota(shape, dim):
    return lax.broadcasted_iota(jnp.int32, shape, dim)


def whole(*shape):
    return pl.BlockSpec(shape, lambda *_: (0,) * len(shape))


def shape(*dims):
    return jax.ShapeDtypeStruct(dims, F32)


def one(k):
    return slice(k, k + 1)


def tile_rows(i):
    return slice(8 * i, 8 * (i + 1))


def from_west(x):
    return pltpu.roll(x, 1, axis=1)


def from_east(x):
    return pltpu.roll(x, x.shape[1] - 1, axis=1)


def lane_to(x, src, dst):
    shift = (dst - src) % LN
    return x if shift == 0 else pltpu.roll(x, shift, axis=1)


def up_row(x, nxt, row):
    return pltpu.roll(jnp.where(row == 0, nxt, x), 7, axis=0)


def down_row(x, prev, row):
    return pltpu.roll(jnp.where(row == 7, prev, x), 1, axis=0)


def skewed(stages, group, count=NL):
    blocks = [range(k, min(k + group, count)) for k in range(0, count, group)]
    held = {}
    for i in range(len(blocks) + len(stages) - 1):
        for n, stage in enumerate(stages):
            if 0 <= i - n < len(blocks):
                for k in blocks[i - n]:
                    held[k] = stage(k, held[k]) if n else stage(k)


def couple(count, thick, kappa):
    safe = jnp.where(count > 0, thick, 1.0)
    return DT * kappa / (safe * safe)


def pressure_step(t, s, wet, cum, thick):
    half = only(wet, 0.5 * (0.015 * (s - 1.0) - 0.02 * (t - 1.0)))
    mid = cum + half
    return thick * mid, mid + half


class Exchange:
    def __init__(self, sizes, send_sem, recv_sem):
        self.rows, self.cols = sizes
        self.row, self.col = lax.axis_index("row"), lax.axis_index("col")
        self.sems = send_sem, recv_sem
        self.used = 0

    def inside(self, drow):
        return (self.row + drow >= 0) & (self.row + drow < self.rows)

    def at(self, drow, dcol):
        return {"row": self.row + drow, "col": lax.rem(self.col + dcol + self.cols, self.cols)}

    def when(self, drow, action):
        if drow:
            pl.when(self.inside(drow))(action)
        else:
            action()

    def barrier(self):
        ready = pltpu.get_barrier_semaphore()
        for drow in SIDES:
            for dcol in SIDES:
                if drow or dcol:
                    self.when(drow, functools.partial(pl.semaphore_signal, ready, device_id=self.at(drow, dcol), device_id_type=pl.DeviceIdType.MESH))
        per_row = len(SIDES)
        known = [self.inside(drow).astype(jnp.int32) for drow in SIDES if drow]
        pl.semaphore_wait(ready, per_row - 1 + per_row * sum(known))

    def clear(self, plan):
        for _, dst, drow, _ in plan:
            if drow:

                @pl.when(jnp.logical_not(self.inside(-drow)))
                def _():
                    dst[:] = jnp.zeros(dst.shape, F32)

    def make(self, plan):
        out = []
        for src, dst, drow, dcol in plan:
            copy = pltpu.make_async_remote_copy(
                src_ref=src,
                dst_ref=dst,
                send_sem=self.sems[0].at[self.used],
                recv_sem=self.sems[1].at[self.used],
                device_id=self.at(drow, dcol),
                device_id_type=pl.DeviceIdType.MESH,
            )
            self.used += 1
            out.append((copy, drow))
        return out

    def start(self, copies):
        for copy, drow in copies:
            self.when(drow, copy.start)

    def wait(self, copies):
        for copy, drow in copies:
            self.when(drow, copy.wait_send)
            self.when(-drow, copy.wait_recv)


def pack_strips(pairs, to_west, to_east):
    lane = iota(TILE, 1)
    first, last = slice(0, LN), slice(NC - LN, NC)

    def turn(n):
        q, sl = n // NB, tile_rows(n % NB)
        b = pairs[q][-1]
        return pltpu.roll(b[sl, first], HALF, axis=1), pltpu.roll(b[sl, last], HALF, axis=1)

    def store(n, turned):
        q, sl = n // NB, tile_rows(n % NB)
        a = pairs[q][0]
        to_west[q, sl, :] = jnp.where(lane < HALF, a[sl, first], turned[0])
        to_east[q, sl, :] = jnp.where(lane < HALF, turned[1], a[sl, last])

    skewed((turn, store), NB, NB * len(pairs))


def strip_plan(to_west, to_east, strips):
    top, bottom = pl.ds(NR - HR, HR), pl.ds(0, HR)
    return [
        (to_east, strips[0], 0, 1),
        (to_west, strips[1], 0, -1),
        (to_east.at[:, top], strips[2], 1, 1),
        (to_west.at[:, top], strips[3], 1, -1),
        (to_east.at[:, bottom], strips[4], -1, 1),
        (to_west.at[:, bottom], strips[5], -1, -1),
    ]


def row_plan(planes, south, north):
    plan = []
    for i, x in enumerate(planes):
        plan.append((x.at[pl.ds(NR - HR, HR), :], south.at[i], 1, 0))
        plan.append((x.at[pl.ds(0, HR), :], north.at[i], -1, 0))
    return plan


def strip_scratch(n):
    return [VM((n, NR, LN), F32)] * 4 + [VM((n, HR, LN), F32)] * 4


def side(i, own, south, north):
    if i < HT:
        return south, tile_rows(i)
    return (own, tile_rows(i - HT)) if i < HT + NB else (north, tile_rows(i - HT - NB))


def halo_pair(i, q, strips):
    (w, e), sl = side(i, strips[:2], strips[2:4], strips[4:])
    lane = iota(TILE, 1)
    w, e = w[q, sl, :], e[q, sl, :]
    return jnp.where(lane < HALF, e, w), pltpu.roll(jnp.where(lane < HALF, w, e), HALF, axis=1)


def mix_tracers(t, s, cnt, depth, strips, tm, sm, pr, pke, pkw, tke, tkw, rs, gains):
    lane = iota(TILE, 1)
    thick = depth / jnp.maximum(cnt, 1).astype(F32)
    c = couple(cnt, thick, KT)
    zero = jnp.zeros(ROW, F32)
    cum = lower = pt = ps = zero
    keep = zero
    ae = aw = jnp.zeros(TILE, F32)
    u0, u3, v0, v3 = strips
    for k in range(NL):
        wet = k < cnt
        tk, sk = t[k], s[k]
        p, cum = pressure_step(tk, sk, wet, cum, thick)
        pr[k] = p
        for n, (x0, x3) in enumerate(((u0, u3), (v0, v3))):
            base = NL * n + k
            ae = jnp.where(lane == base, lane_to(x3[k], LN - 1, base), ae)
            aw = jnp.where(lane == base, lane_to(x0[k], 0, base), aw)
        aw = jnp.where(lane == 2 * NL + k, lane_to(p[:, :LN], 0, 2 * NL + k), aw)
        rs[2, one(k), :] = p[FIRST, :]
        upper = jnp.where(k + 1 < cnt, c, 0.0) if k + 1 < NL else zero
        top = 1.0 + lower * keep if k else jnp.ones_like(zero)
        inv = 1.0 / (top + upper)
        keep = top * inv
        gains[k] = upper * inv
        pt = (jnp.where(wet, tk, 0.0) + lower * pt) * inv
        ps = (jnp.where(wet, sk, 0.0) + lower * ps) * inv
        tm[k] = pt
        sm[k] = ps
        lower = upper
    pke[:] = ae
    pkw[:] = aw
    ae = aw = jnp.zeros(TILE, F32)
    bt = bs = zero
    for k in reversed(range(NL)):
        gain = gains[k]
        bt = tm[k] + gain * bt
        bs = sm[k] + gain * bs
        tm[k] = bt
        sm[k] = bs
        rs[0, one(k), :] = bt[FIRST, :]
        rs[1, one(k), :] = bs[FIRST, :]
        for x, base in ((bt, NL), (bs, 2 * NL)):
            ae = jnp.where(lane == base + k, lane_to(x[:, NC - LN :], LN - 1, base + k), ae)
            aw = jnp.where(lane == base + k, lane_to(x[:, :LN], 0, base + k), aw)
    tke[:] = ae
    tkw[:] = aw


def wide_geometry(planes, strips, south, north, outs):
    ku, kv, du, dv, *state = outs
    row = iota(WIDE, 0)

    def turn(i):
        return [halo_pair(i, q, strips) for q in range(3)]

    def build(i, halo):
        halo = [x for pair in halo for x in pair]
        vals = []
        for n in range(len(planes)):
            part, sl = side(i, planes[n], south.at[n], north.at[n])
            vals.append(jnp.concatenate([part[sl, :], halo[n]], axis=1))
        k, h = vals[:2]
        dz = h / jnp.maximum(k, 1.0)
        kv[tile_rows(i), :] = k
        dv[tile_rows(i), :] = dz
        return vals[2:], from_east(k), from_east(dz)

    def store(i, arg):
        vals, ke, dze = arg
        sl = tile_rows(i)
        hi = tile_rows(min(i + 1, ET - 1))
        k, dz = kv[sl, :], dv[sl, :]
        k_u, k_v = jnp.minimum(k, ke), jnp.minimum(k, up_row(k, kv[hi, :], row))
        dv[sl, :] = 0.5 * (dz + up_row(dz, dv[hi, :], row))
        du[sl, :] = 0.5 * (dz + dze)
        ku[sl, :] = k_u
        kv[sl, :] = k_v
        for out, x, wet in zip(state, vals, (k, k_u, k_v)):
            out[sl, :] = only(wet > 0, x)

    skewed((turn, build, store), TILES, ET)


def tracer_kernel(sizes, t, s, u0, u3, v0, v3, kc, hc, uf, ul, vf, vl, kmt, depth, eta, tu, tv, *rest):
    tm_b, sm_b, pr_b, tke, tkw, rn, rs_b, *rest = rest
    received, rown, wide, rest = rest[:5], rest[5], rest[6:13], rest[13:]
    gains, kf, pke, pkw, prn, prs, south, north, rw, re, rsouth, rnorth, corner, to_west, to_east, *strips, send_sem, recv_sem = rest
    b = pl.program_id(0)
    last = NB // 2 - 1
    net = Exchange(sizes, send_sem, recv_sem)
    planes = (kf, depth, eta, tu, tv)
    head = strip_plan(to_west, to_east, strips) + [(prn, rsouth, 1, 0)] + row_plan(planes, south, north)
    middle = [(prs, rnorth, -1, 0), (pke.at[pl.ds(0, 8), :], rw.at[pl.ds(NR, 8), :], -1, 1)]
    tail = [(pkw.at[pl.ds(NR - 8, 8), :], corner, 1, -1)]

    def piece(i):
        part = pl.ds(16 * i, 16)
        return net.make([(pke.at[part, :], rw.at[part, :], 0, 1), (pkw.at[part, :], re.at[part, :], 0, -1)])

    first_plan = head + middle + tail
    head, middle, tail = net.make(head), net.make(middle), net.make(tail)
    pieces = [piece(i) for i in range(last + 1)]

    @pl.when(b == 0)
    def _():
        kf[:] = kmt[:].astype(F32)
        pack_strips((planes[:2], planes[2:4], planes[4:]), to_west, to_east)
        prn[:] = jnp.zeros(prn.shape, F32)
        prs[:] = jnp.zeros(prs.shape, F32)
        for k in range(NL):
            for n, (lo, hi) in enumerate(((uf, ul), (vf, vl))):
                prn[n, one(k), :] = hi[k, LAST, :]
                prs[n, one(k), :] = lo[k, FIRST, :]
        net.clear(first_plan)
        net.barrier()
        net.start(head)

    for i in range(last):

        @pl.when(b == i + 1)
        def _():
            net.start(pieces[i])

    for half in range(2):
        sl = tile_rows(half)
        tm, sm, rs = tm_b.at[half], sm_b.at[half], rs_b.at[half]
        out = pl.ds(pl.multiple_of(16 * b + 8 * half, 8), 8)
        parts = [x.at[:, sl, :] for x in (t, s, u0, u3, v0, v3)]
        mix_tracers(*parts[:2], kc[sl, :], hc[sl, :], parts[2:], tm, sm, pr_b.at[half], pke.at[out, :], pkw.at[out, :], tke.at[sl, :], tkw.at[sl, :], rs, gains)

    @pl.when(b == 0)
    def _():
        prs[2] = rs_b[0, 2]
        net.start(middle)

    @pl.when(b == last)
    def _():
        net.start(pieces[last] + tail)
        for k in range(NL):
            rn[0, one(k), :] = tm[k, LAST, :]
            rn[1, one(k), :] = sm[k, LAST, :]
        rown[:] = prs[:]
        net.wait(head)
        wide_geometry(planes, strips, south, north, wide)
        net.wait(middle + tail)
        for copies in pieces:
            net.wait(copies)
        for out, x in zip(received, (rw, re, rsouth, rnorth, corner)):
            out[:] = x[:]


PACK = VM((NB,) + SLAB, F32)
PACK_HBM = pltpu.HBM((NB,) + SLAB, F32)


def block_major(f, n=1):
    return pl.BlockSpec((n,) + SLAB, lambda b: (f(b), 0, 0, 0))


def first_rows(f, n=1):
    return pl.BlockSpec((n, 3, LP, NC), lambda b: (f(b), 0, 0, 0))


def tracers(sizes, t, s, u, v, kmt, depth, eta, tu, tv):
    def cols(width, j):
        return pl.BlockSpec((NL, 16, width), lambda b: (0, b, j))

    def slab(i):
        return pl.BlockSpec(SLAB, lambda b: (0, i, 0))

    pack = block_major(lambda b: b, 2)
    plane = pl.BlockSpec((16, NC), lambda b: (b, 0))
    col = pl.BlockSpec((16, LN), lambda b: (b, 0))
    ends = [slab(0), slab(NB - 1)]
    edge = [(NR + 8, LN), (NR, LN), (2, LP, NC), (3, LP, NC), (8, LN)]
    extra = edge + [(3, LP, NC)] + [(ER, EC)] * 7
    sems = [pltpu.SemaphoreType.DMA((6 + 1 + 10 + 3 + NB,))] * 2
    rows = [VM((2, LP, NC), F32), VM((3, LP, NC), F32)] + [VM((5, HR, NC), F32)] * 2
    return pl.pallas_call(
        functools.partial(tracer_kernel, sizes),
        grid=(NB // 2,),
        in_specs=[cols(NC, 0)] * 2 + [cols(LN, 0), cols(LN, 3)] * 2 + [plane] * 2 + ends * 2 + [whole(NR, NC)] * 5,
        out_specs=[pack] * 3 + [col] * 2 + [whole(2, LP, NC), first_rows(lambda b: b, 2)] + [whole(*x) for x in extra],
        out_shape=[PACK] * 2 + [PACK_HBM] + [shape(NR, LN)] * 2 + [shape(2, LP, NC), pltpu.HBM((NB, 3, LP, NC), F32)] + [shape(*x) for x in extra],
        scratch_shapes=[VM(SLAB, F32), VM((NR, NC), F32)] + [VM((NR, LN), F32)] * 2 + rows + [VM(x, F32) for x in edge] + strip_scratch(3) + sems,
        compiler_params=pltpu.CompilerParams(collective_id=0, has_side_effects=True, vmem_limit_bytes=26 << 20),
        name="tracers",
    )(t, s, u, u, v, v, kmt, depth, u, u, v, v, kmt, depth, eta, tu, tv)


def solve_pair(src_a, src_b, ca, cb, na, nb, out_a, out_b, gain_a, gain_b):
    zero = jnp.zeros(ROW, F32)
    la = lb = pa = pb = wa = wb = zero
    for k in range(NL):
        ua = jnp.where(k + 1 < na, ca, 0.0) if k + 1 < NL else zero
        ub = jnp.where(k + 1 < nb, cb, 0.0) if k + 1 < NL else zero
        ta = 1.0 + la * wa if k else jnp.ones_like(zero)
        tb = 1.0 + lb * wb if k else jnp.ones_like(zero)
        ia = 1.0 / (ta + ua)
        ib = 1.0 / (tb + ub)
        wa, wb = ta * ia, tb * ib
        gain_a[k] = ua * ia
        gain_b[k] = ub * ib
        pa = (src_a[k] + la * pa) * ia
        pb = (src_b[k] + lb * pb) * ib
        src_a[k] = pa
        src_b[k] = pb
        la, lb = ua, ub
    xa = xb = sa = sb = zero
    for k in reversed(range(NL)):
        xa = src_a[k] + gain_a[k] * xa
        xb = src_b[k] + gain_b[k] * xb
        out_a[k] = xa
        out_b[k] = xb
        sa += xa
        sb += xb
    return sa, sb


def momentum_kernel(
    u, v, p_b, pfirst, kun, kvn, kux, kvx, du, dv, kus, kvs, rwn, ren, re, rnorth, rsouth, rown, corner,
    us_b, vs_b, fx, fy, su, sv, pke, vrow,
    cc, hh, srcu, srcv, gu, gv, ums, vms,
):
    step = pl.program_id(0)
    last = step == NB
    us, vs, p = us_b.at[0], vs_b.at[0], p_b.at[0]
    row = iota(ROW, 0)
    rowx = iota(WIDE, 0)
    lane = iota(TILE, 1)
    kxn, kyn = kun[:], kvn[:]
    rwv, rev = rwn[:], ren[:]

    def halos(k):
        hu = jnp.where(lane == 0, lane_to(rev, k, 0), lane_to(rwv, k, LN - 1))
        hv = jnp.where(lane == 0, lane_to(rev, NL + k, 0), lane_to(rwv, NL + k, LN - 1))
        return hu, hv

    def masked(k, uk, vk, halo):
        um = only(k < kxn, jnp.concatenate([uk, halo[0]], axis=1))
        return um, only(k < kyn, jnp.concatenate([vk, halo[1]], axis=1))

    @pl.when(step == 0)
    def _():
        for k in range(NL):
            ums[k], vms[k] = masked(k, u[k], v[k], halos(k))
        lev = iota((LP, NC), 0).astype(F32)
        lev1 = iota((LP, LN), 0)
        ks, kw = kus[LAST, :NC], kvs[LAST, :NC]
        s_u = only(lev < ks, rsouth[0])
        s_v = only(lev < kw, rsouth[1])
        pick = only(iota((LP, LN), 1) == lev1 + NL, corner[LAST, :])
        edge = jnp.sum(pick, axis=1, keepdims=True)
        edge = only(lev[:, :1] < kvs[LAST, one(NC)], edge)
        s_ve = jnp.where(iota((LP, NC), 1) == NC - 1, edge, from_east(s_v))
        u_0 = only(lev < kxn[FIRST, :NC], rown[0])
        v_0 = only(lev < kyn[FIRST, :NC], rown[1])
        c_s = 0.25 * ((s_v + s_ve) * (s_u + u_0))
        h_s = s_v + v_0
        h_s = 0.25 * (h_s * h_s) + rown[2]
        for k in range(NL):
            cc[k, LAST, :] = c_s[one(k), :]
            hh[k, LAST, :] = h_s[one(k), :]

    @pl.when(step > 0)
    def _():
        kx, ky = kux[:], kvx[:]
        pev = re[:]
        total = [jnp.zeros(ROW, F32)] * 2

        def edge(k):
            return halos(k) + (lane_to(pev, 2 * NL + k, 0),)

        def shift(k, halo):
            um, vm = ums[k], vms[k]
            uk = jnp.where(last, rnorth[0, one(k), :], u[k])
            vk = jnp.where(last, rnorth[1, one(k), :], v[k])
            pe = jnp.concatenate([p[k], halo[2]], axis=1)
            return masked(k, uk, vk, halo), pe, from_west(um), from_east(vm)

        def flux(k, arg):
            new, pe, u_w, v_e = arg
            um, vm = ums[k], vms[k]
            c = 0.25 * ((vm + v_e) * (um + up_row(um, new[0], rowx)))
            g = u_w + um
            g = 0.25 * (g * g) + pe
            c5 = c[:, :NC]
            return new, from_east(g)[:, :NC] - g[:, :NC], c5, c5 - from_west(c)[:, :NC]

        def tend(k, arg):
            new, dx, c5, dc = arg
            u5, v5, pk = ums[k, :, :NC], vms[k, :, :NC], p[k]
            north = jnp.where(last, rnorth[2, one(k), :], pfirst[0, 2, one(k), :])
            h = v5 + up_row(v5, new[1][:, :NC], row)
            h = 0.25 * (h * h) + up_row(pk, north, row)
            tu = only(k < kx, dx + (c5 - down_row(c5, cc[k], row)))
            tv = only(k < ky, (h - down_row(h, hh[k], row)) + dc)
            total[0] += tu
            total[1] += tv
            srcu[k] = u5 - DT * tu
            srcv[k] = v5 - DT * tv
            cc[k] = c5
            hh[k] = h
            ums[k], vms[k] = new

        skewed((edge, shift, flux, tend), GROUP)
        dzu, dzv = du[:], dv[:]
        fx[:] = -dzu * total[0]
        fy[:] = -dzv * total[1]
        sa, sb = solve_pair(srcu, srcv, couple(kx, dzu, KV), couple(ky, dzv, KV), kx, ky, us, vs, gu, gv)
        sa, sb = dzu * sa, dzv * sb
        su[:] = sa
        sv[:] = sb
        ae = jnp.zeros(TILE, F32)
        for k in range(NL):
            ae = jnp.where(lane == k, lane_to(us[k, :, NC - LN :], LN - 1, k), ae)
        pke[:] = jnp.where(lane == 3 * NL, lane_to(sa[:, NC - LN :], LN - 1, 3 * NL), ae)

        @pl.when(last)
        def _():
            for k in range(NL):
                vrow[one(k), :] = vs[k, LAST, :]
            vrow[one(NL), :] = sb[LAST, :]
            vrow[NL + 1 : LP, :] = jnp.zeros((LP - NL - 1, NC), F32)


def momentum(u, v, p, first, geo, rw, re, rnorth, rsouth, rown, corner):
    ku, kv, du, dv = geo

    def this(b):
        return jnp.maximum(b, 1) - 1

    def ahead(b):
        return jnp.minimum(b, NB - 1)

    cube = pl.BlockSpec(SLAB, lambda b: (0, ahead(b), 0))
    pack = block_major(this)
    near = pl.BlockSpec(ROW, lambda b: (HT + this(b), 0))
    widn = pl.BlockSpec(WIDE, lambda b: (HT + b, 0))
    wids = pl.BlockSpec(WIDE, lambda b: (HT - 1, 0))
    plane = pl.BlockSpec(ROW, lambda b: (this(b), 0))
    col = pl.BlockSpec(TILE, lambda b: (this(b), 0))
    colw = pl.BlockSpec(TILE, lambda b: (b, 0))
    cole = pl.BlockSpec(TILE, lambda b: (ahead(b), 0))
    flat = jax.ShapeDtypeStruct((NR, NC), F32)

    def rows(n):
        return pl.BlockSpec((n, LP, NC), lambda b: (0, 0, 0))

    return pl.pallas_call(
        momentum_kernel,
        grid=(NB + 1,),
        in_specs=[cube, cube, pack, first_rows(ahead), widn, widn, near, near, near, near, wids, wids, colw, cole, col, rows(3), rows(2), rows(3), pl.BlockSpec(TILE, lambda b: (0, 0))],
        out_specs=[pack, pack, plane, plane, plane, plane, col, pl.BlockSpec((LP, NC), lambda b: (0, 0))],
        out_shape=[PACK, PACK_HBM, flat, flat, flat, flat, jax.ShapeDtypeStruct((NR, LN), F32), jax.ShapeDtypeStruct((LP, NC), F32)],
        scratch_shapes=[VM(SLAB, F32)] * 6 + [VM((NL,) + WIDE, F32)] * 2,
        compiler_params=pltpu.CompilerParams(vmem_limit_bytes=22 << 20),
        name="momentum",
    )(u, v, p, first, ku, kv, ku, kv, du, dv, ku, kv, rw, re, re, rnorth, rsouth, rown, corner)


def subcycle_kernel(
    sizes, eta_i, tu_i, tv_i, ku, kv, du, dv, fx, fy, tide, uke, tke, tkw, vrow, trn, trs,
    eta_o, u_o, v_o, ub_o, vb_o, fw, fe, fsouth, fnorth,
    eta, tu, tv, cu, cv, fu, fv, ub, vb, edge, south, north, *rest,
):
    to_west, to_east, *strips, send_sem, recv_sem = rest
    net = Exchange(sizes, send_sem, recv_sem)
    edge[:] = uke[:] + tke[:]
    pack_strips(((fx, fy),), to_west, to_east)
    plan = strip_plan(to_west, to_east, strips) + row_plan((fx, fy), south, north)
    late = [
        (edge, fw, 0, 1),
        (tkw, fe, 0, -1),
        (vrow, fsouth.at[0], 1, 0),
        (trn, fsouth.at[pl.ds(1, 2)], 1, 0),
        (trs.at[0], fnorth, -1, 0),
    ]
    net.clear(plan + late)
    net.barrier()
    plan, late = net.make(plan), net.make(late)
    net.start(plan + late)
    row = iota(WIDE, 0)
    zero = jnp.zeros(WIDE, F32)
    ub[:] = jnp.zeros(ub.shape, F32)
    vb[:] = jnp.zeros(vb.shape, F32)
    eta[:] = eta_i[:]
    tu[:] = tu_i[:]
    tv[:] = tv_i[:]
    cu[:] = DTB * (ku[:] * du[:])
    cv[:] = DTB * (kv[:] * dv[:])
    net.wait(plan)

    def turn(i):
        return halo_pair(i, 0, strips)

    def build(i, halo):
        sl = tile_rows(i)
        for n, (x, out, wet) in enumerate(((fx, fu, ku), (fy, fv, kv))):
            part, rows = side(i, x, south.at[n], north.at[n])
            out[sl, :] = only(wet[sl, :] > 0, DTB * jnp.concatenate([part[rows, :], halo[n]], axis=1))

    skewed((turn, build), TILES, ET)
    norm = 6.0 / (SUB * (SUB + 1) * (SUB + 2))

    def stage(first, last, lo, hi):
        def step(n, _):
            tx, ty = tide[0, n], tide[1, n]
            w = norm * ((n + 1) * (SUB - n)).astype(F32)

            def west(i):
                return from_west(tu[tile_rows(i), :])

            def surface(i, u_w):
                sl = tile_rows(i)
                vn = tv[sl, :]
                south = tv[tile_rows(i - 1), :] if i else zero
                e = eta[sl, :] - DTB * ((tu[sl, :] - u_w) + (vn - down_row(vn, south, row)))
                eta[sl, :] = e
                return from_east(e)

            def update(i, e_e):
                sl = tile_rows(i)
                e = eta[sl, :]
                un = tu[sl, :] + (cu[sl, :] * (tx - (e_e - e)) + fu[sl, :])
                tu[sl, :] = un
                if lo_bar <= i < hi_bar:
                    ub[sl, :] = ub[sl, :] + w * un
                if i > lo:
                    north(i - 1, e, ty, w)

            skewed((lambda i: west(lo + i), lambda i, x: surface(lo + i, x), lambda i, x: update(lo + i, x)), TILES, hi - lo)
            north(hi - 1, eta[tile_rows(hi - 1), :], ty, w)
            return 0

        lax.fori_loop(first, last, step, 0)

    lo_bar, hi_bar = HT - 1, HT + NB

    def north(i, ahead, ty, w):
        sl = tile_rows(i)
        e = eta[sl, :]
        x = tv[sl, :] + (cv[sl, :] * (ty - (up_row(e, ahead, row) - e)) + fv[sl, :])
        tv[sl, :] = x
        if lo_bar <= i < hi_bar:
            vb[sl, :] = vb[sl, :] + w * x

    for s in range(0, SUB, 8):
        stage(s, min(s + 8, SUB), s // 8, ET - s // 8)
    eta_o[:] = eta[HR : HR + NR, :NC]
    u_o[:] = tu[HR : HR + NR, :NC]
    v_o[:] = tv[HR : HR + NR, :NC]
    ub_o[:] = ub[HR - 8 : HR + NR, :]
    vb_o[:] = vb[HR - 8 : HR + NR, :]
    net.wait(late)


def subcycles(sizes, *args):
    vm = pl.BlockSpec(memory_space=VM)
    outs = [shape(NR, NC)] * 3 + [shape(NR + 8, EC)] * 2 + [shape(NR, LN)] * 2 + [shape(3, LP, NC)] * 2
    sems = [pltpu.SemaphoreType.DMA((6 + 4 + 5,))] * 2
    wide = [VM((ER, EC), F32)] * 9
    return pl.pallas_call(
        functools.partial(subcycle_kernel, sizes),
        in_specs=[vm] * 9 + [pl.BlockSpec(memory_space=pltpu.SMEM)] + [vm] * 5 + [pl.BlockSpec(memory_space=pl.ANY)],
        out_specs=[vm] * len(outs),
        out_shape=outs,
        scratch_shapes=wide + [VM((NR, LN), F32)] + [VM((2, HR, NC), F32)] * 2 + strip_scratch(1) + sems,
        compiler_params=pltpu.CompilerParams(collective_id=1, has_side_effects=True, vmem_limit_bytes=22 << 20),
        name="subcycles",
    )(*args)


def finish_kernel(*refs):
    ins, kvs, dvs, vbs, eta, tu, tv, rnorth, rsouth, rown, eta_o, tu_o, tv_o, uo, vo, to, so, ct, cs = refs[:23], *refs[23:]
    cubes, planes, wide = ins[:4], ins[4:9], ins[9:]
    b = pl.program_id(0)
    eta_o[:] = eta[:]
    tu_o[:] = tu[:]
    tv_o[:] = tv[:]

    @pl.when(b == 0)
    def _():
        lev = iota((LP, NC), 0).astype(F32)
        kx = kvs[LAST, :NC]
        cor = correction(vbs[LAST, :NC], rsouth[0, one(NL), :], kx, dvs[LAST, :NC])
        vel = 0.5 * DT * only(lev < kx, rsouth[0] + cor)
        ft = vel * (rsouth[1] + rown[0, 0])
        fs = vel * (rsouth[2] + rown[0, 1])
        for k in range(NL):
            ct[k, LAST, :] = ft[one(k), :]
            cs[k, LAST, :] = fs[one(k), :]

    for half in range(2):
        sl = tile_rows(half)
        outs = [x.at[:, sl, :] for x in (uo, vo, to, so)]
        last = (b == NB // 2 - 1) if half else None
        finish_rows(last, *[x.at[half] for x in cubes], *[x[sl, :] for x in planes], *wide[half::2], rnorth, *outs, ct, cs)


def correction(mean, total, k, dz):
    deep = k * dz
    return (mean - total) / jnp.where(deep > 0, deep, 1.0)


def finish_rows(last, us, vs, t, s, cnt, su, sv, rwv, rev, ku, kv, du, dv, ub, vb, first, rnorth, uo, vo, to, so, ct, cs):
    row = iota(ROW, 0)
    lane = iota(TILE, 1)

    kx, ky = ku[:], kv[:, :NC]
    tot = jnp.concatenate([su, lane_to(rwv, 3 * NL, LN - 1)], axis=1)
    cx = correction(ub[:], tot, kx, du[:])
    cy = correction(vb[:, :NC], sv, ky, dv[:, :NC])
    fields = ((t, to, ct), (s, so, cs))

    def load(k):
        out = [lane_to(rwv, k, LN - 1)]
        for i in range(2):
            base = NL * (i + 1) + k
            out.append(jnp.where(lane == 0, lane_to(rev, base, 0), lane_to(rwv, base, LN - 1)))
        return out

    def east(k, halo):
        wide = [jnp.concatenate([f[0][k], h], axis=1) for f, h in zip(fields, halo[1:])]
        return halo[0], [x + from_east(x) for x in wide]

    def flux(k, arg):
        halo, sums = arg
        ue = only(k < kx, jnp.concatenate([us[k], halo], axis=1) + cx)
        uo[k] = ue[:, :NC]
        f = [(0.5 * DT) * ue * x for x in sums]
        return [(x - from_west(x))[:, :NC] for x in f]

    def store(k, div):
        ve = only(k < ky, vs[k] + cy)
        vo[k] = ve
        hy = (0.5 * DT) * ve
        for i, (x, out, carry) in enumerate(fields):
            own = x[k]
            north = first[0, i, one(k), :]
            if last is not None:
                north = jnp.where(last, rnorth[i, one(k), :], north)
            fy = hy * (own + up_row(own, north, row))
            new = own - (div[i] + (fy - down_row(fy, carry[k], row)))
            carry[k] = fy
            out[k] = only(k < cnt, new)

    skewed((load, east, flux, store), GROUP)


def finish(us, vs, tm, sm, first, kmt, geo, ub, vb, su, sv, rw, re, rnorth, rsouth, state):
    kv, dv = geo[1], geo[3]

    def rows(width):
        return pl.BlockSpec((16, width), lambda b: (b, 0))

    def pair(start):
        return [pl.BlockSpec(WIDE, lambda b, h=h: (start + 2 * b + h, 0)) for h in range(2)]

    def fixed(i):
        return pl.BlockSpec(WIDE, lambda b: (i, 0))

    ahead = [first_rows(lambda b: 2 * b + 1), first_rows(lambda b: jnp.minimum(2 * b + 2, NB - 1))]
    cube = pl.BlockSpec((NL, 16, NC), lambda b: (0, b, 0))
    south = [fixed(HT - 1)] * 2 + [fixed(0)]
    wide = [x for x in (*geo, ub, vb, first) for _ in range(2)]
    return pl.pallas_call(
        finish_kernel,
        grid=(NB // 2,),
        in_specs=[block_major(lambda b: b, 2)] * 4 + [rows(NC)] * 3 + [rows(LN)] * 2 + pair(HT) * 4 + pair(1) * 2 + ahead + south + [rows(NC)] * 3 + [whole(3, LP, NC)] * 2 + [first_rows(lambda b: 0)],
        out_specs=[rows(NC)] * 3 + [cube] * 4,
        out_shape=[shape(NR, NC)] * 3 + [shape(NL, NR, NC)] * 4,
        scratch_shapes=[VM(SLAB, F32)] * 2,
        compiler_params=pltpu.CompilerParams(vmem_limit_bytes=26 << 20),
        name="finish",
    )(us, vs, tm, sm, kmt, su, sv, rw, re, *wide, kv, dv, vb, *state, rnorth, rsouth, first)


def solution(mesh):
    sizes = mesh.shape["row"], mesh.shape["col"]

    def local_step(u, v, t, s, eta, tu, tv, depth, kmt, tide):
        u, v, t, s, eta, tu, tv, depth, kmt = (pltpu.with_memory_space_constraint(x, pltpu.HBM) for x in (u, v, t, s, eta, tu, tv, depth, kmt))
        tm, sm, pr, tke, tkw, trn, first, rw, re, rsouth, rnorth, corner, rown, *wide = tracers(sizes, t, s, u, v, kmt, depth, eta, tu, tv)
        geo, state = wide[:4], wide[4:]
        tm, sm = (pltpu.with_memory_space_constraint(x, pltpu.VMEM) for x in (tm, sm))
        first = pltpu.with_memory_space_constraint(first, pltpu.HBM)
        pr = pltpu.with_memory_space_constraint(pr, pltpu.HBM)
        us, vs, fx, fy, su, sv, uke, vrow = momentum(u, v, pr, first, geo, rw, re, rnorth, rsouth, rown, corner)
        eta_n, u_n, v_n, ub, vb, fw, fe, fsouth, fnorth = subcycles(sizes, *state, *geo, fx, fy, tide.T, uke, tke, tkw, vrow, trn, first)
        us = pltpu.with_memory_space_constraint(us, pltpu.VMEM)
        vs = pltpu.with_memory_space_constraint(vs, pltpu.HBM)
        return finish(us, vs, tm, sm, first, kmt, geo, ub, vb, su, sv, fw, fe, fnorth, fsouth, (eta_n, u_n, v_n))

    cube, plane = P(None, "row", "col"), P("row", "col")
    return jax.shard_map(
        local_step,
        mesh=mesh,
        in_specs=(cube,) * 4 + (plane,) * 5 + (P(None, None),),
        out_specs=(plane,) * 3 + (cube,) * 4,
        check_vma=False,
    )
```

```python
import functools

import jax
import jax.numpy as jnp
from jax import lax
from jax.experimental import pallas as pl
from jax.experimental.pallas import tpu as pltpu
from jax.sharding import PartitionSpec as P

NL = 41
NR = 96
NC = 512
LN = 128
LP = 48
HR = 40
ER = NR + 2 * HR
EC = NC + 128
NB = NR // 8
SUB = 36
GROUP_M = 2
GROUP_F = 3
HALF = 64
SIDES = (-1, 0, 1)
FIRST, LAST = slice(0, 1), slice(7, 8)
TILES = 3
DT = 4.0
DTB = DT / SUB
KV = 0.001
KT = 0.0005
F32 = jnp.float32
HT = HR // 8
ET = ER // 8
SLAB, ROW, WIDE, TILE = (NL, 8, NC), (8, NC), (8, EC), (8, LN)
VM = pltpu.VMEM


def only(mask, x):
    return jnp.where(mask, x, jnp.zeros_like(x))


def iota(shape, dim):
    return lax.broadcasted_iota(jnp.int32, shape, dim)


def whole(*shape):
    return pl.BlockSpec(shape, lambda *_: (0,) * len(shape))


def shape(*dims):
    return jax.ShapeDtypeStruct(dims, F32)


def one(k):
    return slice(k, k + 1)


def tile_rows(i):
    return slice(8 * i, 8 * (i + 1))


def from_west(x):
    return pltpu.roll(x, 1, axis=1)


def from_east(x):
    return pltpu.roll(x, x.shape[1] - 1, axis=1)


def lane_to(x, src, dst):
    shift = (dst - src) % LN
    return x if shift == 0 else pltpu.roll(x, shift, axis=1)


def up_row(x, nxt, row):
    return pltpu.roll(jnp.where(row == 0, nxt, x), 7, axis=0)


def down_row(x, prev, row):
    return pltpu.roll(jnp.where(row == 7, prev, x), 1, axis=0)


def skewed(stages, group, count=NL):
    blocks = [range(k, min(k + group, count)) for k in range(0, count, group)]
    held = {}
    for i in range(len(blocks) + len(stages) - 1):
        for n, stage in enumerate(stages):
            if 0 <= i - n < len(blocks):
                for k in blocks[i - n]:
                    held[k] = stage(k, held[k]) if n else stage(k)


def couple(count, thick, kappa):
    safe = jnp.where(count > 0, thick, 1.0)
    return DT * kappa / (safe * safe)


def pressure_step(t, s, wet, cum, thick):
    half = only(wet, 0.5 * (0.015 * (s - 1.0) - 0.02 * (t - 1.0)))
    mid = cum + half
    return thick * mid, mid + half


class Exchange:
    def __init__(self, sizes, send_sem, recv_sem):
        self.rows, self.cols = sizes
        self.row, self.col = lax.axis_index("row"), lax.axis_index("col")
        self.sems = send_sem, recv_sem
        self.used = 0

    def inside(self, drow):
        return (self.row + drow >= 0) & (self.row + drow < self.rows)

    def at(self, drow, dcol):
        return {"row": self.row + drow, "col": lax.rem(self.col + dcol + self.cols, self.cols)}

    def when(self, drow, action):
        if drow:
            pl.when(self.inside(drow))(action)
        else:
            action()

    def barrier(self):
        ready = pltpu.get_barrier_semaphore()
        for drow in SIDES:
            for dcol in SIDES:
                if drow or dcol:
                    self.when(drow, functools.partial(pl.semaphore_signal, ready, device_id=self.at(drow, dcol), device_id_type=pl.DeviceIdType.MESH))
        per_row = len(SIDES)
        known = [self.inside(drow).astype(jnp.int32) for drow in SIDES if drow]
        pl.semaphore_wait(ready, per_row - 1 + per_row * sum(known))

    def clear(self, plan):
        for _, dst, drow, _ in plan:
            if drow:

                @pl.when(jnp.logical_not(self.inside(-drow)))
                def _():
                    dst[:] = jnp.zeros(dst.shape, F32)

    def make(self, plan):
        out = []
        for src, dst, drow, dcol in plan:
            copy = pltpu.make_async_remote_copy(
                src_ref=src,
                dst_ref=dst,
                send_sem=self.sems[0].at[self.used],
                recv_sem=self.sems[1].at[self.used],
                device_id=self.at(drow, dcol),
                device_id_type=pl.DeviceIdType.MESH,
            )
            self.used += 1
            out.append((copy, drow))
        return out

    def start(self, copies):
        for copy, drow in copies:
            self.when(drow, copy.start)

    def wait(self, copies):
        for copy, drow in copies:
            self.when(drow, copy.wait_send)
            self.when(-drow, copy.wait_recv)


def pack_strips(pairs, to_west, to_east):
    lane = iota(TILE, 1)
    first, last = slice(0, LN), slice(NC - LN, NC)

    def turn(n):
        q, sl = n // NB, tile_rows(n % NB)
        b = pairs[q][-1]
        return pltpu.roll(b[sl, first], HALF, axis=1), pltpu.roll(b[sl, last], HALF, axis=1)

    def store(n, turned):
        q, sl = n // NB, tile_rows(n % NB)
        a = pairs[q][0]
        to_west[q, sl, :] = jnp.where(lane < HALF, a[sl, first], turned[0])
        to_east[q, sl, :] = jnp.where(lane < HALF, turned[1], a[sl, last])

    skewed((turn, store), NB, NB * len(pairs))


def strip_plan(to_west, to_east, strips):
    top, bottom = pl.ds(NR - HR, HR), pl.ds(0, HR)
    return [
        (to_east, strips[0], 0, 1),
        (to_west, strips[1], 0, -1),
        (to_east.at[:, top], strips[2], 1, 1),
        (to_west.at[:, top], strips[3], 1, -1),
        (to_east.at[:, bottom], strips[4], -1, 1),
        (to_west.at[:, bottom], strips[5], -1, -1),
    ]


def row_plan(planes, south, north):
    plan = []
    for i, x in enumerate(planes):
        plan.append((x.at[pl.ds(NR - HR, HR), :], south.at[i], 1, 0))
        plan.append((x.at[pl.ds(0, HR), :], north.at[i], -1, 0))
    return plan


def strip_scratch(n):
    return [VM((n, NR, LN), F32)] * 4 + [VM((n, HR, LN), F32)] * 4


def side(i, own, south, north):
    if i < HT:
        return south, tile_rows(i)
    return (own, tile_rows(i - HT)) if i < HT + NB else (north, tile_rows(i - HT - NB))


def halo_pair(i, q, strips):
    (w, e), sl = side(i, strips[:2], strips[2:4], strips[4:])
    lane = iota(TILE, 1)
    w, e = w[q, sl, :], e[q, sl, :]
    return jnp.where(lane < HALF, e, w), pltpu.roll(jnp.where(lane < HALF, w, e), HALF, axis=1)


def mix_tracers(t, s, cnt, depth, strips, tm, sm, pr, pke, pkw, tke, tkw, rs, gains):
    lane = iota(TILE, 1)
    thick = depth / jnp.maximum(cnt, 1).astype(F32)
    c = couple(cnt, thick, KT)
    zero = jnp.zeros(ROW, F32)
    cum = lower = pt = ps = zero
    keep = zero
    ae = aw = jnp.zeros(TILE, F32)
    u0, u3, v0, v3 = strips
    for k in range(NL):
        wet = k < cnt
        tk, sk = t[k], s[k]
        p, cum = pressure_step(tk, sk, wet, cum, thick)
        pr[k] = p
        for n, (x0, x3) in enumerate(((u0, u3), (v0, v3))):
            base = NL * n + k
            ae = jnp.where(lane == base, lane_to(x3[k], LN - 1, base), ae)
            aw = jnp.where(lane == base, lane_to(x0[k], 0, base), aw)
        aw = jnp.where(lane == 2 * NL + k, lane_to(p[:, :LN], 0, 2 * NL + k), aw)
        rs[2, one(k), :] = p[FIRST, :]
        upper = jnp.where(k + 1 < cnt, c, 0.0) if k + 1 < NL else zero
        top = 1.0 + lower * keep if k else jnp.ones_like(zero)
        inv = 1.0 / (top + upper)
        keep = top * inv
        gains[k] = upper * inv
        pt = (jnp.where(wet, tk, 0.0) + lower * pt) * inv
        ps = (jnp.where(wet, sk, 0.0) + lower * ps) * inv
        tm[k] = pt
        sm[k] = ps
        lower = upper
    pke[:] = ae
    pkw[:] = aw
    ae = aw = jnp.zeros(TILE, F32)
    bt = bs = zero
    for k in reversed(range(NL)):
        gain = gains[k]
        bt = tm[k] + gain * bt
        bs = sm[k] + gain * bs
        tm[k] = bt
        sm[k] = bs
        rs[0, one(k), :] = bt[FIRST, :]
        rs[1, one(k), :] = bs[FIRST, :]
        for x, base in ((bt, NL), (bs, 2 * NL)):
            ae = jnp.where(lane == base + k, lane_to(x[:, NC - LN :], LN - 1, base + k), ae)
            aw = jnp.where(lane == base + k, lane_to(x[:, :LN], 0, base + k), aw)
    tke[:] = ae
    tkw[:] = aw


def wide_geometry(planes, strips, south, north, outs):
    ku, kv, du, dv, *state = outs
    row = iota(WIDE, 0)

    def turn(i):
        return [halo_pair(i, q, strips) for q in range(3)]

    def build(i, halo):
        halo = [x for pair in halo for x in pair]
        vals = []
        for n in range(len(planes)):
            part, sl = side(i, planes[n], south.at[n], north.at[n])
            vals.append(jnp.concatenate([part[sl, :], halo[n]], axis=1))
        k, h = vals[:2]
        dz = h / jnp.maximum(k, 1.0)
        kv[tile_rows(i), :] = k
        dv[tile_rows(i), :] = dz
        return vals[2:], from_east(k), from_east(dz)

    def store(i, arg):
        vals, ke, dze = arg
        sl = tile_rows(i)
        hi = tile_rows(min(i + 1, ET - 1))
        k, dz = kv[sl, :], dv[sl, :]
        k_u, k_v = jnp.minimum(k, ke), jnp.minimum(k, up_row(k, kv[hi, :], row))
        dv[sl, :] = 0.5 * (dz + up_row(dz, dv[hi, :], row))
        du[sl, :] = 0.5 * (dz + dze)
        ku[sl, :] = k_u
        kv[sl, :] = k_v
        for out, x, wet in zip(state, vals, (k, k_u, k_v)):
            out[sl, :] = only(wet > 0, x)

    skewed((turn, build, store), TILES, ET)


def tracer_kernel(sizes, t, s, u0, u3, v0, v3, kc, hc, uf, ul, vf, vl, kmt, depth, eta, tu, tv, *rest):
    tm_b, sm_b, pr_b, tke, tkw, rn, rs_b, *rest = rest
    received, rown, wide, rest = rest[:5], rest[5], rest[6:13], rest[13:]
    gains, kf, pke, pkw, prn, prs, south, north, rw, re, rsouth, rnorth, corner, to_west, to_east, *strips, send_sem, recv_sem = rest
    b = pl.program_id(0)
    last = NB // 2 - 1
    net = Exchange(sizes, send_sem, recv_sem)
    planes = (kf, depth, eta, tu, tv)
    head = strip_plan(to_west, to_east, strips) + [(prn, rsouth, 1, 0)] + row_plan(planes, south, north)
    middle = [(prs, rnorth, -1, 0), (pke.at[pl.ds(0, 8), :], rw.at[pl.ds(NR, 8), :], -1, 1)]
    tail = [(pkw.at[pl.ds(NR - 8, 8), :], corner, 1, -1)]

    def piece(i):
        part = pl.ds(16 * i, 16)
        return net.make([(pke.at[part, :], rw.at[part, :], 0, 1), (pkw.at[part, :], re.at[part, :], 0, -1)])

    first_plan = head + middle + tail
    head, middle, tail = net.make(head), net.make(middle), net.make(tail)
    pieces = [piece(i) for i in range(last + 1)]

    @pl.when(b == 0)
    def _():
        kf[:] = kmt[:].astype(F32)
        pack_strips((planes[:2], planes[2:4], planes[4:]), to_west, to_east)
        prn[:] = jnp.zeros(prn.shape, F32)
        prs[:] = jnp.zeros(prs.shape, F32)
        for k in range(NL):
            for n, (lo, hi) in enumerate(((uf, ul), (vf, vl))):
                prn[n, one(k), :] = hi[k, LAST, :]
                prs[n, one(k), :] = lo[k, FIRST, :]
        net.clear(first_plan)
        net.barrier()
        net.start(head)

    for i in range(last):

        @pl.when(b == i + 1)
        def _():
            net.start(pieces[i])

    for half in range(2):
        sl = tile_rows(half)
        tm, sm, rs = tm_b.at[half], sm_b.at[half], rs_b.at[half]
        out = pl.ds(pl.multiple_of(16 * b + 8 * half, 8), 8)
        parts = [x.at[:, sl, :] for x in (t, s, u0, u3, v0, v3)]
        mix_tracers(*parts[:2], kc[sl, :], hc[sl, :], parts[2:], tm, sm, pr_b.at[half], pke.at[out, :], pkw.at[out, :], tke.at[sl, :], tkw.at[sl, :], rs, gains)

    @pl.when(b == 0)
    def _():
        prs[2] = rs_b[0, 2]
        net.start(middle)

    @pl.when(b == last)
    def _():
        net.start(pieces[last] + tail)
        for k in range(NL):
            rn[0, one(k), :] = tm[k, LAST, :]
            rn[1, one(k), :] = sm[k, LAST, :]
        rown[:] = prs[:]
        net.wait(head)
        wide_geometry(planes, strips, south, north, wide)
        net.wait(middle + tail)
        for copies in pieces:
            net.wait(copies)
        for out, x in zip(received, (rw, re, rsouth, rnorth, corner)):
            out[:] = x[:]


PACK = VM((NB,) + SLAB, F32)
PACK_HBM = pltpu.HBM((NB,) + SLAB, F32)


def block_major(f, n=1):
    return pl.BlockSpec((n,) + SLAB, lambda b: (f(b), 0, 0, 0))


def first_rows(f, n=1):
    return pl.BlockSpec((n, 3, LP, NC), lambda b: (f(b), 0, 0, 0))


def tracers(sizes, t, s, u, v, kmt, depth, eta, tu, tv):
    def cols(width, j):
        return pl.BlockSpec((NL, 16, width), lambda b: (0, b, j))

    def slab(i):
        return pl.BlockSpec(SLAB, lambda b: (0, i, 0))

    pack = block_major(lambda b: b, 2)
    plane = pl.BlockSpec((16, NC), lambda b: (b, 0))
    col = pl.BlockSpec((16, LN), lambda b: (b, 0))
    ends = [slab(0), slab(NB - 1)]
    edge = [(NR + 8, LN), (NR, LN), (2, LP, NC), (3, LP, NC), (8, LN)]
    extra = edge + [(3, LP, NC)] + [(ER, EC)] * 7
    sems = [pltpu.SemaphoreType.DMA((6 + 1 + 10 + 3 + NB,))] * 2
    rows = [VM((2, LP, NC), F32), VM((3, LP, NC), F32)] + [VM((5, HR, NC), F32)] * 2
    return pl.pallas_call(
        functools.partial(tracer_kernel, sizes),
        grid=(NB // 2,),
        in_specs=[cols(NC, 0)] * 2 + [cols(LN, 0), cols(LN, 3)] * 2 + [plane] * 2 + ends * 2 + [whole(NR, NC)] * 5,
        out_specs=[pack] * 3 + [col] * 2 + [whole(2, LP, NC), first_rows(lambda b: b, 2)] + [whole(*x) for x in extra],
        out_shape=[PACK] * 2 + [PACK_HBM] + [shape(NR, LN)] * 2 + [shape(2, LP, NC), pltpu.HBM((NB, 3, LP, NC), F32)] + [shape(*x) for x in extra],
        scratch_shapes=[VM(SLAB, F32), VM((NR, NC), F32)] + [VM((NR, LN), F32)] * 2 + rows + [VM(x, F32) for x in edge] + strip_scratch(3) + sems,
        compiler_params=pltpu.CompilerParams(collective_id=0, has_side_effects=True, vmem_limit_bytes=26 << 20),
        name="tracers",
    )(t, s, u, u, v, v, kmt, depth, u, u, v, v, kmt, depth, eta, tu, tv)


def solve_pair(src_a, src_b, ca, cb, na, nb, out_a, out_b, gain_a, gain_b):
    zero = jnp.zeros(ROW, F32)
    la = lb = pa = pb = wa = wb = zero
    for k in range(NL):
        ua = jnp.where(k + 1 < na, ca, 0.0) if k + 1 < NL else zero
        ub = jnp.where(k + 1 < nb, cb, 0.0) if k + 1 < NL else zero
        ta = 1.0 + la * wa if k else jnp.ones_like(zero)
        tb = 1.0 + lb * wb if k else jnp.ones_like(zero)
        ia = 1.0 / (ta + ua)
        ib = 1.0 / (tb + ub)
        wa, wb = ta * ia, tb * ib
        gain_a[k] = ua * ia
        gain_b[k] = ub * ib
        pa = (src_a[k] + la * pa) * ia
        pb = (src_b[k] + lb * pb) * ib
        src_a[k] = pa
        src_b[k] = pb
        la, lb = ua, ub
    xa = xb = sa = sb = zero
    for k in reversed(range(NL)):
        xa = src_a[k] + gain_a[k] * xa
        xb = src_b[k] + gain_b[k] * xb
        out_a[k] = xa
        out_b[k] = xb
        sa += xa
        sb += xb
    return sa, sb


def momentum_kernel(
    u, v, p_b, pfirst, kun, kvn, kux, kvx, du, dv, kus, kvs, rwn, ren, re, rnorth, rsouth, rown, corner,
    us_b, vs_b, fx, fy, su, sv, pke, vrow,
    cc, hh, srcu, srcv, gu, gv, ums, vms,
):
    step = pl.program_id(0)
    last = step == NB
    us, vs, p = us_b.at[0], vs_b.at[0], p_b.at[0]
    row = iota(ROW, 0)
    rowx = iota(WIDE, 0)
    lane = iota(TILE, 1)
    kxn, kyn = kun[:], kvn[:]
    rwv, rev = rwn[:], ren[:]

    def halos(k):
        hu = jnp.where(lane == 0, lane_to(rev, k, 0), lane_to(rwv, k, LN - 1))
        hv = jnp.where(lane == 0, lane_to(rev, NL + k, 0), lane_to(rwv, NL + k, LN - 1))
        return hu, hv

    def masked(k, uk, vk, halo):
        um = only(k < kxn, jnp.concatenate([uk, halo[0]], axis=1))
        return um, only(k < kyn, jnp.concatenate([vk, halo[1]], axis=1))

    @pl.when(step == 0)
    def _():
        for k in range(NL):
            ums[k], vms[k] = masked(k, u[k], v[k], halos(k))
        lev = iota((LP, NC), 0).astype(F32)
        lev1 = iota((LP, LN), 0)
        ks, kw = kus[LAST, :NC], kvs[LAST, :NC]
        s_u = only(lev < ks, rsouth[0])
        s_v = only(lev < kw, rsouth[1])
        pick = only(iota((LP, LN), 1) == lev1 + NL, corner[LAST, :])
        edge = jnp.sum(pick, axis=1, keepdims=True)
        edge = only(lev[:, :1] < kvs[LAST, one(NC)], edge)
        s_ve = jnp.where(iota((LP, NC), 1) == NC - 1, edge, from_east(s_v))
        u_0 = only(lev < kxn[FIRST, :NC], rown[0])
        v_0 = only(lev < kyn[FIRST, :NC], rown[1])
        c_s = (0.25 * (s_v + s_ve)) * (s_u + u_0)
        h_s = 0.5 * (s_v + v_0)
        h_s = h_s * h_s + rown[2]
        for k in range(NL):
            cc[k, LAST, :] = c_s[one(k), :]
            hh[k, LAST, :] = h_s[one(k), :]

    @pl.when(step > 0)
    def _():
        kx, ky = kux[:], kvx[:]
        pev = re[:]
        total = [jnp.zeros(ROW, F32)] * 2

        def edge(k):
            return halos(k) + (lane_to(pev, 2 * NL + k, 0),)

        def shift(k, halo):
            um, vm = ums[k], vms[k]
            uk = jnp.where(last, rnorth[0, one(k), :], u[k])
            vk = jnp.where(last, rnorth[1, one(k), :], v[k])
            pe = jnp.concatenate([p[k], halo[2]], axis=1)
            return masked(k, uk, vk, halo), pe, from_west(um), from_east(vm)

        def flux(k, arg):
            new, pe, u_w, v_e = arg
            um, vm = ums[k], vms[k]
            c = (0.25 * (vm + v_e)) * (um + up_row(um, new[0], rowx))
            g = 0.5 * (u_w + um)
            g = g * g + pe
            c5 = c[:, :NC]
            return new, from_east(g)[:, :NC] - g[:, :NC], c5, c5 - from_west(c)[:, :NC]

        def tend(k, arg):
            new, dx, c5, dc = arg
            u5, v5, pk = ums[k, :, :NC], vms[k, :, :NC], p[k]
            north = jnp.where(last, rnorth[2, one(k), :], pfirst[0, 2, one(k), :])
            h = 0.5 * (v5 + up_row(v5, new[1][:, :NC], row))
            h = h * h + up_row(pk, north, row)
            tu = only(k < kx, dx + (c5 - down_row(c5, cc[k], row)))
            tv = only(k < ky, (h - down_row(h, hh[k], row)) + dc)
            total[0] += tu
            total[1] += tv
            srcu[k] = u5 - DT * tu
            srcv[k] = v5 - DT * tv
            cc[k] = c5
            hh[k] = h
            ums[k], vms[k] = new

        skewed((edge, shift, flux, tend), GROUP_M)
        dzu, dzv = du[:], dv[:]
        fx[:] = -dzu * total[0]
        fy[:] = -dzv * total[1]
        sa, sb = solve_pair(srcu, srcv, couple(kx, dzu, KV), couple(ky, dzv, KV), kx, ky, us, vs, gu, gv)
        sa, sb = dzu * sa, dzv * sb
        su[:] = sa
        sv[:] = sb
        ae = jnp.zeros(TILE, F32)
        for k in range(NL):
            ae = jnp.where(lane == k, lane_to(us[k, :, NC - LN :], LN - 1, k), ae)
        pke[:] = jnp.where(lane == 3 * NL, lane_to(sa[:, NC - LN :], LN - 1, 3 * NL), ae)

        @pl.when(last)
        def _():
            for k in range(NL):
                vrow[one(k), :] = vs[k, LAST, :]
            vrow[one(NL), :] = sb[LAST, :]
            vrow[NL + 1 : LP, :] = jnp.zeros((LP - NL - 1, NC), F32)


def momentum(u, v, p, first, geo, rw, re, rnorth, rsouth, rown, corner):
    ku, kv, du, dv = geo

    def this(b):
        return jnp.maximum(b, 1) - 1

    def ahead(b):
        return jnp.minimum(b, NB - 1)

    cube = pl.BlockSpec(SLAB, lambda b: (0, ahead(b), 0))
    pack = block_major(this)
    near = pl.BlockSpec(ROW, lambda b: (HT + this(b), 0))
    widn = pl.BlockSpec(WIDE, lambda b: (HT + b, 0))
    wids = pl.BlockSpec(WIDE, lambda b: (HT - 1, 0))
    plane = pl.BlockSpec(ROW, lambda b: (this(b), 0))
    col = pl.BlockSpec(TILE, lambda b: (this(b), 0))
    colw = pl.BlockSpec(TILE, lambda b: (b, 0))
    cole = pl.BlockSpec(TILE, lambda b: (ahead(b), 0))
    flat = jax.ShapeDtypeStruct((NR, NC), F32)

    def rows(n):
        return pl.BlockSpec((n, LP, NC), lambda b: (0, 0, 0))

    return pl.pallas_call(
        momentum_kernel,
        grid=(NB + 1,),
        in_specs=[cube, cube, pack, first_rows(ahead), widn, widn, near, near, near, near, wids, wids, colw, cole, col, rows(3), rows(2), rows(3), pl.BlockSpec(TILE, lambda b: (0, 0))],
        out_specs=[pack, pack, plane, plane, plane, plane, col, pl.BlockSpec((LP, NC), lambda b: (0, 0))],
        out_shape=[PACK, PACK_HBM, flat, flat, flat, flat, jax.ShapeDtypeStruct((NR, LN), F32), jax.ShapeDtypeStruct((LP, NC), F32)],
        scratch_shapes=[VM(SLAB, F32)] * 6 + [VM((NL,) + WIDE, F32)] * 2,
        compiler_params=pltpu.CompilerParams(vmem_limit_bytes=22 << 20),
        name="momentum",
    )(u, v, p, first, ku, kv, ku, kv, du, dv, ku, kv, rw, re, re, rnorth, rsouth, rown, corner)


def subcycle_kernel(
    sizes, eta_i, tu_i, tv_i, ku, kv, du, dv, fx, fy, tide, uke, tke, tkw, vrow, trn, trs,
    eta_o, u_o, v_o, ub_o, vb_o, fw, fe, fsouth, fnorth,
    eta, tu, tv, cu, cv, fu, fv, ub, vb, edge, south, north, *rest,
):
    to_west, to_east, *strips, send_sem, recv_sem = rest
    net = Exchange(sizes, send_sem, recv_sem)
    edge[:] = uke[:] + tke[:]
    pack_strips(((fx, fy),), to_west, to_east)
    plan = strip_plan(to_west, to_east, strips) + row_plan((fx, fy), south, north)
    late = [
        (edge, fw, 0, 1),
        (tkw, fe, 0, -1),
        (vrow, fsouth.at[0], 1, 0),
        (trn, fsouth.at[pl.ds(1, 2)], 1, 0),
        (trs.at[0], fnorth, -1, 0),
    ]
    net.clear(plan + late)
    net.barrier()
    plan, late = net.make(plan), net.make(late)
    net.start(plan + late)
    row = iota(WIDE, 0)
    zero = jnp.zeros(WIDE, F32)
    ub[:] = jnp.zeros(ub.shape, F32)
    vb[:] = jnp.zeros(vb.shape, F32)
    eta[:] = eta_i[:]
    tu[:] = tu_i[:]
    tv[:] = tv_i[:]
    cu[:] = DTB * (ku[:] * du[:])
    cv[:] = DTB * (kv[:] * dv[:])
    net.wait(plan)

    def turn(i):
        return halo_pair(i, 0, strips)

    def build(i, halo):
        sl = tile_rows(i)
        for n, (x, out, wet) in enumerate(((fx, fu, ku), (fy, fv, kv))):
            part, rows = side(i, x, south.at[n], north.at[n])
            out[sl, :] = only(wet[sl, :] > 0, DTB * jnp.concatenate([part[rows, :], halo[n]], axis=1))

    skewed((turn, build), TILES, ET)
    norm = 6.0 / (SUB * (SUB + 1) * (SUB + 2))

    def stage(first, last, lo, hi):
        def step(n, _):
            tx, ty = tide[0, n], tide[1, n]
            w = norm * ((n + 1) * (SUB - n)).astype(F32)

            def west(i):
                return from_west(tu[tile_rows(i), :])

            def surface(i, u_w):
                sl = tile_rows(i)
                vn = tv[sl, :]
                south = tv[tile_rows(i - 1), :] if i else zero
                e = eta[sl, :] - DTB * ((tu[sl, :] - u_w) + (vn - down_row(vn, south, row)))
                eta[sl, :] = e
                return from_east(e)

            def update(i, e_e):
                sl = tile_rows(i)
                e = eta[sl, :]
                un = tu[sl, :] + (cu[sl, :] * (tx - (e_e - e)) + fu[sl, :])
                tu[sl, :] = un
                if lo_bar <= i < hi_bar:
                    ub[sl, :] = ub[sl, :] + w * un
                if i > lo:
                    north(i - 1, e, ty, w)

            skewed((lambda i: west(lo + i), lambda i, x: surface(lo + i, x), lambda i, x: update(lo + i, x)), TILES, hi - lo)
            north(hi - 1, eta[tile_rows(hi - 1), :], ty, w)
            return 0

        lax.fori_loop(first, last, step, 0)

    lo_bar, hi_bar = HT - 1, HT + NB

    def north(i, ahead, ty, w):
        sl = tile_rows(i)
        e = eta[sl, :]
        x = tv[sl, :] + (cv[sl, :] * (ty - (up_row(e, ahead, row) - e)) + fv[sl, :])
        tv[sl, :] = x
        if lo_bar <= i < hi_bar:
            vb[sl, :] = vb[sl, :] + w * x

    for s in range(0, SUB, 8):
        stage(s, min(s + 8, SUB), s // 8, ET - s // 8)
    eta_o[:] = eta[HR : HR + NR, :NC]
    u_o[:] = tu[HR : HR + NR, :NC]
    v_o[:] = tv[HR : HR + NR, :NC]
    ub_o[:] = ub[HR - 8 : HR + NR, :]
    vb_o[:] = vb[HR - 8 : HR + NR, :]
    net.wait(late)


def subcycles(sizes, *args):
    vm = pl.BlockSpec(memory_space=VM)
    outs = [shape(NR, NC)] * 3 + [shape(NR + 8, EC)] * 2 + [shape(NR, LN)] * 2 + [shape(3, LP, NC)] * 2
    sems = [pltpu.SemaphoreType.DMA((6 + 4 + 5,))] * 2
    wide = [VM((ER, EC), F32)] * 9
    return pl.pallas_call(
        functools.partial(subcycle_kernel, sizes),
        in_specs=[vm] * 9 + [pl.BlockSpec(memory_space=pltpu.SMEM)] + [vm] * 5 + [pl.BlockSpec(memory_space=pl.ANY)],
        out_specs=[vm] * len(outs),
        out_shape=outs,
        scratch_shapes=wide + [VM((NR, LN), F32)] + [VM((2, HR, NC), F32)] * 2 + strip_scratch(1) + sems,
        compiler_params=pltpu.CompilerParams(collective_id=1, has_side_effects=True, vmem_limit_bytes=22 << 20),
        name="subcycles",
    )(*args)


def finish_kernel(*refs):
    ins, kvs, dvs, vbs, eta, tu, tv, rnorth, rsouth, rown, eta_o, tu_o, tv_o, uo, vo, to, so, ct, cs = refs[:23], *refs[23:]
    cubes, planes, wide = ins[:4], ins[4:9], ins[9:]
    b = pl.program_id(0)
    eta_o[:] = eta[:]
    tu_o[:] = tu[:]
    tv_o[:] = tv[:]

    @pl.when(b == 0)
    def _():
        lev = iota((LP, NC), 0).astype(F32)
        kx = kvs[LAST, :NC]
        cor = correction(vbs[LAST, :NC], rsouth[0, one(NL), :], kx, dvs[LAST, :NC])
        vel = 0.5 * only(lev < kx, rsouth[0] + cor)
        ft = vel * (rsouth[1] + rown[0, 0])
        fs = vel * (rsouth[2] + rown[0, 1])
        for k in range(NL):
            ct[k, LAST, :] = ft[one(k), :]
            cs[k, LAST, :] = fs[one(k), :]

    for half in range(2):
        sl = tile_rows(half)
        outs = [x.at[:, sl, :] for x in (uo, vo, to, so)]
        last = (b == NB // 2 - 1) if half else None
        finish_rows(last, *[x.at[half] for x in cubes], *[x[sl, :] for x in planes], *wide[half::2], rnorth, *outs, ct, cs)


def correction(mean, total, k, dz):
    deep = k * dz
    return (mean - total) / jnp.where(deep > 0, deep, 1.0)


def finish_rows(last, us, vs, t, s, cnt, su, sv, rwv, rev, ku, kv, du, dv, ub, vb, first, rnorth, uo, vo, to, so, ct, cs):
    row = iota(ROW, 0)
    lane = iota(TILE, 1)

    kx, ky = ku[:], kv[:, :NC]
    tot = jnp.concatenate([su, lane_to(rwv, 3 * NL, LN - 1)], axis=1)
    cx = correction(ub[:], tot, kx, du[:])
    cy = correction(vb[:, :NC], sv, ky, dv[:, :NC])
    fields = ((t, to, ct), (s, so, cs))

    def load(k):
        out = [lane_to(rwv, k, LN - 1)]
        for i in range(2):
            base = NL * (i + 1) + k
            out.append(jnp.where(lane == 0, lane_to(rev, base, 0), lane_to(rwv, base, LN - 1)))
        return out

    def east(k, halo):
        wide = [jnp.concatenate([f[0][k], h], axis=1) for f, h in zip(fields, halo[1:])]
        return halo[0], [x + from_east(x) for x in wide]

    def flux(k, arg):
        halo, sums = arg
        ue = only(k < kx, jnp.concatenate([us[k], halo], axis=1) + cx)
        uo[k] = ue[:, :NC]
        half = 0.5 * ue
        f = [half * x for x in sums]
        return [(x - from_west(x))[:, :NC] for x in f]

    def store(k, div):
        ve = only(k < ky, vs[k] + cy)
        vo[k] = ve
        hy = 0.5 * ve
        for i, (x, out, carry) in enumerate(fields):
            own = x[k]
            north = first[0, i, one(k), :]
            if last is not None:
                north = jnp.where(last, rnorth[i, one(k), :], north)
            fy = hy * (own + up_row(own, north, row))
            new = own - DT * (div[i] + (fy - down_row(fy, carry[k], row)))
            carry[k] = fy
            out[k] = only(k < cnt, new)

    skewed((load, east, flux, store), GROUP_F)


def finish(us, vs, tm, sm, first, kmt, geo, ub, vb, su, sv, rw, re, rnorth, rsouth, state):
    kv, dv = geo[1], geo[3]

    def rows(width):
        return pl.BlockSpec((16, width), lambda b: (b, 0))

    def pair(start):
        return [pl.BlockSpec(WIDE, lambda b, h=h: (start + 2 * b + h, 0)) for h in range(2)]

    def fixed(i):
        return pl.BlockSpec(WIDE, lambda b: (i, 0))

    ahead = [first_rows(lambda b: 2 * b + 1), first_rows(lambda b: jnp.minimum(2 * b + 2, NB - 1))]
    cube = pl.BlockSpec((NL, 16, NC), lambda b: (0, b, 0))
    south = [fixed(HT - 1)] * 2 + [fixed(0)]
    wide = [x for x in (*geo, ub, vb, first) for _ in range(2)]
    return pl.pallas_call(
        finish_kernel,
        grid=(NB // 2,),
        in_specs=[block_major(lambda b: b, 2)] * 4 + [rows(NC)] * 3 + [rows(LN)] * 2 + pair(HT) * 4 + pair(1) * 2 + ahead + south + [rows(NC)] * 3 + [whole(3, LP, NC)] * 2 + [first_rows(lambda b: 0)],
        out_specs=[rows(NC)] * 3 + [cube] * 4,
        out_shape=[shape(NR, NC)] * 3 + [shape(NL, NR, NC)] * 4,
        scratch_shapes=[VM(SLAB, F32)] * 2,
        compiler_params=pltpu.CompilerParams(vmem_limit_bytes=26 << 20),
        name="finish",
    )(us, vs, tm, sm, kmt, su, sv, rw, re, *wide, kv, dv, vb, *state, rnorth, rsouth, first)


def solution(mesh):
    sizes = mesh.shape["row"], mesh.shape["col"]

    def local_step(u, v, t, s, eta, tu, tv, depth, kmt, tide):
        u, v, t, s, eta, tu, tv, depth, kmt = (pltpu.with_memory_space_constraint(x, pltpu.HBM) for x in (u, v, t, s, eta, tu, tv, depth, kmt))
        tm, sm, pr, tke, tkw, trn, first, rw, re, rsouth, rnorth, corner, rown, *wide = tracers(sizes, t, s, u, v, kmt, depth, eta, tu, tv)
        geo, state = wide[:4], wide[4:]
        tm, sm = (pltpu.with_memory_space_constraint(x, pltpu.VMEM) for x in (tm, sm))
        first = pltpu.with_memory_space_constraint(first, pltpu.HBM)
        pr = pltpu.with_memory_space_constraint(pr, pltpu.HBM)
        us, vs, fx, fy, su, sv, uke, vrow = momentum(u, v, pr, first, geo, rw, re, rnorth, rsouth, rown, corner)
        eta_n, u_n, v_n, ub, vb, fw, fe, fsouth, fnorth = subcycles(sizes, *state, *geo, fx, fy, tide.T, uke, tke, tkw, vrow, trn, first)
        us = pltpu.with_memory_space_constraint(us, pltpu.VMEM)
        vs = pltpu.with_memory_space_constraint(vs, pltpu.HBM)
        return finish(us, vs, tm, sm, first, kmt, geo, ub, vb, su, sv, fw, fe, fnorth, fsouth, (eta_n, u_n, v_n))

    cube, plane = P(None, "row", "col"), P("row", "col")
    return jax.shard_map(
        local_step,
        mesh=mesh,
        in_specs=(cube,) * 4 + (plane,) * 5 + (P(None, None),),
        out_specs=(plane,) * 3 + (cube,) * 4,
        check_vma=False,
    )
```

```python
import functools

import jax
import jax.numpy as jnp
from jax import lax
from jax.experimental import pallas as pl
from jax.experimental.pallas import tpu as pltpu
from jax.sharding import PartitionSpec as P

NL = 41
NR = 96
NC = 512
LN = 128
LP = 48
HR = 40
ER = NR + 2 * HR
EC = NC + 128
NB = NR // 8
SUB = 36
GROUP_M = 2
GROUP_F = 3
HALF = 64
SIDES = (-1, 0, 1)
FIRST, LAST = slice(0, 1), slice(7, 8)
TILES = 3
DT = 4.0
DTB = DT / SUB
KV = 0.001
KT = 0.0005
F32 = jnp.float32
HT = HR // 8
ET = ER // 8
SLAB, ROW, WIDE, TILE = (NL, 8, NC), (8, NC), (8, EC), (8, LN)
VM = pltpu.VMEM


def only(mask, x):
    return jnp.where(mask, x, jnp.zeros_like(x))


def iota(shape, dim):
    return lax.broadcasted_iota(jnp.int32, shape, dim)


def whole(*shape):
    return pl.BlockSpec(shape, lambda *_: (0,) * len(shape))


def shape(*dims):
    return jax.ShapeDtypeStruct(dims, F32)


def one(k):
    return slice(k, k + 1)


def tile_rows(i):
    return slice(8 * i, 8 * (i + 1))


def from_west(x):
    return pltpu.roll(x, 1, axis=1)


def from_east(x):
    return pltpu.roll(x, x.shape[1] - 1, axis=1)


def lane_to(x, src, dst):
    shift = (dst - src) % LN
    return x if shift == 0 else pltpu.roll(x, shift, axis=1)


def up_row(x, nxt, row):
    return pltpu.roll(jnp.where(row == 0, nxt, x), 7, axis=0)


def down_row(x, prev, row):
    return pltpu.roll(jnp.where(row == 7, prev, x), 1, axis=0)


def skewed(stages, group, count=NL):
    blocks = [range(k, min(k + group, count)) for k in range(0, count, group)]
    held = {}
    for i in range(len(blocks) + len(stages) - 1):
        for n, stage in enumerate(stages):
            if 0 <= i - n < len(blocks):
                for k in blocks[i - n]:
                    held[k] = stage(k, held[k]) if n else stage(k)


def couple(count, thick, kappa):
    safe = jnp.where(count > 0, thick, 1.0)
    return DT * kappa / (safe * safe)


def pressure_step(t, s, wet, cum, thick):
    half = only(wet, 0.5 * (0.015 * (s - 1.0) - 0.02 * (t - 1.0)))
    mid = cum + half
    return thick * mid, mid + half


class Exchange:
    def __init__(self, sizes, send_sem, recv_sem):
        self.rows, self.cols = sizes
        self.row, self.col = lax.axis_index("row"), lax.axis_index("col")
        self.sems = send_sem, recv_sem
        self.used = 0

    def inside(self, drow):
        return (self.row + drow >= 0) & (self.row + drow < self.rows)

    def at(self, drow, dcol):
        return {"row": self.row + drow, "col": lax.rem(self.col + dcol + self.cols, self.cols)}

    def when(self, drow, action):
        if drow:
            pl.when(self.inside(drow))(action)
        else:
            action()

    def announce(self):
        ready = pltpu.get_barrier_semaphore()
        for drow in SIDES:
            for dcol in SIDES:
                if drow or dcol:
                    self.when(drow, functools.partial(pl.semaphore_signal, ready, device_id=self.at(drow, dcol), device_id_type=pl.DeviceIdType.MESH))

    def ready(self):
        per_row = len(SIDES)
        known = [self.inside(drow).astype(jnp.int32) for drow in SIDES if drow]
        pl.semaphore_wait(pltpu.get_barrier_semaphore(), per_row - 1 + per_row * sum(known))

    def clear(self, plan):
        for _, dst, drow, _ in plan:
            if drow:

                @pl.when(jnp.logical_not(self.inside(-drow)))
                def _():
                    dst[:] = jnp.zeros(dst.shape, F32)

    def make(self, plan):
        out = []
        for src, dst, drow, dcol in plan:
            copy = pltpu.make_async_remote_copy(
                src_ref=src,
                dst_ref=dst,
                send_sem=self.sems[0].at[self.used],
                recv_sem=self.sems[1].at[self.used],
                device_id=self.at(drow, dcol),
                device_id_type=pl.DeviceIdType.MESH,
            )
            self.used += 1
            out.append((copy, drow))
        return out

    def start(self, copies):
        for copy, drow in copies:
            self.when(drow, copy.start)

    def wait(self, copies):
        for copy, drow in copies:
            self.when(drow, copy.wait_send)
            self.when(-drow, copy.wait_recv)


def pack_strips(pairs, to_west, to_east):
    lane = iota(TILE, 1)
    first, last = slice(0, LN), slice(NC - LN, NC)

    def turn(n):
        q, sl = n // NB, tile_rows(n % NB)
        b = pairs[q][-1]
        return pltpu.roll(b[sl, first], HALF, axis=1), pltpu.roll(b[sl, last], HALF, axis=1)

    def store(n, turned):
        q, sl = n // NB, tile_rows(n % NB)
        a = pairs[q][0]
        to_west[q, sl, :] = jnp.where(lane < HALF, a[sl, first], turned[0])
        to_east[q, sl, :] = jnp.where(lane < HALF, turned[1], a[sl, last])

    skewed((turn, store), NB, NB * len(pairs))


def strip_plan(to_west, to_east, strips):
    top, bottom = pl.ds(NR - HR, HR), pl.ds(0, HR)
    return [
        (to_east, strips[0], 0, 1),
        (to_west, strips[1], 0, -1),
        (to_east.at[:, top], strips[2], 1, 1),
        (to_west.at[:, top], strips[3], 1, -1),
        (to_east.at[:, bottom], strips[4], -1, 1),
        (to_west.at[:, bottom], strips[5], -1, -1),
    ]


def row_plan(planes, south, north):
    plan = []
    for i, x in enumerate(planes):
        plan.append((x.at[pl.ds(NR - HR, HR), :], south.at[i], 1, 0))
        plan.append((x.at[pl.ds(0, HR), :], north.at[i], -1, 0))
    return plan


def strip_scratch(n):
    return [VM((n, NR, LN), F32)] * 4 + [VM((n, HR, LN), F32)] * 4


def side(i, own, south, north):
    if i < HT:
        return south, tile_rows(i)
    return (own, tile_rows(i - HT)) if i < HT + NB else (north, tile_rows(i - HT - NB))


def halo_pair(i, q, strips):
    (w, e), sl = side(i, strips[:2], strips[2:4], strips[4:])
    lane = iota(TILE, 1)
    w, e = w[q, sl, :], e[q, sl, :]
    return jnp.where(lane < HALF, e, w), pltpu.roll(jnp.where(lane < HALF, w, e), HALF, axis=1)


def mix_tracers(t, s, cnt, depth, strips, tm, sm, pr, pke, pkw, tke, tkw, rs, gains):
    lane = iota(TILE, 1)
    thick = depth / jnp.maximum(cnt, 1).astype(F32)
    c = couple(cnt, thick, KT)
    zero = jnp.zeros(ROW, F32)
    cum = lower = pt = ps = zero
    keep = zero
    ae = aw = jnp.zeros(TILE, F32)
    u0, u3, v0, v3 = strips
    for k in range(NL):
        wet = k < cnt
        tk, sk = t[k], s[k]
        p, cum = pressure_step(tk, sk, wet, cum, thick)
        pr[k] = p
        for n, (x0, x3) in enumerate(((u0, u3), (v0, v3))):
            base = NL * n + k
            ae = jnp.where(lane == base, lane_to(x3[k], LN - 1, base), ae)
            aw = jnp.where(lane == base, lane_to(x0[k], 0, base), aw)
        aw = jnp.where(lane == 2 * NL + k, lane_to(p[:, :LN], 0, 2 * NL + k), aw)
        rs[2, one(k), :] = p[FIRST, :]
        upper = jnp.where(k + 1 < cnt, c, 0.0) if k + 1 < NL else zero
        top = 1.0 + lower * keep if k else jnp.ones_like(zero)
        inv = 1.0 / (top + upper)
        keep = top * inv
        gains[k] = upper * inv
        pt = (jnp.where(wet, tk, 0.0) + lower * pt) * inv
        ps = (jnp.where(wet, sk, 0.0) + lower * ps) * inv
        tm[k] = pt
        sm[k] = ps
        lower = upper
    pke[:] = ae
    pkw[:] = aw
    ae = aw = jnp.zeros(TILE, F32)
    bt = bs = zero
    for k in reversed(range(NL)):
        gain = gains[k]
        bt = tm[k] + gain * bt
        bs = sm[k] + gain * bs
        tm[k] = bt
        sm[k] = bs
        rs[0, one(k), :] = bt[FIRST, :]
        rs[1, one(k), :] = bs[FIRST, :]
        for x, base in ((bt, NL), (bs, 2 * NL)):
            ae = jnp.where(lane == base + k, lane_to(x[:, NC - LN :], LN - 1, base + k), ae)
            aw = jnp.where(lane == base + k, lane_to(x[:, :LN], 0, base + k), aw)
    tke[:] = ae
    tkw[:] = aw


def wide_geometry(planes, strips, south, north, outs):
    ku, kv, du, dv, *state = outs
    row = iota(WIDE, 0)

    def turn(i):
        return [halo_pair(i, q, strips) for q in range(3)]

    def build(i, halo):
        halo = [x for pair in halo for x in pair]
        vals = []
        for n in range(len(planes)):
            part, sl = side(i, planes[n], south.at[n], north.at[n])
            vals.append(jnp.concatenate([part[sl, :], halo[n]], axis=1))
        k, h = vals[:2]
        dz = h / jnp.maximum(k, 1.0)
        kv[tile_rows(i), :] = k
        dv[tile_rows(i), :] = dz
        return vals[2:], from_east(k), from_east(dz)

    def store(i, arg):
        vals, ke, dze = arg
        sl = tile_rows(i)
        hi = tile_rows(min(i + 1, ET - 1))
        k, dz = kv[sl, :], dv[sl, :]
        k_u, k_v = jnp.minimum(k, ke), jnp.minimum(k, up_row(k, kv[hi, :], row))
        dv[sl, :] = 0.5 * (dz + up_row(dz, dv[hi, :], row))
        du[sl, :] = 0.5 * (dz + dze)
        ku[sl, :] = k_u
        kv[sl, :] = k_v
        for out, x, wet in zip(state, vals, (k, k_u, k_v)):
            out[sl, :] = only(wet > 0, x)

    skewed((turn, build, store), TILES, ET)


def tracer_kernel(sizes, t, s, u0, u3, v0, v3, kc, hc, uf, ul, vf, vl, kmt, depth, eta, tu, tv, *rest):
    tm_b, sm_b, pr_b, tke, tkw, rn, rs_b, *rest = rest
    received, rown, wide, rest = rest[:5], rest[5], rest[6:13], rest[13:]
    gains, kf, pke, pkw, prn, prs, south, north, rw, re, rsouth, rnorth, corner, to_west, to_east, *strips, send_sem, recv_sem = rest
    b = pl.program_id(0)
    last = NB // 2 - 1
    net = Exchange(sizes, send_sem, recv_sem)
    planes = (kf, depth, eta, tu, tv)
    head = strip_plan(to_west, to_east, strips) + [(prn, rsouth, 1, 0)] + row_plan(planes, south, north)
    middle = [(prs, rnorth, -1, 0), (pke.at[pl.ds(0, 8), :], rw.at[pl.ds(NR, 8), :], -1, 1)]
    tail = [(pkw.at[pl.ds(NR - 8, 8), :], corner, 1, -1)]

    def piece(i):
        part = pl.ds(16 * i, 16)
        return net.make([(pke.at[part, :], rw.at[part, :], 0, 1), (pkw.at[part, :], re.at[part, :], 0, -1)])

    first_plan = head + middle + tail
    head, middle, tail = net.make(head), net.make(middle), net.make(tail)
    pieces = [piece(i) for i in range(last + 1)]

    @pl.when(b == 0)
    def _():
        net.clear(first_plan)
        net.announce()
        kf[:] = kmt[:].astype(F32)
        pack_strips((planes[:2], planes[2:4], planes[4:]), to_west, to_east)
        prn[:] = jnp.zeros(prn.shape, F32)
        prs[:] = jnp.zeros(prs.shape, F32)
        for k in range(NL):
            for n, (lo, hi) in enumerate(((uf, ul), (vf, vl))):
                prn[n, one(k), :] = hi[k, LAST, :]
                prs[n, one(k), :] = lo[k, FIRST, :]
        net.ready()
        net.start(head)

    for i in range(last):

        @pl.when(b == i + 1)
        def _():
            net.start(pieces[i])

    for half in range(2):
        sl = tile_rows(half)
        tm, sm, rs = tm_b.at[half], sm_b.at[half], rs_b.at[half]
        out = pl.ds(pl.multiple_of(16 * b + 8 * half, 8), 8)
        parts = [x.at[:, sl, :] for x in (t, s, u0, u3, v0, v3)]
        mix_tracers(*parts[:2], kc[sl, :], hc[sl, :], parts[2:], tm, sm, pr_b.at[half], pke.at[out, :], pkw.at[out, :], tke.at[sl, :], tkw.at[sl, :], rs, gains)

    @pl.when(b == 0)
    def _():
        prs[2] = rs_b[0, 2]
        net.start(middle)

    @pl.when(b == last)
    def _():
        net.start(pieces[last] + tail)
        for k in range(NL):
            rn[0, one(k), :] = tm[k, LAST, :]
            rn[1, one(k), :] = sm[k, LAST, :]
        rown[:] = prs[:]
        net.wait(head)
        wide_geometry(planes, strips, south, north, wide)
        net.wait(middle + tail)
        for copies in pieces:
            net.wait(copies)
        for out, x in zip(received, (rw, re, rsouth, rnorth, corner)):
            out[:] = x[:]


PACK = VM((NB,) + SLAB, F32)
PACK_HBM = pltpu.HBM((NB,) + SLAB, F32)


def block_major(f, n=1):
    return pl.BlockSpec((n,) + SLAB, lambda b: (f(b), 0, 0, 0))


def first_rows(f, n=1):
    return pl.BlockSpec((n, 3, LP, NC), lambda b: (f(b), 0, 0, 0))


def tracers(sizes, t, s, u, v, kmt, depth, eta, tu, tv):
    def cols(width, j):
        return pl.BlockSpec((NL, 16, width), lambda b: (0, b, j))

    def slab(i):
        return pl.BlockSpec(SLAB, lambda b: (0, i, 0))

    pack = block_major(lambda b: b, 2)
    plane = pl.BlockSpec((16, NC), lambda b: (b, 0))
    col = pl.BlockSpec((16, LN), lambda b: (b, 0))
    ends = [slab(0), slab(NB - 1)]
    edge = [(NR + 8, LN), (NR, LN), (2, LP, NC), (3, LP, NC), (8, LN)]
    extra = edge + [(3, LP, NC)] + [(ER, EC)] * 7
    sems = [pltpu.SemaphoreType.DMA((6 + 1 + 10 + 3 + NB,))] * 2
    rows = [VM((2, LP, NC), F32), VM((3, LP, NC), F32)] + [VM((5, HR, NC), F32)] * 2
    return pl.pallas_call(
        functools.partial(tracer_kernel, sizes),
        grid=(NB // 2,),
        in_specs=[cols(NC, 0)] * 2 + [cols(LN, 0), cols(LN, 3)] * 2 + [plane] * 2 + ends * 2 + [whole(NR, NC)] * 5,
        out_specs=[pack] * 3 + [col] * 2 + [whole(2, LP, NC), first_rows(lambda b: b, 2)] + [whole(*x) for x in extra],
        out_shape=[PACK] * 2 + [PACK_HBM] + [shape(NR, LN)] * 2 + [shape(2, LP, NC), pltpu.HBM((NB, 3, LP, NC), F32)] + [shape(*x) for x in extra],
        scratch_shapes=[VM(SLAB, F32), VM((NR, NC), F32)] + [VM((NR, LN), F32)] * 2 + rows + [VM(x, F32) for x in edge] + strip_scratch(3) + sems,
        compiler_params=pltpu.CompilerParams(collective_id=0, has_side_effects=True, vmem_limit_bytes=26 << 20),
        name="tracers",
    )(t, s, u, u, v, v, kmt, depth, u, u, v, v, kmt, depth, eta, tu, tv)


def solve_pair(src_a, src_b, ca, cb, na, nb, out_a, out_b, gain_a, gain_b):
    zero = jnp.zeros(ROW, F32)
    la = lb = pa = pb = wa = wb = zero
    for k in range(NL):
        ua = jnp.where(k + 1 < na, ca, 0.0) if k + 1 < NL else zero
        ub = jnp.where(k + 1 < nb, cb, 0.0) if k + 1 < NL else zero
        ta = 1.0 + la * wa if k else jnp.ones_like(zero)
        tb = 1.0 + lb * wb if k else jnp.ones_like(zero)
        ia = 1.0 / (ta + ua)
        ib = 1.0 / (tb + ub)
        wa, wb = ta * ia, tb * ib
        gain_a[k] = ua * ia
        gain_b[k] = ub * ib
        pa = (src_a[k] + la * pa) * ia
        pb = (src_b[k] + lb * pb) * ib
        src_a[k] = pa
        src_b[k] = pb
        la, lb = ua, ub
    xa = xb = sa = sb = zero
    for k in reversed(range(NL)):
        xa = src_a[k] + gain_a[k] * xa
        xb = src_b[k] + gain_b[k] * xb
        out_a[k] = xa
        out_b[k] = xb
        sa += xa
        sb += xb
    return sa, sb


def momentum_kernel(
    u, v, p_b, pfirst, kun, kvn, kux, kvx, du, dv, kus, kvs, rwn, ren, re, rnorth, rsouth, rown, corner,
    us_b, vs_b, fx, fy, su, sv, pke, vrow,
    cc, hh, srcu, srcv, gu, gv, ums, vms,
):
    step = pl.program_id(0)
    last = step == NB
    us, vs, p = us_b.at[0], vs_b.at[0], p_b.at[0]
    row = iota(ROW, 0)
    rowx = iota(WIDE, 0)
    lane = iota(TILE, 1)
    kxn, kyn = kun[:], kvn[:]
    rwv, rev = rwn[:], ren[:]

    def halos(k):
        hu = jnp.where(lane == 0, lane_to(rev, k, 0), lane_to(rwv, k, LN - 1))
        hv = jnp.where(lane == 0, lane_to(rev, NL + k, 0), lane_to(rwv, NL + k, LN - 1))
        return hu, hv

    def masked(k, uk, vk, halo):
        um = only(k < kxn, jnp.concatenate([uk, halo[0]], axis=1))
        return um, only(k < kyn, jnp.concatenate([vk, halo[1]], axis=1))

    @pl.when(step == 0)
    def _():
        for k in range(NL):
            ums[k], vms[k] = masked(k, u[k], v[k], halos(k))
        lev = iota((LP, NC), 0).astype(F32)
        lev1 = iota((LP, LN), 0)
        ks, kw = kus[LAST, :NC], kvs[LAST, :NC]
        s_u = only(lev < ks, rsouth[0])
        s_v = only(lev < kw, rsouth[1])
        pick = only(iota((LP, LN), 1) == lev1 + NL, corner[LAST, :])
        edge = jnp.sum(pick, axis=1, keepdims=True)
        edge = only(lev[:, :1] < kvs[LAST, one(NC)], edge)
        s_ve = jnp.where(iota((LP, NC), 1) == NC - 1, edge, from_east(s_v))
        u_0 = only(lev < kxn[FIRST, :NC], rown[0])
        v_0 = only(lev < kyn[FIRST, :NC], rown[1])
        c_s = (0.25 * (s_v + s_ve)) * (s_u + u_0)
        h_s = 0.5 * (s_v + v_0)
        h_s = h_s * h_s + rown[2]
        for k in range(NL):
            cc[k, LAST, :] = c_s[one(k), :]
            hh[k, LAST, :] = h_s[one(k), :]

    @pl.when(step > 0)
    def _():
        kx, ky = kux[:], kvx[:]
        pev = re[:]
        total = [jnp.zeros(ROW, F32)] * 2

        def edge(k):
            return halos(k) + (lane_to(pev, 2 * NL + k, 0),)

        def shift(k, halo):
            um, vm = ums[k], vms[k]
            uk = jnp.where(last, rnorth[0, one(k), :], u[k])
            vk = jnp.where(last, rnorth[1, one(k), :], v[k])
            pe = jnp.concatenate([p[k], halo[2]], axis=1)
            return masked(k, uk, vk, halo), pe, from_west(um), from_east(vm)

        def flux(k, arg):
            new, pe, u_w, v_e = arg
            um, vm = ums[k], vms[k]
            c = (0.25 * (vm + v_e)) * (um + up_row(um, new[0], rowx))
            g = 0.5 * (u_w + um)
            g = g * g + pe
            c5 = c[:, :NC]
            return new, from_east(g)[:, :NC] - g[:, :NC], c5, c5 - from_west(c)[:, :NC]

        def tend(k, arg):
            new, dx, c5, dc = arg
            u5, v5, pk = ums[k, :, :NC], vms[k, :, :NC], p[k]
            north = jnp.where(last, rnorth[2, one(k), :], pfirst[0, 2, one(k), :])
            h = 0.5 * (v5 + up_row(v5, new[1][:, :NC], row))
            h = h * h + up_row(pk, north, row)
            tu = only(k < kx, dx + (c5 - down_row(c5, cc[k], row)))
            tv = only(k < ky, (h - down_row(h, hh[k], row)) + dc)
            total[0] += tu
            total[1] += tv
            srcu[k] = u5 - DT * tu
            srcv[k] = v5 - DT * tv
            cc[k] = c5
            hh[k] = h
            ums[k], vms[k] = new

        skewed((edge, shift, flux, tend), GROUP_M)
        dzu, dzv = du[:], dv[:]
        fx[:] = -dzu * total[0]
        fy[:] = -dzv * total[1]
        sa, sb = solve_pair(srcu, srcv, couple(kx, dzu, KV), couple(ky, dzv, KV), kx, ky, us, vs, gu, gv)
        sa, sb = dzu * sa, dzv * sb
        su[:] = sa
        sv[:] = sb
        ae = jnp.zeros(TILE, F32)
        for k in range(NL):
            ae = jnp.where(lane == k, lane_to(us[k, :, NC - LN :], LN - 1, k), ae)
        pke[:] = jnp.where(lane == 3 * NL, lane_to(sa[:, NC - LN :], LN - 1, 3 * NL), ae)

        @pl.when(last)
        def _():
            for k in range(NL):
                vrow[one(k), :] = vs[k, LAST, :]
            vrow[one(NL), :] = sb[LAST, :]
            vrow[NL + 1 : LP, :] = jnp.zeros((LP - NL - 1, NC), F32)


def momentum(u, v, p, first, geo, rw, re, rnorth, rsouth, rown, corner):
    ku, kv, du, dv = geo

    def this(b):
        return jnp.maximum(b, 1) - 1

    def ahead(b):
        return jnp.minimum(b, NB - 1)

    cube = pl.BlockSpec(SLAB, lambda b: (0, ahead(b), 0))
    pack = block_major(this)
    near = pl.BlockSpec(ROW, lambda b: (HT + this(b), 0))
    widn = pl.BlockSpec(WIDE, lambda b: (HT + b, 0))
    wids = pl.BlockSpec(WIDE, lambda b: (HT - 1, 0))
    plane = pl.BlockSpec(ROW, lambda b: (this(b), 0))
    col = pl.BlockSpec(TILE, lambda b: (this(b), 0))
    colw = pl.BlockSpec(TILE, lambda b: (b, 0))
    cole = pl.BlockSpec(TILE, lambda b: (ahead(b), 0))
    flat = jax.ShapeDtypeStruct((NR, NC), F32)

    def rows(n):
        return pl.BlockSpec((n, LP, NC), lambda b: (0, 0, 0))

    return pl.pallas_call(
        momentum_kernel,
        grid=(NB + 1,),
        in_specs=[cube, cube, pack, first_rows(ahead), widn, widn, near, near, near, near, wids, wids, colw, cole, col, rows(3), rows(2), rows(3), pl.BlockSpec(TILE, lambda b: (0, 0))],
        out_specs=[pack, pack, plane, plane, plane, plane, col, pl.BlockSpec((LP, NC), lambda b: (0, 0))],
        out_shape=[PACK, PACK_HBM, flat, flat, flat, flat, jax.ShapeDtypeStruct((NR, LN), F32), jax.ShapeDtypeStruct((LP, NC), F32)],
        scratch_shapes=[VM(SLAB, F32)] * 6 + [VM((NL,) + WIDE, F32)] * 2,
        compiler_params=pltpu.CompilerParams(vmem_limit_bytes=22 << 20),
        name="momentum",
    )(u, v, p, first, ku, kv, ku, kv, du, dv, ku, kv, rw, re, re, rnorth, rsouth, rown, corner)


def subcycle_kernel(
    sizes, eta_i, tu_i, tv_i, ku, kv, du, dv, fx, fy, tide, uke, tke, tkw, vrow, trn, trs,
    eta_o, u_o, v_o, ub_o, vb_o, fw, fe, fsouth, fnorth,
    eta, tu, tv, cu, cv, fu, fv, ub, vb, edge, south, north, *rest,
):
    to_west, to_east, *strips, send_sem, recv_sem = rest
    net = Exchange(sizes, send_sem, recv_sem)
    plan = strip_plan(to_west, to_east, strips) + row_plan((fx, fy), south, north)
    late = [
        (edge, fw, 0, 1),
        (tkw, fe, 0, -1),
        (vrow, fsouth.at[0], 1, 0),
        (trn, fsouth.at[pl.ds(1, 2)], 1, 0),
        (trs.at[0], fnorth, -1, 0),
    ]
    net.clear(plan + late)
    net.announce()
    edge[:] = uke[:] + tke[:]
    pack_strips(((fx, fy),), to_west, to_east)
    row = iota(WIDE, 0)
    zero = jnp.zeros(WIDE, F32)
    ub[:] = jnp.zeros(ub.shape, F32)
    vb[:] = jnp.zeros(vb.shape, F32)
    eta[:] = eta_i[:]
    tu[:] = tu_i[:]
    tv[:] = tv_i[:]
    plan, late = net.make(plan), net.make(late)
    net.ready()
    net.start(plan)
    cu[:] = DTB * (ku[:] * du[:])
    cv[:] = DTB * (kv[:] * dv[:])
    net.wait(plan)
    net.start(late)

    def turn(i):
        return halo_pair(i, 0, strips)

    def build(i, halo):
        sl = tile_rows(i)
        for n, (x, out, wet) in enumerate(((fx, fu, ku), (fy, fv, kv))):
            part, rows = side(i, x, south.at[n], north.at[n])
            out[sl, :] = only(wet[sl, :] > 0, DTB * jnp.concatenate([part[rows, :], halo[n]], axis=1))

    skewed((turn, build), TILES, ET)
    norm = 6.0 / (SUB * (SUB + 1) * (SUB + 2))

    def stage(first, last, lo, hi):
        def step(n, _):
            tx, ty = tide[0, n], tide[1, n]
            w = norm * ((n + 1) * (SUB - n)).astype(F32)

            def west(i):
                return from_west(tu[tile_rows(i), :])

            def surface(i, u_w):
                sl = tile_rows(i)
                vn = tv[sl, :]
                south = tv[tile_rows(i - 1), :] if i else zero
                e = eta[sl, :] - DTB * ((tu[sl, :] - u_w) + (vn - down_row(vn, south, row)))
                eta[sl, :] = e
                return from_east(e)

            def update(i, e_e):
                sl = tile_rows(i)
                e = eta[sl, :]
                un = tu[sl, :] + (cu[sl, :] * (tx - (e_e - e)) + fu[sl, :])
                tu[sl, :] = un
                if lo_bar <= i < hi_bar:
                    ub[sl, :] = ub[sl, :] + w * un
                if i > lo:
                    north(i - 1, e, ty, w)

            skewed((lambda i: west(lo + i), lambda i, x: surface(lo + i, x), lambda i, x: update(lo + i, x)), TILES, hi - lo)
            north(hi - 1, eta[tile_rows(hi - 1), :], ty, w)
            return 0

        lax.fori_loop(first, last, step, 0)

    lo_bar, hi_bar = HT - 1, HT + NB

    def north(i, ahead, ty, w):
        sl = tile_rows(i)
        e = eta[sl, :]
        x = tv[sl, :] + (cv[sl, :] * (ty - (up_row(e, ahead, row) - e)) + fv[sl, :])
        tv[sl, :] = x
        if lo_bar <= i < hi_bar:
            vb[sl, :] = vb[sl, :] + w * x

    for s in range(0, SUB, 8):
        stage(s, min(s + 8, SUB), s // 8, ET - s // 8)
    eta_o[:] = eta[HR : HR + NR, :NC]
    u_o[:] = tu[HR : HR + NR, :NC]
    v_o[:] = tv[HR : HR + NR, :NC]
    ub_o[:] = ub[HR - 8 : HR + NR, :]
    vb_o[:] = vb[HR - 8 : HR + NR, :]
    net.wait(late)


def subcycles(sizes, *args):
    vm = pl.BlockSpec(memory_space=VM)
    outs = [shape(NR, NC)] * 3 + [shape(NR + 8, EC)] * 2 + [shape(NR, LN)] * 2 + [shape(3, LP, NC)] * 2
    sems = [pltpu.SemaphoreType.DMA((6 + 4 + 5,))] * 2
    wide = [VM((ER, EC), F32)] * 9
    return pl.pallas_call(
        functools.partial(subcycle_kernel, sizes),
        in_specs=[vm] * 9 + [pl.BlockSpec(memory_space=pltpu.SMEM)] + [vm] * 5 + [pl.BlockSpec(memory_space=pl.ANY)],
        out_specs=[vm] * len(outs),
        out_shape=outs,
        scratch_shapes=wide + [VM((NR, LN), F32)] + [VM((2, HR, NC), F32)] * 2 + strip_scratch(1) + sems,
        compiler_params=pltpu.CompilerParams(collective_id=1, has_side_effects=True, vmem_limit_bytes=22 << 20),
        name="subcycles",
    )(*args)


def finish_kernel(*refs):
    ins, kvs, dvs, vbs, eta, tu, tv, rnorth, rsouth, rown, eta_o, tu_o, tv_o, uo, vo, to, so, ct, cs = refs[:23], *refs[23:]
    cubes, planes, wide = ins[:4], ins[4:9], ins[9:]
    b = pl.program_id(0)
    eta_o[:] = eta[:]
    tu_o[:] = tu[:]
    tv_o[:] = tv[:]

    @pl.when(b == 0)
    def _():
        lev = iota((LP, NC), 0).astype(F32)
        kx = kvs[LAST, :NC]
        cor = correction(vbs[LAST, :NC], rsouth[0, one(NL), :], kx, dvs[LAST, :NC])
        vel = 0.5 * only(lev < kx, rsouth[0] + cor)
        ft = vel * (rsouth[1] + rown[0, 0])
        fs = vel * (rsouth[2] + rown[0, 1])
        for k in range(NL):
            ct[k, LAST, :] = ft[one(k), :]
            cs[k, LAST, :] = fs[one(k), :]

    for half in range(2):
        sl = tile_rows(half)
        outs = [x.at[:, sl, :] for x in (uo, vo, to, so)]
        last = (b == NB // 2 - 1) if half else None
        finish_rows(last, *[x.at[half] for x in cubes], *[x[sl, :] for x in planes], *wide[half::2], rnorth, *outs, ct, cs)


def correction(mean, total, k, dz):
    deep = k * dz
    return (mean - total) / jnp.where(deep > 0, deep, 1.0)


def finish_rows(last, us, vs, t, s, cnt, su, sv, rwv, rev, ku, kv, du, dv, ub, vb, first, rnorth, uo, vo, to, so, ct, cs):
    row = iota(ROW, 0)
    lane = iota(TILE, 1)

    kx, ky = ku[:], kv[:, :NC]
    tot = jnp.concatenate([su, lane_to(rwv, 3 * NL, LN - 1)], axis=1)
    cx = correction(ub[:], tot, kx, du[:])
    cy = correction(vb[:, :NC], sv, ky, dv[:, :NC])
    fields = ((t, to, ct), (s, so, cs))

    def load(k):
        out = [lane_to(rwv, k, LN - 1)]
        for i in range(2):
            base = NL * (i + 1) + k
            out.append(jnp.where(lane == 0, lane_to(rev, base, 0), lane_to(rwv, base, LN - 1)))
        return out

    def east(k, halo):
        wide = [jnp.concatenate([f[0][k], h], axis=1) for f, h in zip(fields, halo[1:])]
        return halo[0], [x + from_east(x) for x in wide]

    def flux(k, arg):
        halo, sums = arg
        ue = only(k < kx, jnp.concatenate([us[k], halo], axis=1) + cx)
        uo[k] = ue[:, :NC]
        half = 0.5 * ue
        f = [half * x for x in sums]
        return [(x - from_west(x))[:, :NC] for x in f]

    def store(k, div):
        ve = only(k < ky, vs[k] + cy)
        vo[k] = ve
        hy = 0.5 * ve
        for i, (x, out, carry) in enumerate(fields):
            own = x[k]
            north = first[0, i, one(k), :]
            if last is not None:
                north = jnp.where(last, rnorth[i, one(k), :], north)
            fy = hy * (own + up_row(own, north, row))
            new = own - DT * (div[i] + (fy - down_row(fy, carry[k], row)))
            carry[k] = fy
            out[k] = only(k < cnt, new)

    skewed((load, east, flux, store), GROUP_F)


def finish(us, vs, tm, sm, first, kmt, geo, ub, vb, su, sv, rw, re, rnorth, rsouth, state):
    kv, dv = geo[1], geo[3]

    def rows(width):
        return pl.BlockSpec((16, width), lambda b: (b, 0))

    def pair(start):
        return [pl.BlockSpec(WIDE, lambda b, h=h: (start + 2 * b + h, 0)) for h in range(2)]

    def fixed(i):
        return pl.BlockSpec(WIDE, lambda b: (i, 0))

    ahead = [first_rows(lambda b: 2 * b + 1), first_rows(lambda b: jnp.minimum(2 * b + 2, NB - 1))]
    cube = pl.BlockSpec((NL, 16, NC), lambda b: (0, b, 0))
    south = [fixed(HT - 1)] * 2 + [fixed(0)]
    wide = [x for x in (*geo, ub, vb, first) for _ in range(2)]
    return pl.pallas_call(
        finish_kernel,
        grid=(NB // 2,),
        in_specs=[block_major(lambda b: b, 2)] * 4 + [rows(NC)] * 3 + [rows(LN)] * 2 + pair(HT) * 4 + pair(1) * 2 + ahead + south + [rows(NC)] * 3 + [whole(3, LP, NC)] * 2 + [first_rows(lambda b: 0)],
        out_specs=[rows(NC)] * 3 + [cube] * 4,
        out_shape=[shape(NR, NC)] * 3 + [shape(NL, NR, NC)] * 4,
        scratch_shapes=[VM(SLAB, F32)] * 2,
        compiler_params=pltpu.CompilerParams(vmem_limit_bytes=26 << 20),
        name="finish",
    )(us, vs, tm, sm, kmt, su, sv, rw, re, *wide, kv, dv, vb, *state, rnorth, rsouth, first)


def solution(mesh):
    sizes = mesh.shape["row"], mesh.shape["col"]

    def local_step(u, v, t, s, eta, tu, tv, depth, kmt, tide):
        u, v, t, s, eta, tu, tv, depth, kmt = (pltpu.with_memory_space_constraint(x, pltpu.HBM) for x in (u, v, t, s, eta, tu, tv, depth, kmt))
        tm, sm, pr, tke, tkw, trn, first, rw, re, rsouth, rnorth, corner, rown, *wide = tracers(sizes, t, s, u, v, kmt, depth, eta, tu, tv)
        geo, state = wide[:4], wide[4:]
        tm, sm = (pltpu.with_memory_space_constraint(x, pltpu.VMEM) for x in (tm, sm))
        first = pltpu.with_memory_space_constraint(first, pltpu.HBM)
        pr = pltpu.with_memory_space_constraint(pr, pltpu.HBM)
        us, vs, fx, fy, su, sv, uke, vrow = momentum(u, v, pr, first, geo, rw, re, rnorth, rsouth, rown, corner)
        eta_n, u_n, v_n, ub, vb, fw, fe, fsouth, fnorth = subcycles(sizes, *state, *geo, fx, fy, tide.T, uke, tke, tkw, vrow, trn, first)
        us = pltpu.with_memory_space_constraint(us, pltpu.VMEM)
        vs = pltpu.with_memory_space_constraint(vs, pltpu.HBM)
        return finish(us, vs, tm, sm, first, kmt, geo, ub, vb, su, sv, fw, fe, fnorth, fsouth, (eta_n, u_n, v_n))

    cube, plane = P(None, "row", "col"), P("row", "col")
    return jax.shard_map(
        local_step,
        mesh=mesh,
        in_specs=(cube,) * 4 + (plane,) * 5 + (P(None, None),),
        out_specs=(plane,) * 3 + (cube,) * 4,
        check_vma=False,
    )
```

```python
import functools

import jax
import jax.numpy as jnp
from jax import lax
from jax.experimental import pallas as pl
from jax.experimental.pallas import tpu as pltpu
from jax.sharding import PartitionSpec as P

NL = 41
NR = 96
NC = 512
LN = 128
LP = 48
HR = 40
ER = NR + 2 * HR
EC = NC + 128
NB = NR // 8
SUB = 36
GROUP_M = 2
GROUP_F = 3
HALF = 64
SIDES = (-1, 0, 1)
FIRST, LAST = slice(0, 1), slice(7, 8)
TILES = 3
DT = 4.0
DTB = DT / SUB
KV = 0.001
KT = 0.0005
F32 = jnp.float32
HT = HR // 8
ET = ER // 8
SLAB, ROW, WIDE, TILE = (NL, 8, NC), (8, NC), (8, EC), (8, LN)
VM = pltpu.VMEM


def only(mask, x):
    return jnp.where(mask, x, jnp.zeros_like(x))


def iota(shape, dim):
    return lax.broadcasted_iota(jnp.int32, shape, dim)


def whole(*shape):
    return pl.BlockSpec(shape, lambda *_: (0,) * len(shape))


def shape(*dims):
    return jax.ShapeDtypeStruct(dims, F32)


def one(k):
    return slice(k, k + 1)


def tile_rows(i):
    return slice(8 * i, 8 * (i + 1))


def from_west(x):
    return pltpu.roll(x, 1, axis=1)


def from_east(x):
    return pltpu.roll(x, x.shape[1] - 1, axis=1)


def lane_to(x, src, dst):
    shift = (dst - src) % LN
    return x if shift == 0 else pltpu.roll(x, shift, axis=1)


def up_row(x, nxt, row):
    return pltpu.roll(jnp.where(row == 0, nxt, x), 7, axis=0)


def down_row(x, prev, row):
    return pltpu.roll(jnp.where(row == 7, prev, x), 1, axis=0)


def skewed(stages, group, count=NL):
    blocks = [range(k, min(k + group, count)) for k in range(0, count, group)]
    held = {}
    for i in range(len(blocks) + len(stages) - 1):
        for n, stage in enumerate(stages):
            if 0 <= i - n < len(blocks):
                for k in blocks[i - n]:
                    held[k] = stage(k, held[k]) if n else stage(k)


def couple(count, thick, kappa):
    safe = jnp.where(count > 0, thick, 1.0)
    return DT * kappa / (safe * safe)


def pressure_step(t, s, wet, cum, thick):
    half = only(wet, 0.5 * (0.015 * (s - 1.0) - 0.02 * (t - 1.0)))
    mid = cum + half
    return thick * mid, mid + half


class Exchange:
    def __init__(self, sizes, send_sem, recv_sem):
        self.rows, self.cols = sizes
        self.row, self.col = lax.axis_index("row"), lax.axis_index("col")
        self.sems = send_sem, recv_sem
        self.used = 0

    def inside(self, drow):
        return (self.row + drow >= 0) & (self.row + drow < self.rows)

    def at(self, drow, dcol):
        return {"row": self.row + drow, "col": lax.rem(self.col + dcol + self.cols, self.cols)}

    def when(self, drow, action):
        if drow:
            pl.when(self.inside(drow))(action)
        else:
            action()

    def announce(self):
        ready = pltpu.get_barrier_semaphore()
        for drow in SIDES:
            for dcol in SIDES:
                if drow or dcol:
                    self.when(drow, functools.partial(pl.semaphore_signal, ready, device_id=self.at(drow, dcol), device_id_type=pl.DeviceIdType.MESH))

    def ready(self):
        per_row = len(SIDES)
        known = [self.inside(drow).astype(jnp.int32) for drow in SIDES if drow]
        pl.semaphore_wait(pltpu.get_barrier_semaphore(), per_row - 1 + per_row * sum(known))

    def clear(self, plan):
        for _, dst, drow, _ in plan:
            if drow:

                @pl.when(jnp.logical_not(self.inside(-drow)))
                def _():
                    dst[:] = jnp.zeros(dst.shape, F32)

    def make(self, plan):
        out = []
        for src, dst, drow, dcol in plan:
            copy = pltpu.make_async_remote_copy(
                src_ref=src,
                dst_ref=dst,
                send_sem=self.sems[0].at[self.used],
                recv_sem=self.sems[1].at[self.used],
                device_id=self.at(drow, dcol),
                device_id_type=pl.DeviceIdType.MESH,
            )
            self.used += 1
            out.append((copy, drow))
        return out

    def start(self, copies):
        for copy, drow in copies:
            self.when(drow, copy.start)

    def wait(self, copies):
        for copy, drow in copies:
            self.when(drow, copy.wait_send)
            self.when(-drow, copy.wait_recv)


def pack_strips(pairs, to_west, to_east):
    lane = iota(TILE, 1)
    first, last = slice(0, LN), slice(NC - LN, NC)

    def turn(n):
        q, sl = n // NB, tile_rows(n % NB)
        b = pairs[q][-1]
        return pltpu.roll(b[sl, first], HALF, axis=1), pltpu.roll(b[sl, last], HALF, axis=1)

    def store(n, turned):
        q, sl = n // NB, tile_rows(n % NB)
        a = pairs[q][0]
        to_west[q, sl, :] = jnp.where(lane < HALF, a[sl, first], turned[0])
        to_east[q, sl, :] = jnp.where(lane < HALF, turned[1], a[sl, last])

    skewed((turn, store), NB, NB * len(pairs))


def strip_plan(to_west, to_east, strips):
    top, bottom = pl.ds(NR - HR, HR), pl.ds(0, HR)
    return [
        (to_east, strips[0], 0, 1),
        (to_west, strips[1], 0, -1),
        (to_east.at[:, top], strips[2], 1, 1),
        (to_west.at[:, top], strips[3], 1, -1),
        (to_east.at[:, bottom], strips[4], -1, 1),
        (to_west.at[:, bottom], strips[5], -1, -1),
    ]


def row_plan(planes, south, north):
    plan = []
    for i, x in enumerate(planes):
        plan.append((x.at[pl.ds(NR - HR, HR), :], south.at[i], 1, 0))
        plan.append((x.at[pl.ds(0, HR), :], north.at[i], -1, 0))
    return plan


def strip_scratch(n):
    return [VM((n, NR, LN), F32)] * 4 + [VM((n, HR, LN), F32)] * 4


def side(i, own, south, north):
    if i < HT:
        return south, tile_rows(i)
    return (own, tile_rows(i - HT)) if i < HT + NB else (north, tile_rows(i - HT - NB))


def halo_pair(i, q, strips):
    (w, e), sl = side(i, strips[:2], strips[2:4], strips[4:])
    lane = iota(TILE, 1)
    w, e = w[q, sl, :], e[q, sl, :]
    return jnp.where(lane < HALF, e, w), pltpu.roll(jnp.where(lane < HALF, w, e), HALF, axis=1)


def mix_tracers(t, s, cnt, depth, strips, tm, sm, pr, pke, pkw, tke, tkw, rs, gains):
    lane = iota(TILE, 1)
    thick = depth / jnp.maximum(cnt, 1).astype(F32)
    c = couple(cnt, thick, KT)
    zero = jnp.zeros(ROW, F32)
    cum = lower = pt = ps = zero
    keep = zero
    ae = aw = jnp.zeros(TILE, F32)
    u0, u3, v0, v3 = strips
    for k in range(NL):
        wet = k < cnt
        tk, sk = t[k], s[k]
        p, cum = pressure_step(tk, sk, wet, cum, thick)
        pr[k] = p
        for n, (x0, x3) in enumerate(((u0, u3), (v0, v3))):
            base = NL * n + k
            ae = jnp.where(lane == base, lane_to(x3[k], LN - 1, base), ae)
            aw = jnp.where(lane == base, lane_to(x0[k], 0, base), aw)
        aw = jnp.where(lane == 2 * NL + k, lane_to(p[:, :LN], 0, 2 * NL + k), aw)
        rs[2, one(k), :] = p[FIRST, :]
        upper = jnp.where(k + 1 < cnt, c, 0.0) if k + 1 < NL else zero
        top = 1.0 + lower * keep if k else jnp.ones_like(zero)
        inv = 1.0 / (top + upper)
        keep = top * inv
        gains[k] = upper * inv
        pt = (jnp.where(wet, tk, 0.0) + lower * pt) * inv
        ps = (jnp.where(wet, sk, 0.0) + lower * ps) * inv
        tm[k] = pt
        sm[k] = ps
        lower = upper
    pke[:] = ae
    pkw[:] = aw
    ae = aw = jnp.zeros(TILE, F32)
    bt = bs = zero
    for k in reversed(range(NL)):
        gain = gains[k]
        bt = tm[k] + gain * bt
        bs = sm[k] + gain * bs
        tm[k] = bt
        sm[k] = bs
        rs[0, one(k), :] = bt[FIRST, :]
        rs[1, one(k), :] = bs[FIRST, :]
        for x, base in ((bt, NL), (bs, 2 * NL)):
            ae = jnp.where(lane == base + k, lane_to(x[:, NC - LN :], LN - 1, base + k), ae)
            aw = jnp.where(lane == base + k, lane_to(x[:, :LN], 0, base + k), aw)
    tke[:] = ae
    tkw[:] = aw


def wide_geometry(planes, strips, south, north, outs):
    ku, kv, du, dv, *state = outs
    row = iota(WIDE, 0)

    def turn(i):
        return [halo_pair(i, q, strips) for q in range(3)]

    def build(i, halo):
        halo = [x for pair in halo for x in pair]
        vals = []
        for n in range(len(planes)):
            part, sl = side(i, planes[n], south.at[n], north.at[n])
            vals.append(jnp.concatenate([part[sl, :], halo[n]], axis=1))
        k, h = vals[:2]
        dz = h / jnp.maximum(k, 1.0)
        kv[tile_rows(i), :] = k
        dv[tile_rows(i), :] = dz
        return vals[2:], from_east(k), from_east(dz)

    def store(i, arg):
        vals, ke, dze = arg
        sl = tile_rows(i)
        hi = tile_rows(min(i + 1, ET - 1))
        k, dz = kv[sl, :], dv[sl, :]
        k_u, k_v = jnp.minimum(k, ke), jnp.minimum(k, up_row(k, kv[hi, :], row))
        dv[sl, :] = 0.5 * (dz + up_row(dz, dv[hi, :], row))
        du[sl, :] = 0.5 * (dz + dze)
        ku[sl, :] = k_u
        kv[sl, :] = k_v
        for out, x, wet in zip(state, vals, (k, k_u, k_v)):
            out[sl, :] = only(wet > 0, x)

    skewed((turn, build, store), TILES, ET)


def tracer_kernel(sizes, t, s, u0, u3, v0, v3, kc, hc, uf, ul, vf, vl, kmt, depth, eta, tu, tv, *rest):
    tm_b, sm_b, pr_b, tke, tkw, rn, rs_b, *rest = rest
    received, rown, wide, rest = rest[:5], rest[5], rest[6:13], rest[13:]
    gains, kf, pke, pkw, prn, prs, south, north, rw, re, rsouth, rnorth, corner, to_west, to_east, *strips, send_sem, recv_sem = rest
    b = pl.program_id(0)
    last = NB // 2 - 1
    net = Exchange(sizes, send_sem, recv_sem)
    planes = (kf, depth, eta, tu, tv)
    head = strip_plan(to_west, to_east, strips) + [(prn, rsouth, 1, 0)] + row_plan(planes, south, north)
    middle = [(prs, rnorth, -1, 0), (pke.at[pl.ds(0, 8), :], rw.at[pl.ds(NR, 8), :], -1, 1)]
    tail = [(pkw.at[pl.ds(NR - 8, 8), :], corner, 1, -1)]

    def piece(i):
        part = pl.ds(16 * i, 16)
        return net.make([(pke.at[part, :], rw.at[part, :], 0, 1), (pkw.at[part, :], re.at[part, :], 0, -1)])

    first_plan = head + middle + tail
    head, middle, tail = net.make(head), net.make(middle), net.make(tail)
    pieces = [piece(i) for i in range(last + 1)]

    @pl.when(b == 0)
    def _():
        net.clear(first_plan)
        net.announce()
        kf[:] = kmt[:].astype(F32)
        pack_strips((planes[:2], planes[2:4], planes[4:]), to_west, to_east)
        prn[:] = jnp.zeros(prn.shape, F32)
        prs[:] = jnp.zeros(prs.shape, F32)
        for k in range(NL):
            for n, (lo, hi) in enumerate(((uf, ul), (vf, vl))):
                prn[n, one(k), :] = hi[k, LAST, :]
                prs[n, one(k), :] = lo[k, FIRST, :]
        net.ready()
        net.start(head)

    for i in range(last):

        @pl.when(b == i + 1)
        def _():
            net.start(pieces[i])

    for half in range(2):
        sl = tile_rows(half)
        tm, sm, rs = tm_b.at[half], sm_b.at[half], rs_b.at[half]
        out = pl.ds(pl.multiple_of(16 * b + 8 * half, 8), 8)
        parts = [x.at[:, sl, :] for x in (t, s, u0, u3, v0, v3)]
        mix_tracers(*parts[:2], kc[sl, :], hc[sl, :], parts[2:], tm, sm, pr_b.at[half], pke.at[out, :], pkw.at[out, :], tke.at[sl, :], tkw.at[sl, :], rs, gains)

    @pl.when(b == 0)
    def _():
        prs[2] = rs_b[0, 2]
        net.start(middle)

    @pl.when(b == last)
    def _():
        net.start(pieces[last] + tail)
        for k in range(NL):
            rn[0, one(k), :] = tm[k, LAST, :]
            rn[1, one(k), :] = sm[k, LAST, :]
        rown[:] = prs[:]
        net.wait(head)
        wide_geometry(planes, strips, south, north, wide)
        net.wait(middle + tail)
        for copies in pieces:
            net.wait(copies)
        for out, x in zip(received, (rw, re, rsouth, rnorth, corner)):
            out[:] = x[:]


PACK = VM((NB,) + SLAB, F32)
PACK_HBM = pltpu.HBM((NB,) + SLAB, F32)


def block_major(f, n=1):
    return pl.BlockSpec((n,) + SLAB, lambda b: (f(b), 0, 0, 0))


def first_rows(f, n=1):
    return pl.BlockSpec((n, 3, LP, NC), lambda b: (f(b), 0, 0, 0))


def tracers(sizes, t, s, u, v, kmt, depth, eta, tu, tv):
    def cols(width, j):
        return pl.BlockSpec((NL, 16, width), lambda b: (0, b, j))

    def slab(i):
        return pl.BlockSpec(SLAB, lambda b: (0, i, 0))

    pack = block_major(lambda b: b, 2)
    plane = pl.BlockSpec((16, NC), lambda b: (b, 0))
    col = pl.BlockSpec((16, LN), lambda b: (b, 0))
    ends = [slab(0), slab(NB - 1)]
    edge = [(NR + 8, LN), (NR, LN), (2, LP, NC), (3, LP, NC), (8, LN)]
    extra = edge + [(3, LP, NC)] + [(ER, EC)] * 7
    sems = [pltpu.SemaphoreType.DMA((6 + 1 + 10 + 3 + NB,))] * 2
    rows = [VM((2, LP, NC), F32), VM((3, LP, NC), F32)] + [VM((5, HR, NC), F32)] * 2
    return pl.pallas_call(
        functools.partial(tracer_kernel, sizes),
        grid=(NB // 2,),
        in_specs=[cols(NC, 0)] * 2 + [cols(LN, 0), cols(LN, 3)] * 2 + [plane] * 2 + ends * 2 + [whole(NR, NC)] * 5,
        out_specs=[pack] * 3 + [col] * 2 + [whole(2, LP, NC), first_rows(lambda b: b, 2)] + [whole(*x) for x in extra],
        out_shape=[PACK] * 2 + [PACK_HBM] + [shape(NR, LN)] * 2 + [shape(2, LP, NC), pltpu.HBM((NB, 3, LP, NC), F32)] + [shape(*x) for x in extra],
        scratch_shapes=[VM(SLAB, F32), VM((NR, NC), F32)] + [VM((NR, LN), F32)] * 2 + rows + [VM(x, F32) for x in edge] + strip_scratch(3) + sems,
        compiler_params=pltpu.CompilerParams(collective_id=0, has_side_effects=True, vmem_limit_bytes=26 << 20),
        name="tracers",
    )(t, s, u, u, v, v, kmt, depth, u, u, v, v, kmt, depth, eta, tu, tv)


def solve_pair(src_a, src_b, ca, cb, na, nb, out_a, out_b, gain_a, gain_b):
    zero = jnp.zeros(ROW, F32)
    la = lb = pa = pb = wa = wb = zero
    for k in range(NL):
        ua = jnp.where(k + 1 < na, ca, 0.0) if k + 1 < NL else zero
        ub = jnp.where(k + 1 < nb, cb, 0.0) if k + 1 < NL else zero
        ta = 1.0 + la * wa if k else jnp.ones_like(zero)
        tb = 1.0 + lb * wb if k else jnp.ones_like(zero)
        ia = 1.0 / (ta + ua)
        ib = 1.0 / (tb + ub)
        wa, wb = ta * ia, tb * ib
        gain_a[k] = ua * ia
        gain_b[k] = ub * ib
        pa = (src_a[k] + la * pa) * ia
        pb = (src_b[k] + lb * pb) * ib
        src_a[k] = pa
        src_b[k] = pb
        la, lb = ua, ub
    xa = xb = sa = sb = zero
    for k in reversed(range(NL)):
        xa = src_a[k] + gain_a[k] * xa
        xb = src_b[k] + gain_b[k] * xb
        out_a[k] = xa
        out_b[k] = xb
        sa += xa
        sb += xb
    return sa, sb


def momentum_kernel(
    u, v, p_b, pfirst, kun, kvn, kux, kvx, du, dv, kus, kvs, rwn, ren, re, rnorth, rsouth, rown, corner,
    us_b, vs_b, fx, fy, su, sv, pke, vrow,
    cc, hh, srcu, srcv, gu, gv, ums, vms,
):
    step = pl.program_id(0)
    last = step == NB
    us, vs, p = us_b.at[0], vs_b.at[0], p_b.at[0]
    row = iota(ROW, 0)
    rowx = iota(WIDE, 0)
    lane = iota(TILE, 1)
    kxn, kyn = kun[:], kvn[:]
    rwv, rev = rwn[:], ren[:]

    def halos(k):
        hu = jnp.where(lane == 0, lane_to(rev, k, 0), lane_to(rwv, k, LN - 1))
        hv = jnp.where(lane == 0, lane_to(rev, NL + k, 0), lane_to(rwv, NL + k, LN - 1))
        return hu, hv

    def masked(k, uk, vk, halo):
        um = only(k < kxn, jnp.concatenate([uk, halo[0]], axis=1))
        return um, only(k < kyn, jnp.concatenate([vk, halo[1]], axis=1))

    @pl.when(step == 0)
    def _():
        for k in range(NL):
            ums[k], vms[k] = masked(k, u[k], v[k], halos(k))
        lev = iota((LP, NC), 0).astype(F32)
        lev1 = iota((LP, LN), 0)
        ks, kw = kus[LAST, :NC], kvs[LAST, :NC]
        s_u = only(lev < ks, rsouth[0])
        s_v = only(lev < kw, rsouth[1])
        pick = only(iota((LP, LN), 1) == lev1 + NL, corner[LAST, :])
        edge = jnp.sum(pick, axis=1, keepdims=True)
        edge = only(lev[:, :1] < kvs[LAST, one(NC)], edge)
        s_ve = jnp.where(iota((LP, NC), 1) == NC - 1, edge, from_east(s_v))
        u_0 = only(lev < kxn[FIRST, :NC], rown[0])
        v_0 = only(lev < kyn[FIRST, :NC], rown[1])
        c_s = (0.25 * (s_v + s_ve)) * (s_u + u_0)
        h_s = 0.5 * (s_v + v_0)
        h_s = h_s * h_s + rown[2]
        for k in range(NL):
            cc[k, LAST, :] = c_s[one(k), :]
            hh[k, LAST, :] = h_s[one(k), :]

    @pl.when(step > 0)
    def _():
        kx, ky = kux[:], kvx[:]
        pev = re[:]
        total = [jnp.zeros(ROW, F32)] * 2

        def edge(k):
            return halos(k) + (lane_to(pev, 2 * NL + k, 0),)

        def shift(k, halo):
            um, vm = ums[k], vms[k]
            uk = jnp.where(last, rnorth[0, one(k), :], u[k])
            vk = jnp.where(last, rnorth[1, one(k), :], v[k])
            pe = jnp.concatenate([p[k], halo[2]], axis=1)
            return masked(k, uk, vk, halo), pe, from_west(um), from_east(vm)

        def flux(k, arg):
            new, pe, u_w, v_e = arg
            um, vm = ums[k], vms[k]
            c = (0.25 * (vm + v_e)) * (um + up_row(um, new[0], rowx))
            g = 0.5 * (u_w + um)
            g = g * g + pe
            c5 = c[:, :NC]
            return new, from_east(g)[:, :NC] - g[:, :NC], c5, c5 - from_west(c)[:, :NC]

        def tend(k, arg):
            new, dx, c5, dc = arg
            u5, v5, pk = ums[k, :, :NC], vms[k, :, :NC], p[k]
            north = jnp.where(last, rnorth[2, one(k), :], pfirst[0, 2, one(k), :])
            h = 0.5 * (v5 + up_row(v5, new[1][:, :NC], row))
            h = h * h + up_row(pk, north, row)
            tu = only(k < kx, dx + (c5 - down_row(c5, cc[k], row)))
            tv = only(k < ky, (h - down_row(h, hh[k], row)) + dc)
            total[0] += tu
            total[1] += tv
            srcu[k] = u5 - DT * tu
            srcv[k] = v5 - DT * tv
            cc[k] = c5
            hh[k] = h
            ums[k], vms[k] = new

        skewed((edge, shift, flux, tend), GROUP_M)
        dzu, dzv = du[:], dv[:]
        fx[:] = -dzu * total[0]
        fy[:] = -dzv * total[1]
        sa, sb = solve_pair(srcu, srcv, couple(kx, dzu, KV), couple(ky, dzv, KV), kx, ky, us, vs, gu, gv)
        sa, sb = dzu * sa, dzv * sb
        su[:] = sa
        sv[:] = sb
        ae = jnp.zeros(TILE, F32)
        for k in range(NL):
            ae = jnp.where(lane == k, lane_to(us[k, :, NC - LN :], LN - 1, k), ae)
        pke[:] = jnp.where(lane == 3 * NL, lane_to(sa[:, NC - LN :], LN - 1, 3 * NL), ae)

        @pl.when(last)
        def _():
            for k in range(NL):
                vrow[one(k), :] = vs[k, LAST, :]
            vrow[one(NL), :] = sb[LAST, :]
            vrow[NL + 1 : LP, :] = jnp.zeros((LP - NL - 1, NC), F32)


def momentum(u, v, p, first, geo, rw, re, rnorth, rsouth, rown, corner):
    ku, kv, du, dv = geo

    def this(b):
        return jnp.maximum(b, 1) - 1

    def ahead(b):
        return jnp.minimum(b, NB - 1)

    cube = pl.BlockSpec(SLAB, lambda b: (0, ahead(b), 0))
    pack = block_major(this)
    near = pl.BlockSpec(ROW, lambda b: (HT + this(b), 0))
    widn = pl.BlockSpec(WIDE, lambda b: (HT + b, 0))
    wids = pl.BlockSpec(WIDE, lambda b: (HT - 1, 0))
    plane = pl.BlockSpec(ROW, lambda b: (this(b), 0))
    col = pl.BlockSpec(TILE, lambda b: (this(b), 0))
    colw = pl.BlockSpec(TILE, lambda b: (b, 0))
    cole = pl.BlockSpec(TILE, lambda b: (ahead(b), 0))
    flat = jax.ShapeDtypeStruct((NR, NC), F32)

    def rows(n):
        return pl.BlockSpec((n, LP, NC), lambda b: (0, 0, 0))

    return pl.pallas_call(
        momentum_kernel,
        grid=(NB + 1,),
        in_specs=[cube, cube, pack, first_rows(ahead), widn, widn, near, near, near, near, wids, wids, colw, cole, col, rows(3), rows(2), rows(3), pl.BlockSpec(TILE, lambda b: (0, 0))],
        out_specs=[pack, pack, plane, plane, plane, plane, col, pl.BlockSpec((LP, NC), lambda b: (0, 0))],
        out_shape=[PACK, PACK_HBM, flat, flat, flat, flat, jax.ShapeDtypeStruct((NR, LN), F32), jax.ShapeDtypeStruct((LP, NC), F32)],
        scratch_shapes=[VM(SLAB, F32)] * 6 + [VM((NL,) + WIDE, F32)] * 2,
        compiler_params=pltpu.CompilerParams(vmem_limit_bytes=22 << 20),
        name="momentum",
    )(u, v, p, first, ku, kv, ku, kv, du, dv, ku, kv, rw, re, re, rnorth, rsouth, rown, corner)


def subcycle_kernel(
    sizes, eta_i, tu_i, tv_i, ku, kv, du, dv, fx, fy, tide, uke, tke, tkw, vrow, trn, trs,
    eta_o, u_o, v_o, ub_o, vb_o, fw, fe, fsouth, fnorth,
    eta, tu, tv, cu, cv, fu, fv, ub, vb, edge, south, north, *rest,
):
    to_west, to_east, *strips, send_sem, recv_sem = rest
    net = Exchange(sizes, send_sem, recv_sem)
    plan = strip_plan(to_west, to_east, strips) + row_plan((fx, fy), south, north)
    late = [
        (edge, fw, 0, 1),
        (tkw, fe, 0, -1),
        (vrow, fsouth.at[0], 1, 0),
        (trn, fsouth.at[pl.ds(1, 2)], 1, 0),
        (trs.at[0], fnorth, -1, 0),
    ]
    net.clear(plan + late)
    net.announce()
    edge[:] = uke[:] + tke[:]
    pack_strips(((fx, fy),), to_west, to_east)
    row = iota(WIDE, 0)
    zero = jnp.zeros(WIDE, F32)
    ub[:] = jnp.zeros(ub.shape, F32)
    vb[:] = jnp.zeros(vb.shape, F32)
    eta[:] = eta_i[:]
    tu[:] = tu_i[:]
    tv[:] = tv_i[:]
    plan, late = net.make(plan), net.make(late)
    net.ready()
    net.start(plan)
    cu[:] = DTB * (ku[:] * du[:])
    cv[:] = DTB * (kv[:] * dv[:])
    net.wait(plan)
    net.start(late)

    def turn(i):
        return halo_pair(i, 0, strips)

    def build(i, halo):
        sl = tile_rows(i)
        for n, (x, out, wet) in enumerate(((fx, fu, ku), (fy, fv, kv))):
            part, rows = side(i, x, south.at[n], north.at[n])
            out[sl, :] = only(wet[sl, :] > 0, DTB * jnp.concatenate([part[rows, :], halo[n]], axis=1))

    skewed((turn, build), TILES, ET)
    norm = 6.0 / (SUB * (SUB + 1) * (SUB + 2))

    def stage(first, last, lo, hi):
        def step(n, _):
            tx, ty = tide[0, n], tide[1, n]
            w = norm * ((n + 1) * (SUB - n)).astype(F32)

            def west(i):
                return from_west(tu[tile_rows(i), :])

            def surface(i, u_w):
                sl = tile_rows(i)
                vn = tv[sl, :]
                south = tv[tile_rows(i - 1), :] if i else zero
                e = eta[sl, :] - DTB * ((tu[sl, :] - u_w) + (vn - down_row(vn, south, row)))
                eta[sl, :] = e
                return from_east(e)

            def update(i, e_e):
                sl = tile_rows(i)
                e = eta[sl, :]
                un = tu[sl, :] + (cu[sl, :] * (tx - (e_e - e)) + fu[sl, :])
                tu[sl, :] = un
                if lo_bar <= i < hi_bar:
                    ub[sl, :] = ub[sl, :] + w * un
                if i > lo:
                    north(i - 1, e, ty, w)

            skewed((lambda i: west(lo + i), lambda i, x: surface(lo + i, x), lambda i, x: update(lo + i, x)), TILES, hi - lo)
            north(hi - 1, eta[tile_rows(hi - 1), :], ty, w)
            return 0

        lax.fori_loop(first, last, step, 0)

    lo_bar, hi_bar = HT - 1, HT + NB

    def north(i, ahead, ty, w):
        sl = tile_rows(i)
        e = eta[sl, :]
        x = tv[sl, :] + (cv[sl, :] * (ty - (up_row(e, ahead, row) - e)) + fv[sl, :])
        tv[sl, :] = x
        if lo_bar <= i < hi_bar:
            vb[sl, :] = vb[sl, :] + w * x

    for s in range(HT):
        stage(max(8 * s - 3, 0), min(8 * s + 5, SUB), s, ET - s)
    eta_o[:] = eta[HR : HR + NR, :NC]
    u_o[:] = tu[HR : HR + NR, :NC]
    v_o[:] = tv[HR : HR + NR, :NC]
    ub_o[:] = ub[HR - 8 : HR + NR, :]
    vb_o[:] = vb[HR - 8 : HR + NR, :]
    net.wait(late)


def subcycles(sizes, *args):
    vm = pl.BlockSpec(memory_space=VM)
    outs = [shape(NR, NC)] * 3 + [shape(NR + 8, EC)] * 2 + [shape(NR, LN)] * 2 + [shape(3, LP, NC)] * 2
    sems = [pltpu.SemaphoreType.DMA((6 + 4 + 5,))] * 2
    wide = [VM((ER, EC), F32)] * 9
    return pl.pallas_call(
        functools.partial(subcycle_kernel, sizes),
        in_specs=[vm] * 9 + [pl.BlockSpec(memory_space=pltpu.SMEM)] + [vm] * 5 + [pl.BlockSpec(memory_space=pl.ANY)],
        out_specs=[vm] * len(outs),
        out_shape=outs,
        scratch_shapes=wide + [VM((NR, LN), F32)] + [VM((2, HR, NC), F32)] * 2 + strip_scratch(1) + sems,
        compiler_params=pltpu.CompilerParams(collective_id=1, has_side_effects=True, vmem_limit_bytes=22 << 20),
        name="subcycles",
    )(*args)


def finish_kernel(*refs):
    ins, kvs, dvs, vbs, eta, tu, tv, rnorth, rsouth, rown, eta_o, tu_o, tv_o, uo, vo, to, so, ct, cs = refs[:23], *refs[23:]
    cubes, planes, wide = ins[:4], ins[4:9], ins[9:]
    b = pl.program_id(0)
    eta_o[:] = eta[:]
    tu_o[:] = tu[:]
    tv_o[:] = tv[:]

    @pl.when(b == 0)
    def _():
        lev = iota((LP, NC), 0).astype(F32)
        kx = kvs[LAST, :NC]
        cor = correction(vbs[LAST, :NC], rsouth[0, one(NL), :], kx, dvs[LAST, :NC])
        vel = 0.5 * only(lev < kx, rsouth[0] + cor)
        ft = vel * (rsouth[1] + rown[0, 0])
        fs = vel * (rsouth[2] + rown[0, 1])
        for k in range(NL):
            ct[k, LAST, :] = ft[one(k), :]
            cs[k, LAST, :] = fs[one(k), :]

    for half in range(2):
        sl = tile_rows(half)
        outs = [x.at[:, sl, :] for x in (uo, vo, to, so)]
        last = (b == NB // 2 - 1) if half else None
        finish_rows(last, *[x.at[half] for x in cubes], *[x[sl, :] for x in planes], *wide[half::2], rnorth, *outs, ct, cs)


def correction(mean, total, k, dz):
    deep = k * dz
    return (mean - total) / jnp.where(deep > 0, deep, 1.0)


def finish_rows(last, us, vs, t, s, cnt, su, sv, rwv, rev, ku, kv, du, dv, ub, vb, first, rnorth, uo, vo, to, so, ct, cs):
    row = iota(ROW, 0)
    lane = iota(TILE, 1)

    kx, ky = ku[:], kv[:, :NC]
    tot = jnp.concatenate([su, lane_to(rwv, 3 * NL, LN - 1)], axis=1)
    cx = correction(ub[:], tot, kx, du[:])
    cy = correction(vb[:, :NC], sv, ky, dv[:, :NC])
    fields = ((t, to, ct), (s, so, cs))

    def load(k):
        out = [lane_to(rwv, k, LN - 1)]
        for i in range(2):
            base = NL * (i + 1) + k
            out.append(jnp.where(lane == 0, lane_to(rev, base, 0), lane_to(rwv, base, LN - 1)))
        return out

    def east(k, halo):
        wide = [jnp.concatenate([f[0][k], h], axis=1) for f, h in zip(fields, halo[1:])]
        return halo[0], [x + from_east(x) for x in wide]

    def flux(k, arg):
        halo, sums = arg
        ue = only(k < kx, jnp.concatenate([us[k], halo], axis=1) + cx)
        uo[k] = ue[:, :NC]
        half = 0.5 * ue
        f = [half * x for x in sums]
        return [(x - from_west(x))[:, :NC] for x in f]

    def store(k, div):
        ve = only(k < ky, vs[k] + cy)
        vo[k] = ve
        hy = 0.5 * ve
        for i, (x, out, carry) in enumerate(fields):
            own = x[k]
            north = first[0, i, one(k), :]
            if last is not None:
                north = jnp.where(last, rnorth[i, one(k), :], north)
            fy = hy * (own + up_row(own, north, row))
            new = own - DT * (div[i] + (fy - down_row(fy, carry[k], row)))
            carry[k] = fy
            out[k] = only(k < cnt, new)

    skewed((load, east, flux, store), GROUP_F)


def finish(us, vs, tm, sm, first, kmt, geo, ub, vb, su, sv, rw, re, rnorth, rsouth, state):
    kv, dv = geo[1], geo[3]

    def rows(width):
        return pl.BlockSpec((16, width), lambda b: (b, 0))

    def pair(start):
        return [pl.BlockSpec(WIDE, lambda b, h=h: (start + 2 * b + h, 0)) for h in range(2)]

    def fixed(i):
        return pl.BlockSpec(WIDE, lambda b: (i, 0))

    ahead = [first_rows(lambda b: 2 * b + 1), first_rows(lambda b: jnp.minimum(2 * b + 2, NB - 1))]
    cube = pl.BlockSpec((NL, 16, NC), lambda b: (0, b, 0))
    south = [fixed(HT - 1)] * 2 + [fixed(0)]
    wide = [x for x in (*geo, ub, vb, first) for _ in range(2)]
    return pl.pallas_call(
        finish_kernel,
        grid=(NB // 2,),
        in_specs=[block_major(lambda b: b, 2)] * 4 + [rows(NC)] * 3 + [rows(LN)] * 2 + pair(HT) * 4 + pair(1) * 2 + ahead + south + [rows(NC)] * 3 + [whole(3, LP, NC)] * 2 + [first_rows(lambda b: 0)],
        out_specs=[rows(NC)] * 3 + [cube] * 4,
        out_shape=[shape(NR, NC)] * 3 + [shape(NL, NR, NC)] * 4,
        scratch_shapes=[VM(SLAB, F32)] * 2,
        compiler_params=pltpu.CompilerParams(vmem_limit_bytes=26 << 20),
        name="finish",
    )(us, vs, tm, sm, kmt, su, sv, rw, re, *wide, kv, dv, vb, *state, rnorth, rsouth, first)


def solution(mesh):
    sizes = mesh.shape["row"], mesh.shape["col"]

    def local_step(u, v, t, s, eta, tu, tv, depth, kmt, tide):
        u, v, t, s, eta, tu, tv, depth, kmt = (pltpu.with_memory_space_constraint(x, pltpu.HBM) for x in (u, v, t, s, eta, tu, tv, depth, kmt))
        tm, sm, pr, tke, tkw, trn, first, rw, re, rsouth, rnorth, corner, rown, *wide = tracers(sizes, t, s, u, v, kmt, depth, eta, tu, tv)
        geo, state = wide[:4], wide[4:]
        tm, sm = (pltpu.with_memory_space_constraint(x, pltpu.VMEM) for x in (tm, sm))
        first = pltpu.with_memory_space_constraint(first, pltpu.HBM)
        pr = pltpu.with_memory_space_constraint(pr, pltpu.HBM)
        us, vs, fx, fy, su, sv, uke, vrow = momentum(u, v, pr, first, geo, rw, re, rnorth, rsouth, rown, corner)
        eta_n, u_n, v_n, ub, vb, fw, fe, fsouth, fnorth = subcycles(sizes, *state, *geo, fx, fy, tide.T, uke, tke, tkw, vrow, trn, first)
        us = pltpu.with_memory_space_constraint(us, pltpu.VMEM)
        vs = pltpu.with_memory_space_constraint(vs, pltpu.HBM)
        return finish(us, vs, tm, sm, first, kmt, geo, ub, vb, su, sv, fw, fe, fnorth, fsouth, (eta_n, u_n, v_n))

    cube, plane = P(None, "row", "col"), P("row", "col")
    return jax.shard_map(
        local_step,
        mesh=mesh,
        in_specs=(cube,) * 4 + (plane,) * 5 + (P(None, None),),
        out_specs=(plane,) * 3 + (cube,) * 4,
        check_vma=False,
    )
```
